128 devices in a mesh: band: 8 (over y, core), row: 16 (over x, z).
Axes of the slice: x: 4, y: 4, z: 4, core: 2. Of those that a mesh axis runs over, the one named last changes fastest.
Arguments:
- observed: bfloat16 [224, 512, 680], P('band', 'row'), may hold values from -60 to 60
- row_taps: float32 [224, 25], P('band'), may hold values from 0 to 0.08
- col_taps: float32 [224, 25], P('band'), may hold values from 0 to 0.08
- spectral_basis: bfloat16 [224, 32], replicated, may hold values from -0.375 to 0.375
- ridge_weights: float32 [32], replicated, may hold values from 0.05 to 0.5
Outputs:
- coefficients: float32 [32, 512, 680], P(None, 'row', 'band')
- residual: float32 [32, 512, 680], P(None, 'row', 'band')
The draws below stay inside these ranges and needn't reach their ends.
All inputs are finite; a program needn't handle non-finite values.
Results may differ from the reference program's by a relative error of at most 0.01.
Values may be sent and summed in bfloat16 or wider, within the bound.
A program may use at most 64 MiB of HBM per device.

```python
import math
import jax
import jax.numpy as jnp
from jax import lax

B = 224
K = 32
W = 680
TAPS = 25
ITERS = 2
H = 512


def draw_observed(key, part):
    position = jnp.arange(W, dtype=jnp.float32) / (W - 1)
    profile = 2.0 * jnp.exp(jnp.log(4.0) * position)
    values = jax.random.normal(key, (B, H, W), jnp.float32)
    values = jnp.clip(values * profile[None, None, :], -60.0, 60.0)
    return values.astype(jnp.bfloat16)


def block_levels(stream_key, extent, shards, low, top_value):
    gain = 1.0
    for dim, parts in shards:
        draws = jax.random.uniform(jax.random.fold_in(jax.random.fold_in(stream_key, 6), dim), (parts,), jnp.float32, low / len(shards), top_value / len(shards))
        gain = gain * jnp.repeat(jnp.exp(draws), extent[dim] // parts).reshape((-1,) + (1,) * (len(extent) - 1 - dim))
    return gain


def normal_values(rng, shape, spread, bound, kind=jnp.bfloat16):
    entries = spread * jax.random.normal(rng, shape, jnp.float32)
    return jnp.clip(entries, min=-bound, max=bound).astype(kind)


def setup_inputs(seed: int = 0) -> dict:
    streams_of = jax.random.split(jax.random.key(seed), 6)
    observed = draw_observed(jax.random.fold_in(streams_of[5], 71), 0)
    row_taps = jnp.clip(0.08 * jax.random.uniform(streams_of[1], (B, TAPS), jnp.float32) ** block_levels(streams_of[1], (B, TAPS), ((0, 8),), -0.2, 0.2), 0.0, 0.08)
    col_taps = jnp.clip(0.08 * jax.random.uniform(streams_of[2], (B, TAPS), jnp.float32) ** block_levels(streams_of[2], (B, TAPS), ((0, 8),), -0.2, 0.2), 0.0, 0.08)
    spectral_basis = normal_values(streams_of[3], (B, K), B ** -0.5, 0.375)
    ridge_weights = jnp.clip(jnp.exp(jax.random.uniform(streams_of[4], (K,), jnp.float32, math.log(0.05), math.log(0.5))), 0.05, 0.5)
    return dict(observed=observed, row_taps=row_taps, col_taps=col_taps, spectral_basis=spectral_basis, ridge_weights=ridge_weights)


def rows_plain(field, kernel):
    radius = (kernel.shape[0] - 1) // 2
    height = field.shape[0]
    padded = jnp.pad(field, ((radius, radius), (0, 0)))
    running = jnp.zeros(field.shape, jnp.float32)
    for offset in range(kernel.shape[0]):
        running = running + kernel[offset] * padded[offset:offset + height, :].astype(jnp.float32)
    return running


def cols_plain(field, kernel):
    radius = (kernel.shape[0] - 1) // 2
    width_cols = field.shape[1]
    padded = jnp.pad(field, ((0, 0), (radius, radius)))
    running = jnp.zeros(field.shape, jnp.float32)
    for offset in range(kernel.shape[0]):
        running = running + kernel[offset] * padded[:, offset:offset + width_cols]
    return running


def blur_plain(field, row_kernel, col_kernel):
    return cols_plain(rows_plain(field, row_kernel), col_kernel)


def adjoint_band(items):
    field, row_kernel, col_kernel = items
    return blur_plain(field, row_kernel[::-1], col_kernel[::-1]).astype(jnp.bfloat16)


def normal_band(items):
    field, row_kernel, col_kernel = items
    blurred = blur_plain(field, row_kernel, col_kernel).astype(jnp.bfloat16)
    return blur_plain(blurred, row_kernel[::-1], col_kernel[::-1]).astype(jnp.bfloat16)


def reference(observed, row_taps, col_taps, spectral_basis, ridge_weights):
    bands, height, width_cols = observed.shape
    comps = spectral_basis.shape[1]
    basis_wide = spectral_basis.astype(jnp.float32)
    adjoint_obs = lax.map(adjoint_band, (observed, row_taps, col_taps))
    rhs = jnp.dot(spectral_basis.T, adjoint_obs.reshape(bands, height * width_cols), preferred_element_type=jnp.float32).reshape(comps, height, width_cols)

    def normal_map(direction):
        spectra = jnp.dot(basis_wide, direction.reshape(comps, height * width_cols), precision=lax.Precision.HIGHEST)
        spectra = spectra.reshape(bands, height, width_cols).astype(jnp.bfloat16)
        returned = lax.map(normal_band, (spectra, row_taps, col_taps))
        projected = jnp.dot(spectral_basis.T, returned.reshape(bands, height * width_cols), preferred_element_type=jnp.float32).reshape(comps, height, width_cols)
        return projected + ridge_weights[:, None, None] * direction

    solution = jnp.zeros_like(rhs)
    residual = rhs
    direction = rhs
    norm_now = jnp.sum(residual * residual)
    for iteration in range(ITERS):
        mapped = normal_map(direction)
        alpha = norm_now / jnp.sum(direction * mapped)
        solution = solution + alpha * direction
        residual = residual - alpha * mapped
        norm_next = jnp.sum(residual * residual)
        direction = residual + (norm_next / norm_now) * direction
        norm_now = norm_next
    return solution, residual
```

```python
import functools

import jax
import jax.numpy as jnp
from jax import lax
from jax.experimental import pallas as pl
from jax.experimental.pallas import tpu as pltpu
from jax.sharding import Mesh
from jax.sharding import PartitionSpec as P

AXES = ("band_0", "band_1", "row_0", "row_1")
BAND = ("band_0", "band_1")
ROW = ("row_0", "row_1")
TAPS = 25
RAD = 12
HALO = 24
LANES = 128
BF = jnp.bfloat16
F32 = jnp.float32


def iota(shape, dim):
    return lax.broadcasted_iota(jnp.int32, shape, dim)


def toeplitz(line, rows, lanes, shift):
    step = pltpu.roll(jnp.broadcast_to(line, (8, lanes)), 0, 1, stride=1, stride_axis=0)
    tiles = []
    for g in range(rows // 8):
        turn = (shift + 8 * g) % lanes
        tiles.append(pltpu.roll(step, turn, 1) if turn else step)
    return jnp.concatenate(tiles, axis=0)


def mm(a, b):
    return lax.dot_general(a, b, (((1,), (0,)), ((), ())), preferred_element_type=F32)


def normal_build_kernel(sizes, taps_ref, tt_ref, rr_ref):
    rows, cols, height, width = sizes
    row_dev = lax.axis_index(ROW)
    col_dev = lax.axis_index(BAND)
    mid_c = cols + 2 * RAD
    mid_r = rows + 2 * RAD
    ext_r = rows + 2 * HALO
    ku = tt_ref.shape[1]
    i1, u1 = iota((ku, LANES), 0), iota((ku, LANES), 1)
    col_u = col_dev * cols - RAD + u1
    keep1 = (i1 - u1 >= 0) & (i1 - u1 < TAPS) & (u1 < mid_c) & (col_u >= 0) & (col_u < width)
    u2, o2 = iota((LANES, LANES), 0), iota((LANES, LANES), 1)
    keep2 = (u2 - o2 >= 0) & (u2 - o2 < TAPS) & (o2 < cols) & (u2 < mid_c)
    ur, lr = iota((64, 256), 0), iota((64, 256), 1)
    row_u = row_dev * rows - RAD + ur
    keep_r = (ur < mid_r) & (row_u >= 0) & (row_u < height)
    r2, v2 = iota((rows, LANES), 0), iota((rows, LANES), 1)
    keep_r2 = (v2 - r2 >= 0) & (v2 - r2 < TAPS)

    def body(t, carry):
        for q in range(3):
            b = 3 * t + q
            line = taps_ref[b]
            ct, ctr = line[0:1, :LANES], line[1:2, :LANES]
            rt, rtr = line[2:3], line[3:4, :LANES]
            t1 = jnp.where(keep1, toeplitz(ctr, ku, LANES, -HALO), 0.0).astype(BF)
            t2 = jnp.where(keep2, toeplitz(ct, LANES, LANES, -HALO), 0.0).astype(BF)
            tt_ref[b] = mm(t1, t2).astype(BF)
            d1 = lr - ext_r * q - ur
            r1 = jnp.where(keep_r & (d1 >= 0) & (d1 < TAPS), toeplitz(rt, 64, 256, ext_r * q), 0.0)
            ra = jnp.where(keep_r2, toeplitz(rtr, rows, LANES, 0), 0.0).astype(BF)
            rr_ref[t, rows * q : rows * (q + 1), :] = mm(ra[:, :64], r1.astype(BF)).astype(BF)
        return carry

    lax.fori_loop(0, rr_ref.shape[0], body, 0)


def normal_kernel(sizes, pe_ref, e8_ref, p8_ref, tt_ref, rr_ref, p_ref, ridge_ref, out_ref, spec, mid, fin):
    rows, cols, _, _ = sizes
    ext_r = rows + 2 * HALO
    comps = p_ref.shape[0]
    bands = tt_ref.shape[0]
    chunk = 45

    def expand(i, carry):
        x = pe_ref[:, pl.ds(pl.multiple_of(16 * i, 16), 16), :].astype(F32)
        x0 = x[:, :8, :].reshape(comps * 8, 256).astype(BF)
        x1 = x[:, 8:, :].reshape(comps * 8, 256).astype(BF)
        for m in range(bands // chunk):
            e = e8_ref[8 * chunk * m : 8 * chunk * (m + 1), :]
            y0 = mm(e, x0).reshape(chunk, 8, 256)
            y1 = mm(e, x1).reshape(chunk, 8, 256)
            y = jnp.concatenate([y0, y1], axis=1).astype(BF)
            spec[chunk * m : chunk * (m + 1), pl.ds(pl.multiple_of(16 * i, 16), 16), :] = y
        return carry

    lax.fori_loop(0, ext_r // 16, expand, 0)

    ku = tt_ref.shape[1]

    def columns(g, carry):
        for q in range(9):
            b = 9 * g + q
            mid[b] = mm(spec[b][:, :ku], tt_ref[b]).astype(BF)
        return carry

    lax.fori_loop(0, bands // 9, columns, 0)

    def along(g, carry):
        for q in range(5):
            t = 5 * g + q
            x = mid[pl.ds(3 * t, 3)].reshape(3 * ext_r, LANES)
            y = mm(rr_ref[t][:, : 3 * ext_r], x)
            fin[pl.ds(3 * t, 3)] = y.reshape(3, rows, LANES)
        return carry

    lax.fori_loop(0, bands // 15, along, 0)

    def project(i, carry):
        sl = pl.ds(pl.multiple_of(8 * i, 8), 8)
        x = fin[:, sl, :].reshape(bands * 8, LANES).astype(BF)
        y = mm(p8_ref[...], x).reshape(comps, 8, LANES)
        out_ref[:, sl, :] = y + ridge_ref[...] * p_ref[:, sl, :]
        return carry

    lax.fori_loop(0, rows // 8, project, 0)


def rhs_kernel(sizes, obs_ref, taps_ref, p8_ref, out_ref, racc, tacc, fin):
    rows, cols, _, _ = sizes
    nb = obs_ref.shape[0]
    mid_r = rows + 2 * RAD
    win = 2 * cols + 2 * RAD
    kw = tacc.shape[0]
    pairs = fin.shape[0]
    r, l = iota((rows, 256), 0), iota((rows, 256), 1)
    w, o = iota((kw, LANES), 0), iota((kw, LANES), 1)
    keep_a = (w - o >= 0) & (w - o < TAPS) & (o < cols) & (w < win)
    o_b = o + cols
    keep_b = (w - o_b >= 0) & (w - o_b < TAPS) & (o < cols) & (w < win)

    def body(g, carry):
        for q in range(4):
            b = 4 * g + q
            rtr = taps_ref[b][3:4]
            d = l - mid_r * q - r
            m = jnp.where((d >= 0) & (d < TAPS), toeplitz(rtr, rows, 256, mid_r * q), 0.0)
            racc[rows * q : rows * (q + 1), :] = m.astype(BF)
        x = obs_ref[pl.ds(4 * g, 4)].astype(F32).reshape(4 * mid_r, obs_ref.shape[2]).astype(BF)
        y = mm(racc[:, : 4 * mid_r], x)
        full = obs_ref.shape[2]
        wins = []
        for k in range(pairs):
            start = 2 * cols * k - RAD
            wins.append(pltpu.roll(y, (full - start) % full, 1)[:, :256].astype(BF))
        for q in range(4):
            b = 4 * g + q
            ct = taps_ref[b][0:1, :LANES]
            ta = jnp.where(keep_a, toeplitz(ct, kw, LANES, -HALO), 0.0).astype(BF)
            tb = jnp.where(keep_b, toeplitz(ct, kw, LANES, -HALO - cols), 0.0).astype(BF)
            tacc[:, :LANES] = ta
            tacc[:, LANES:] = tb
            x = jnp.concatenate([v[rows * q : rows * (q + 1)] for v in wins], axis=0)
            z = mm(x[:, :kw], tacc[...])
            for k in range(pairs):
                fin[k, b] = z[rows * k : rows * (k + 1)]
        return carry

    lax.fori_loop(0, nb // 4, body, 0)
    comps = out_ref.shape[1]
    for k in range(pairs):
        def project(i, carry):
            sl = pl.ds(pl.multiple_of(8 * i, 8), 8)
            x = fin[k, :, sl, :].reshape(nb * 8, 256).astype(BF)
            y = mm(p8_ref[...], x).reshape(comps, 8, 256)
            out_ref[2 * k, :, sl, :] = y[:, :, :LANES]
            out_ref[2 * k + 1, :, sl, :] = y[:, :, LANES:]
            return carry

        lax.fori_loop(0, rows // 8, project, 0)


def vmem():
    return pl.BlockSpec(memory_space=pltpu.VMEM)


def call(kernel, outs, ins, scratch, flops):
    return pl.pallas_call(
        kernel,
        out_shape=outs,
        in_specs=[vmem()] * ins,
        out_specs=jax.tree.map(lambda _: vmem(), outs),
        scratch_shapes=scratch,
        compiler_params=pltpu.CompilerParams(vmem_limit_bytes=60 * 1024 * 1024),
        cost_estimate=pl.CostEstimate(flops=flops, bytes_accessed=16 * 1024 * 1024, transcendentals=0),
    )


def shifted(x, axis, step):
    count = lax.axis_size(axis)
    if step > 0:
        pairs = [(i, i + 1) for i in range(count - 1)]
    else:
        pairs = [(i + 1, i) for i in range(count - 1)]
    return lax.ppermute(x, axis, pairs)


def local(height, width, observed, row_taps, col_taps, spectral_basis, ridge_weights):
    own, rows, _ = observed.shape
    bands, comps = spectral_basis.shape
    cols = width // lax.axis_size(BAND)
    sizes = (rows, cols, height, width)
    full = -(-width // LANES) * LANES
    padded_bands = -(-bands // 45) * 45

    obs = jnp.concatenate(
        [shifted(observed[:, rows - RAD :], ROW, 1), observed, shifted(observed[:, :RAD], ROW, -1)], axis=1
    )
    obs = jnp.pad(obs, ((0, 0), (0, 0), (0, full - width)))

    both = jnp.stack([col_taps, col_taps[:, ::-1], row_taps, row_taps[:, ::-1]], axis=1)
    own_lines = jnp.pad(both, ((0, 0), (0, 4), (0, 256 - TAPS)))
    every = lax.all_gather(both, BAND, axis=0, tiled=True)
    every = jnp.pad(every, ((0, padded_bands - bands), (0, 4), (0, 256 - TAPS)))

    eye = jnp.eye(8, dtype=BF)
    basis = jnp.pad(spectral_basis, ((0, padded_bands - bands), (0, 0)))
    e8 = (basis[:, None, :, None] * eye[None, :, None, :]).reshape(padded_bands * 8, comps * 8)
    p8 = (basis.T[:, None, :, None] * eye[None, :, None, :]).reshape(comps * 8, padded_bands * 8)
    mine = lax.dynamic_slice_in_dim(spectral_basis, lax.axis_index(BAND) * own, own, 0)
    p8_own = (mine.T[:, None, :, None] * eye[None, :, None, :]).reshape(comps * 8, own * 8)

    ku = 144
    tt, rr = call(
        functools.partial(normal_build_kernel, sizes),
        (
            jax.ShapeDtypeStruct((padded_bands, ku, LANES), BF),
            jax.ShapeDtypeStruct((padded_bands // 3, 3 * rows, 256), BF),
        ),
        1,
        [],
        2 * 10**9,
    )(every)

    partial = call(
        functools.partial(rhs_kernel, sizes),
        jax.ShapeDtypeStruct((lax.axis_size(BAND), comps, rows, LANES), F32),
        3,
        [
            pltpu.VMEM((4 * rows, 256), BF),
            pltpu.VMEM((208, 256), BF),
            pltpu.VMEM((lax.axis_size(BAND) // 2, own, rows, 256), F32),
        ],
        2 * 10**9,
    )(obs, own_lines, p8_own)
    rhs = lax.psum_scatter(partial, BAND, scatter_dimension=0, tiled=True)[0]

    ridge = jnp.broadcast_to(ridge_weights[:, None, None], (comps, 8, LANES))

    def normal(p):
        b = p[:, :, :cols].astype(BF)
        ext = jnp.concatenate([shifted(b[:, rows - HALO :], ROW, 1), b, shifted(b[:, :HALO], ROW, -1)], axis=1)
        ext = jnp.concatenate(
            [shifted(ext[:, :, cols - HALO :], BAND, 1), ext, shifted(ext[:, :, :HALO], BAND, -1)], axis=2
        )
        ext = jnp.pad(ext, ((0, 0), (0, 0), (0, 256 - ext.shape[2])))
        return call(
            functools.partial(normal_kernel, sizes),
            jax.ShapeDtypeStruct((comps, rows, LANES), F32),
            7,
            [
                pltpu.VMEM((padded_bands, rows + 2 * HALO, 256), BF),
                pltpu.VMEM((padded_bands, rows + 2 * HALO, LANES), BF),
                pltpu.VMEM((padded_bands, rows, LANES), F32),
            ],
            2 * 10**10,
        )(ext, e8, p8, tt, rr, p, ridge)

    q = normal(rhs)
    s = normal(q)

    dots = lax.psum(
        jnp.stack([jnp.sum(rhs * rhs), jnp.sum(rhs * q), jnp.sum(q * q), jnp.sum(rhs * s), jnp.sum(q * s)]), AXES
    )
    rr0, rq, qq, rs, qs = [dots[i] for i in range(5)]
    alpha = rr0 / rq
    rr1 = rr0 - 2.0 * alpha * rq + alpha * alpha * qq
    beta = rr1 / rr0
    g = 1.0 + beta
    curve = g * g * rq - alpha * g * (qq + rs) + alpha * alpha * qs
    alpha2 = rr1 / curve
    coefs = alpha * rhs + alpha2 * (g * rhs - alpha * q)
    resid = (rhs - alpha * q) - alpha2 * (g * q - alpha * s)
    return coefs[:, :, :cols], resid[:, :, :cols]


def solution(mesh):
    split = Mesh(mesh.devices.reshape(4, 2, 4, 4), AXES)
    placed = (P(BAND, ROW, None), P(BAND, None), P(BAND, None), P(), P())

    def whole(observed, row_taps, col_taps, spectral_basis, ridge_weights):
        _, height, width = observed.shape
        return jax.shard_map(
            functools.partial(local, height, width),
            mesh=split,
            in_specs=placed,
            out_specs=(P(None, ROW, BAND), P(None, ROW, BAND)),
            check_vma=False,
        )(observed, row_taps, col_taps, spectral_basis, ridge_weights)

    return whole
```

```python
import functools

import jax
import jax.numpy as jnp
from jax import lax
from jax.experimental import pallas as pl
from jax.experimental.pallas import tpu as pltpu
from jax.sharding import Mesh
from jax.sharding import PartitionSpec as P

AXES = ("band_0", "band_1", "row_0", "row_1")
BAND = ("band_0", "band_1")
ROW = ("row_0", "row_1")
TAPS = 25
RAD = 12
HALO = 24
LANES = 128
SLOT = 64
BF = jnp.bfloat16
F32 = jnp.float32


def iota(shape, dim):
    return lax.broadcasted_iota(jnp.int32, shape, dim)


def mm(a, b):
    return lax.dot_general(a, b, (((1,), (0,)), ((), ())), preferred_element_type=F32)


def onehot(mask):
    return jnp.where(mask, 1.0, 0.0)


def staircase(line, rows, shift):
    step = pltpu.roll(jnp.broadcast_to(line, (8, LANES)), 0, 1, stride=1, stride_axis=0)
    tiles = []
    for g in range(rows // 8):
        turn = (shift + 8 * g) % LANES
        tiles.append(pltpu.roll(step, turn, 1) if turn else step)
    return jnp.concatenate(tiles, axis=0)


def kernel(
    dims, obs, edges, feats, taps, basis, basis_t, ridge,
    out_x, out_r,
    edge_in, line_in, lines, rows_adj, cols_adj, zed, keep, out_a, in_a, out_b, in_b,
    tt, rr, e8, p8, p8_own, spec, mid, fin, work, ext, pack, pack_in, vec, red_src, red_in,
    edge_sem, line_sem, a_sem, b_sem, row_sem, col_sem, red_sem,
):
    cols, sizes = dims
    ny, nc, nx, nz = sizes
    nbd, nrow = ny * nc, nx * nz
    y, core = lax.axis_index("band_0"), lax.axis_index("band_1")
    x, z = lax.axis_index("row_0"), lax.axis_index("row_1")
    j, i_row = y * nc + core, x * nz + z
    own, rows, full = obs.shape
    bands, comps = basis.shape
    ext_r = rows + 2 * HALO
    nblk, next_ = rows // 8, ext_r // 8
    ck = comps * 8
    ku = tt.shape[1]
    first, last = j == 0, j == nbd - 1
    top_dev, low_dev = i_row == 0, i_row == nrow - 1

    def at_band(jj):
        return (jj // nc, lax.rem(jj, nc), x, z)

    def at_row(ii):
        return (y, core, ii // nz, lax.rem(ii, nz))

    up = at_row(lax.rem(i_row + nrow - 1, nrow))
    down = at_row(lax.rem(i_row + 1, nrow))
    left = at_band(lax.rem(j + nbd - 1, nbd))
    right = at_band(lax.rem(j + 1, nbd))
    partner = (y, 1 - core, x, z)
    peers = [at_band(lax.rem(j + s, nbd)) for s in range(1, nbd)]
    peers_x = [(y, core, lax.rem(x + s, nx), z) for s in range(1, nx)]
    peers_z = [(y, core, x, lax.rem(z + s, nz)) for s in range(1, nz)]

    barrier = pltpu.get_barrier_semaphore()
    everyone = [up, down] + peers + peers_x + peers_z
    for d in everyone:
        pl.semaphore_signal(barrier, inc=1, device_id=d, device_id_type=pl.DeviceIdType.MESH)
    pl.semaphore_wait(barrier, len(everyone))

    def remote(src, dst, send, recv, device):
        return pltpu.make_async_remote_copy(
            src_ref=src, dst_ref=dst, send_sem=send, recv_sem=recv,
            device_id=device, device_id_type=pl.DeviceIdType.MESH,
        )

    to_up = remote(edges.at[0], edge_in.at[1], edge_sem.at[0], edge_sem.at[2], up)
    to_down = remote(edges.at[1], edge_in.at[0], edge_sem.at[1], edge_sem.at[3], down)
    to_up.start()
    to_down.start()

    line_copies = []
    row_kind = jnp.where(low_dev, 3, 2)
    for s in range(1, nbd):
        dest = lax.rem(j + s, nbd)
        for k, kind in enumerate((jnp.where(dest == nbd - 1, 1, 0), row_kind)):
            c = remote(
                feats.at[kind], line_in.at[j, k], line_sem.at[0, s - 1, k], line_sem.at[1, s - 1, k], at_band(dest)
            )
            c.start()
            line_copies.append(c)
    line_in[j, 0] = feats[jnp.where(last, 1, 0)]
    line_in[j, 1] = feats[row_kind]

    r, l = iota((rows, LANES), 0), iota((rows, LANES), 1)

    def own_rows(g, carry):
        for q in range(4):
            line = taps[4 * g + q][1:2]
            d = l - rows * q + RAD - r
            m = (d >= 0) & (d < TAPS) & (l >= rows * q) & (l < rows * (q + 1))
            mine = jnp.where(m, staircase(line, rows, rows * q - RAD), 0.0)
            k = l - RAD * q
            d = k - r
            m = (d >= 0) & (d < TAPS) & (k >= 0) & (k < RAD)
            above = jnp.where(m, staircase(line, rows, RAD * q), 0.0)
            k = l - 4 * RAD - RAD * q
            d = k + rows + RAD - r
            m = (d >= 0) & (d < TAPS) & (k >= 0) & (k < RAD)
            below = jnp.where(m, staircase(line, rows, 4 * RAD + RAD * q - RAD - rows), 0.0)
            rows_adj[g, rows * q : rows * (q + 1), :LANES] = mine.astype(BF)
            rows_adj[g, rows * q : rows * (q + 1), LANES:] = (above + below).astype(BF)
        return carry

    lax.fori_loop(0, own // 4, own_rows, 0)

    kw = cols_adj.shape[1]
    w, o = iota((kw, LANES), 0), iota((kw, LANES), 1)

    def own_cols(b, carry):
        line = taps[b][0:1]
        for k in range(2):
            d = w - o - cols * k
            m = (d >= 0) & (d < TAPS) & (o < cols)
            t = jnp.where(m, staircase(line, kw, -HALO - cols * k), 0.0)
            cols_adj[b, :, LANES * k : LANES * (k + 1)] = t.astype(BF)
        return carry

    lax.fori_loop(0, own, own_cols, 0)

    spread = onehot(iota((comps, ck), 0) == (iota((comps, ck), 1) >> 3)).astype(BF)
    wide = mm(basis[...], spread)
    step = bands // 4
    er, el = iota((8 * step, ck), 0), iota((8 * step, ck), 1)
    for c in range(4):
        v = jnp.broadcast_to(wide[step * c : step * (c + 1)][:, None, :], (step, 8, ck)).reshape(8 * step, ck)
        e8[8 * step * c : 8 * step * (c + 1)] = jnp.where((er & 7) == (el & 7), v, 0.0).astype(BF)
    tall = onehot(iota((ck, comps), 1) == (iota((ck, comps), 0) >> 3)).astype(BF)
    tall = mm(tall, basis_t[...]).astype(BF)
    br, bl = iota((256, 256), 0), iota((256, 256), 1)
    same = (br & 7) == (bl & 7)

    def widen(start):
        return jnp.where(same, mm(tall, onehot(br == start + (bl >> 3)).astype(BF)), 0.0).astype(BF)

    for c in range(bands // 32):
        p8[:, 256 * c : 256 * (c + 1)] = widen(32 * c)
    p8_own[...] = widen(own * j)

    for c in line_copies:
        c.wait()
    for k in range(2):
        for jj in range(nbd):
            lines[k, own * jj : own * (jj + 1)] = line_in[jj, k][:own].astype(F32)
    groups = bands // 8
    wide_n = 16 * LANES

    def shifted(depth, hit, edge_hit):
        f, n = iota((depth, wide_n), 0), iota((depth, wide_n), 1)
        s = onehot(f == hit(n))
        if edge_hit is not None:
            s = s - onehot(f == edge_hit(n))
        return s.astype(BF)

    def unfold(k, depth, sel):
        res = mm(lines[k, :, :depth].astype(BF), sel)
        for t in range(16):
            work[:, 8 * t : 8 * (t + 1), :] = res[:, LANES * t : LANES * (t + 1)].reshape(groups, 8, LANES)

    def tt_pair(p, carry, depth):
        def hit(n):
            a, b = 16 * p + (n >> 7), n & 127
            return jnp.where((b < cols) & (a < cols + 2 * HALO) & (a - b <= 2 * HALO), a - b, -1)

        def edge_hit(n):
            a, b = 16 * p + (n >> 7) - HALO, n & 127
            a, b = jnp.where(last, cols - 1 - a, a), jnp.where(last, cols - 1 - b, b)
            ok = (first | last) & (a >= 0) & (a < RAD) & (b >= 0) & (b < RAD)
            return jnp.where(ok, SLOT + RAD * a + b, -1)

        unfold(0, depth, shifted(depth, hit, edge_hit if depth > SLOT else None))

        def place(g, c):
            for s in range(8):
                v = work[g, pl.ds(s, 16, stride=8), :]
                tt[8 * g + s, pl.ds(pl.multiple_of(16 * p, 16), 16), :] = v.astype(BF)
            return c

        lax.fori_loop(0, groups, place, 0)
        return carry

    lax.fori_loop(0, ku // 16, functools.partial(tt_pair, depth=SLOT), 0)

    @pl.when(first | last)
    def _():
        p0 = jnp.where(first, HALO // 16, (cols + RAD - 1) // 16)
        lax.fori_loop(p0, p0 + 2, functools.partial(tt_pair, depth=256), 0)

    third = rr.shape[0]
    lane16 = iota((16, LANES), 1)

    def rr_pair(p, carry):
        def hit(n):
            a, b = 16 * p + (n >> 7), n & 127
            return jnp.where((b < ext_r) & (b >= a) & (b - a <= 2 * HALO), b - a, -1)

        def edge_hit(n):
            a, b = 16 * p + (n >> 7), (n & 127) - HALO
            a, b = jnp.where(low_dev, rows - 1 - a, a), jnp.where(low_dev, rows - 1 - b, b)
            ok = (top_dev | low_dev) & (a >= 0) & (a < RAD) & (b >= 0) & (b < RAD)
            return jnp.where(ok, SLOT + RAD * a + b, -1)

        unfold(1, 256, shifted(256, hit, edge_hit))
        for q in range(3):
            lo = ext_r * q

            def place(g, c):
                for s in range(8):
                    v = work[g, pl.ds(s, 16, stride=8), :]
                    if lo % LANES:
                        v = pltpu.roll(v, lo % LANES, 1)
                    t0 = v if lo + ext_r <= LANES else jnp.where(lane16 >= lo, v, 0.0)
                    t1 = v if lo >= LANES else jnp.where(lane16 < lo + ext_r - LANES, v, 0.0)
                    at = (8 * g + s - third * q, pl.ds(pl.multiple_of(rows * q + 16 * p, 16), 16))
                    rr[at + (slice(0, LANES),)] = t0.astype(BF)
                    rr[at + (slice(LANES, 2 * LANES),)] = t1.astype(BF)
                return c

            lax.fori_loop(third * q // 8, min(third * (q + 1), bands) // 8, place, 0)
        return carry

    lax.fori_loop(0, rows // 16, rr_pair, 0)

    to_up.wait()
    to_down.wait()
    above_ok, below_ok = i_row > 0, i_row < nrow - 1

    def adjoint(g, carry):
        e = pl.ds(pl.multiple_of(4 * RAD * g, 16), 4 * RAD)
        above = edge_in[0, e]
        below = edge_in[1, e]
        mine = obs[pl.ds(4 * g, 4)].reshape(4 * rows, full)
        above = jnp.where(above_ok, above, jnp.zeros_like(above))
        below = jnp.where(below_ok, below, jnp.zeros_like(below))
        v = mm(rows_adj[g][:, : 4 * rows + 8 * RAD], jnp.concatenate([mine, above, below], axis=0))
        wins = []
        for k in range(ny):
            start = nc * cols * k - RAD
            wins.append(pltpu.roll(v, (full - start) % full, 1)[:, :256].astype(BF))
        for q in range(4):
            u = jnp.concatenate([t[rows * q : rows * (q + 1)] for t in wins], axis=0)
            u = mm(u[:, :kw], cols_adj[4 * g + q])
            for k in range(ny):
                zed[k, 4 * g + q] = u[rows * k : rows * (k + 1)]
        return carry

    lax.fori_loop(0, own // 4, adjoint, 0)

    offsets = [s for s in (2, 1, 3, 0) if s < ny]
    a_copies, b_copies = [], []

    def merge(idx):
        a_copies[idx].wait()
        done = idx == len(offsets) - 1

        def add(i, carry):
            v = keep[idx, i] + in_a[idx, i].astype(F32)
            if done:
                vec[0, i] = v
            else:
                out_b[idx, i] = v.astype(BF)
            return carry

        lax.fori_loop(0, nblk, add, 0)
        if not done:
            dest = (lax.rem(y + offsets[idx], ny), core, x, z)
            c = remote(out_b.at[idx], in_b.at[idx], b_sem.at[0, idx], b_sem.at[1, idx], dest)
            c.start()
            b_copies.append(c)

    for idx, off in enumerate(offsets):
        k = lax.rem(y + off, ny)

        def project(i, carry):
            v = zed[k, :, pl.ds(pl.multiple_of(8 * i, 8), 8), :].reshape(own * 8, 256).astype(BF)
            v = mm(p8_own[:, : own * 8], v)
            lo, hi = v[:, :LANES], v[:, LANES:]
            keep[idx, i] = jnp.where(core == 0, lo, hi)
            out_a[idx, i] = jnp.where(core == 0, hi, lo).astype(BF)
            return carry

        lax.fori_loop(0, nblk, project, 0)
        c = remote(out_a.at[idx], in_a.at[idx], a_sem.at[0, idx], a_sem.at[1, idx], partner)
        c.start()
        a_copies.append(c)
        if idx:
            merge(idx - 1)
    merge(len(offsets) - 1)
    mid[pl.ds(bands, mid.shape[0] - bands)] = jnp.zeros((mid.shape[0] - bands, ext_r, LANES), BF)
    for idx, c in enumerate(b_copies):
        c.wait()

        def collect(i, carry):
            vec[0, i] = vec[0, i] + in_b[idx, i].astype(F32)
            return carry

        lax.fori_loop(0, nblk, collect, 0)

    chunk = ck // 4
    per = next_ // 2
    lane_c = iota((chunk, LANES), 1)
    lane_k = iota((ck, LANES), 1)

    def normal(n, carry):
        def stage(i, c):
            ext[n, 3 + i] = vec[n, i].astype(BF)
            return c

        lax.fori_loop(0, nblk, stage, 0)
        r_up = remote(ext.at[n, pl.ds(3, 3)], ext.at[n, pl.ds(3 + nblk, 3)], row_sem.at[n, 0], row_sem.at[n, 2], up)
        r_down = remote(ext.at[n, pl.ds(nblk, 3)], ext.at[n, pl.ds(0, 3)], row_sem.at[n, 1], row_sem.at[n, 3], down)
        r_up.start()
        r_down.start()
        r_up.wait()
        r_down.wait()

        def packing(c, cc):
            t, part = c // 4, lax.rem(c, 4)
            sl = pl.ds(pl.multiple_of(chunk * part, chunk), chunk)
            a = jnp.zeros((chunk, LANES), F32)
            b = a
            for g in range(per):
                v = ext[n, per * t + g, sl, :].astype(F32)
                m = (lane_c >= HALO * g) & (lane_c < HALO * (g + 1))
                a = jnp.where(m, pltpu.roll(v, HALO * g, 1) if g else v, a)
                b = jnp.where(m, pltpu.roll(v, (HALO * g - cols + HALO) % LANES, 1), b)
            pack[n, 0, t, sl, :] = a.astype(BF)
            pack[n, 1, t, sl, :] = b.astype(BF)
            return cc

        lax.fori_loop(0, 8, packing, 0)
        c_left = remote(pack.at[n, 0], pack_in.at[n, 1], col_sem.at[n, 0], col_sem.at[n, 2], left)
        c_right = remote(pack.at[n, 1], pack_in.at[n, 0], col_sem.at[n, 1], col_sem.at[n, 3], right)
        c_left.start()
        c_right.start()
        c_left.wait()
        c_right.wait()

        def block(blk):
            t, g = blk // per, lax.rem(blk, per)
            mine = pltpu.roll(ext[n, blk].astype(F32), HALO, 1)
            a = pltpu.roll(pack_in[n, 0, t].astype(F32), lax.rem(LANES - HALO * g, LANES), 1)
            b = pltpu.roll(pack_in[n, 1, t].astype(F32), lax.rem(2 * LANES + cols + HALO - HALO * g, LANES), 1)
            inside = jnp.logical_not((top_dev & (blk < 3)) | (low_dev & (blk >= 3 + nblk)))
            a_ok = inside & jnp.logical_not(first)
            b_ok = inside & jnp.logical_not(last)
            a = jnp.where(a_ok, a, 0.0)
            b = jnp.where(b_ok, b, 0.0)
            mine = jnp.where(inside, mine, 0.0)
            t0 = jnp.where(lane_k < HALO, a, jnp.where(lane_k < HALO + cols, mine, b))
            t1 = jnp.where(lane_k < cols + 2 * HALO - LANES, b, 0.0)
            return jnp.concatenate([t0, t1], axis=1).astype(BF)

        def expand(i, c):
            x0, x1 = block(2 * i), block(2 * i + 1)
            for m in range(4):
                e = e8[8 * step * m : 8 * step * (m + 1)]
                y0 = mm(e, x0).reshape(step, 8, 256)
                y1 = mm(e, x1).reshape(step, 8, 256)
                v = jnp.concatenate([y0, y1], axis=1).astype(BF)
                spec[step * m : step * (m + 1), pl.ds(pl.multiple_of(16 * i, 16), 16), :] = v
            return c

        lax.fori_loop(0, next_ // 2, expand, 0)

        def columns(g, c):
            for q in range(8):
                b = 8 * g + q
                mid[b] = mm(spec[b][:, :ku], tt[b]).astype(BF)
            return c

        lax.fori_loop(0, bands // 8, columns, 0)

        def along(g, c):
            for q in range(5):
                t = 5 * g + q
                v = jnp.concatenate([mid[t], mid[third + t], mid[2 * third + t]], axis=0)
                v = mm(rr[t][:, : 3 * ext_r], v)
                for k in range(3):
                    fin[third * k + t] = v[rows * k : rows * (k + 1)]
            return c

        lax.fori_loop(0, third // 5, along, 0)

        def project(i, c):
            v = fin[:bands, pl.ds(pl.multiple_of(8 * i, 8), 8), :].reshape(bands * 8, LANES).astype(BF)
            vec[n + 1, i] = mm(p8[...], v) + ridge[...] * vec[n, i]
            return c

        lax.fori_loop(0, nblk, project, 0)
        return carry

    lax.fori_loop(0, 2, normal, 0)

    def products(i, sums):
        a, b, c = vec[0, i], vec[1, i], vec[2, i]
        parts = [a * a, a * b, b * b, a * c, b * c]
        return tuple(s + jnp.sum(v.reshape(comps, 8, LANES), axis=0) for s, v in zip(sums, parts))

    zero = jnp.zeros((8, LANES), F32)
    sums = lax.fori_loop(0, nblk, products, (zero,) * 5)
    total = jnp.concatenate([jnp.sum(v, axis=0, keepdims=True) for v in sums] + [jnp.zeros((3, LANES), F32)], axis=0)
    at = 0
    for level, (group, place, count) in enumerate(((peers, j, nbd), (peers_x, x, nx), (peers_z, z, nz))):
        red_src[level] = total
        red_in[level, place] = total
        copies = []
        for d in group:
            c = remote(red_src.at[level], red_in.at[level, place], red_sem.at[0, at], red_sem.at[1, at], d)
            c.start()
            copies.append(c)
            at += 1
        for c in copies:
            c.wait()
        total = red_in[level, 0]
        for k in range(1, count):
            total = total + red_in[level, k]
    tot = jnp.sum(total, axis=1, keepdims=True)
    r00, r01, r11, r02, r12 = [tot[k : k + 1] for k in range(5)]
    alpha = r00 / r01
    new = r00 - 2.0 * alpha * r01 + alpha * alpha * r11
    gain = 1.0 + new / r00
    curve = gain * gain * r01 - alpha * gain * (r11 + r02) + alpha * alpha * r12
    alpha2 = new / curve

    def finish(i, carry):
        a, b, c = vec[0, i], vec[1, i], vec[2, i]
        xs = alpha * a + alpha2 * (gain * a - alpha * b)
        rs = (a - alpha * b) - alpha2 * (gain * b - alpha * c)
        sl = pl.ds(pl.multiple_of(8 * i, 8), 8)
        out_x[:, sl, :] = xs.reshape(comps, 8, LANES)[:, :, :cols]
        out_r[:, sl, :] = rs.reshape(comps, 8, LANES)[:, :, :cols]
        return carry

    lax.fori_loop(0, nblk, finish, 0)


def features(t):
    wide = jnp.pad(t, ((0, 0), (0, 0), (TAPS - 1, TAPS - 1)))
    auto = sum(t[:, :, m : m + 1] * wide[:, :, m : m + 2 * TAPS - 1] for m in range(TAPS))
    tail = jnp.pad(t[:, :, RAD + 1 :], ((0, 0), (0, 0), (0, RAD)))
    cut = 0.0
    for m in range(RAD):
        v = tail[:, :, m : m + RAD]
        cut = cut + v[:, :, :, None] * v[:, :, None, :]
    cut = cut.reshape(t.shape[0], t.shape[1], RAD * RAD)
    auto = jnp.pad(auto, ((0, 0), (0, 0), (0, SLOT - 2 * TAPS + 1)))
    both = jnp.concatenate([auto, cut], axis=2)
    return jnp.pad(both, ((0, 0), (0, -t.shape[1] % 16), (0, 256 - both.shape[2]))).astype(BF)


def local(height, width, sizes, observed, row_taps, col_taps, spectral_basis, ridge_weights):
    own, rows, _ = observed.shape
    bands, comps = spectral_basis.shape
    ny, nc, nx, nz = sizes
    nbd = ny * nc
    cols = width // nbd
    full = -(-width // LANES) * LANES
    ext_r = rows + 2 * HALO
    ck, nblk = comps * 8, rows // 8
    third = -(-bands // 24) * 8
    ku = -(-(cols + 2 * HALO) // 16) * 16
    kw = -(-(nc * cols + 2 * RAD) // 16) * 16

    obs = jnp.pad(observed, ((0, 0), (0, 0), (0, full - width)))
    edges = jnp.stack([obs[:, :RAD].reshape(own * RAD, full), obs[:, rows - RAD :].reshape(own * RAD, full)])
    feats = features(jnp.stack([col_taps, col_taps[:, ::-1], row_taps, row_taps[:, ::-1]]))
    taps = jnp.pad(jnp.stack([col_taps, row_taps[:, ::-1]], axis=1), ((0, 0), (0, 6), (0, LANES - TAPS)))
    basis_t = jnp.pad(spectral_basis.T, ((0, 0), (0, 256 - bands)))
    ridge = jnp.broadcast_to(jnp.repeat(ridge_weights, 8)[:, None], (ck, LANES))

    def vm(*shape, dtype=BF):
        return pltpu.VMEM(shape, dtype)

    dma = pltpu.SemaphoreType.DMA
    scratch = [
        vm(2, own * RAD, full),
        vm(nbd, 2, feats.shape[1], 256),
        vm(2, bands, 256, dtype=F32),
        vm(own // 4, 4 * rows, 256),
        vm(own, kw, 256),
        vm(ny, own, rows, 256, dtype=F32),
        vm(ny, nblk, ck, LANES, dtype=F32),
        vm(ny, nblk, ck, LANES),
        vm(ny, nblk, ck, LANES),
        vm(ny - 1, nblk, ck, LANES),
        vm(ny - 1, nblk, ck, LANES),
        vm(bands, ku, LANES),
        vm(third, 3 * rows, 256),
        vm(bands * 8, ck),
        vm(ck, bands * 8),
        vm(ck, 256),
        vm(bands, ext_r, 256),
        vm(3 * third, ext_r, LANES),
        vm(3 * third, rows, LANES, dtype=F32),
        vm(bands // 8, LANES, LANES, dtype=F32),
        vm(2, ext_r // 8, ck, LANES),
        vm(2, 2, 2, ck, LANES),
        vm(2, 2, 2, ck, LANES),
        vm(3, nblk, ck, LANES, dtype=F32),
        vm(3, 8, LANES, dtype=F32),
        vm(3, max(nbd, nx, nz), 8, LANES, dtype=F32),
        dma((4,)),
        dma((2, nbd - 1, 2)),
        dma((2, ny)),
        dma((2, ny - 1)),
        dma((2, 4)),
        dma((2, 4)),
        dma((2, nbd + nx + nz - 3)),
    ]
    shape = jax.ShapeDtypeStruct((comps, rows, cols), F32)
    vmem = pl.BlockSpec(memory_space=pltpu.VMEM)
    return pl.pallas_call(
        functools.partial(kernel, (cols, sizes)),
        out_shape=(shape, shape),
        in_specs=[vmem] * 7,
        out_specs=(vmem, vmem),
        scratch_shapes=scratch,
        compiler_params=pltpu.CompilerParams(
            collective_id=0, has_side_effects=True, vmem_limit_bytes=67043328
        ),
    )(obs, edges, feats, taps, spectral_basis, basis_t, ridge)


def solution(mesh):
    sizes = (4, 2, 4, 4)
    split = Mesh(mesh.devices.reshape(sizes), AXES)
    placed = (P(BAND, ROW, None), P(BAND, None), P(BAND, None), P(), P())

    def whole(observed, row_taps, col_taps, spectral_basis, ridge_weights):
        _, height, width = observed.shape
        return jax.shard_map(
            functools.partial(local, height, width, sizes),
            mesh=split,
            in_specs=placed,
            out_specs=(P(None, ROW, BAND), P(None, ROW, BAND)),
            check_vma=False,
        )(observed, row_taps, col_taps, spectral_basis, ridge_weights)

    return whole
```

```python
import functools

import jax
import jax.numpy as jnp
from jax import lax
from jax.experimental import pallas as pl
from jax.experimental.pallas import tpu as pltpu
from jax.sharding import Mesh
from jax.sharding import PartitionSpec as P

AXES = ("band_0", "band_1", "row_0", "row_1")
BAND = ("band_0", "band_1")
ROW = ("row_0", "row_1")
TAPS = 25
RAD = 12
HALO = 24
LANES = 128
SLOT = 64
BF = jnp.bfloat16
F32 = jnp.float32


def iota(shape, dim):
    return lax.broadcasted_iota(jnp.int32, shape, dim)


def mm(a, b):
    return lax.dot_general(a, b, (((1,), (0,)), ((), ())), preferred_element_type=F32)


def onehot(mask):
    return jnp.where(mask, 1.0, 0.0)


def staircase(line, rows, shift):
    step = pltpu.roll(jnp.broadcast_to(line, (8, LANES)), 0, 1, stride=1, stride_axis=0)
    tiles = []
    for g in range(rows // 8):
        turn = (shift + 8 * g) % LANES
        tiles.append(pltpu.roll(step, turn, 1) if turn else step)
    return jnp.concatenate(tiles, axis=0)


def kernel(
    dims, obs, edges, feats, taps, basis, basis_t, ridge,
    out_x, out_r,
    edge_in, line_in, lines, rows_adj, cols_adj, zed, keep, out_a, in_a, out_b, in_b,
    tt, rr, e8, p8, p8_own, spec, mid, fin, work, ext, pack, pack_in, vec, red_src, red_in,
    edge_sem, line_sem, a_sem, b_sem, row_sem, col_sem, red_sem,
):
    cols, sizes = dims
    ny, nc, nx, nz = sizes
    nbd, nrow = ny * nc, nx * nz
    y, core = lax.axis_index("band_0"), lax.axis_index("band_1")
    x, z = lax.axis_index("row_0"), lax.axis_index("row_1")
    j, i_row = y * nc + core, x * nz + z
    own, rows, full = obs.shape
    bands, comps = basis.shape
    ext_r = rows + 2 * HALO
    nblk, next_ = rows // 8, ext_r // 8
    ck = comps * 8
    ku = tt.shape[1]
    first, last = j == 0, j == nbd - 1
    top_dev, low_dev = i_row == 0, i_row == nrow - 1

    def at_band(jj):
        return (jj // nc, lax.rem(jj, nc), x, z)

    def at_row(ii):
        return (y, core, ii // nz, lax.rem(ii, nz))

    up = at_row(lax.rem(i_row + nrow - 1, nrow))
    down = at_row(lax.rem(i_row + 1, nrow))
    left = at_band(lax.rem(j + nbd - 1, nbd))
    right = at_band(lax.rem(j + 1, nbd))
    partner = (y, 1 - core, x, z)
    peers = [at_band(lax.rem(j + s, nbd)) for s in range(1, nbd)]
    peers_r = [at_row(lax.rem(i_row + s, nrow)) for s in range(1, nrow)]

    barrier = pltpu.get_barrier_semaphore()
    everyone = peers + peers_r
    for d in everyone:
        pl.semaphore_signal(barrier, inc=1, device_id=d, device_id_type=pl.DeviceIdType.MESH)
    pl.semaphore_wait(barrier, len(everyone))

    def remote(src, dst, send, recv, device):
        return pltpu.make_async_remote_copy(
            src_ref=src, dst_ref=dst, send_sem=send, recv_sem=recv,
            device_id=device, device_id_type=pl.DeviceIdType.MESH,
        )

    to_up = remote(edges.at[0], edge_in.at[1], edge_sem.at[0], edge_sem.at[2], up)
    to_down = remote(edges.at[1], edge_in.at[0], edge_sem.at[1], edge_sem.at[3], down)
    to_up.start()
    to_down.start()

    line_copies = []
    row_kind = jnp.where(low_dev, 3, 2)
    for s in range(1, nbd):
        dest = lax.rem(j + s, nbd)
        for k, kind in enumerate((jnp.where(dest == nbd - 1, 1, 0), row_kind)):
            c = remote(
                feats.at[kind], line_in.at[j, k], line_sem.at[0, s - 1, k], line_sem.at[1, s - 1, k], at_band(dest)
            )
            c.start()
            line_copies.append(c)
    line_in[j, 0] = feats[jnp.where(last, 1, 0)]
    line_in[j, 1] = feats[row_kind]

    r, l = iota((rows, LANES), 0), iota((rows, LANES), 1)

    def own_rows(g, carry):
        for q in range(4):
            line = taps[4 * g + q][1:2]
            d = l - rows * q + RAD - r
            m = (d >= 0) & (d < TAPS) & (l >= rows * q) & (l < rows * (q + 1))
            mine = jnp.where(m, staircase(line, rows, rows * q - RAD), 0.0)
            k = l - RAD * q
            d = k - r
            m = (d >= 0) & (d < TAPS) & (k >= 0) & (k < RAD)
            above = jnp.where(m, staircase(line, rows, RAD * q), 0.0)
            k = l - 4 * RAD - RAD * q
            d = k + rows + RAD - r
            m = (d >= 0) & (d < TAPS) & (k >= 0) & (k < RAD)
            below = jnp.where(m, staircase(line, rows, 4 * RAD + RAD * q - RAD - rows), 0.0)
            rows_adj[g, rows * q : rows * (q + 1), :LANES] = mine.astype(BF)
            rows_adj[g, rows * q : rows * (q + 1), LANES:] = (above + below).astype(BF)
        return carry

    lax.fori_loop(0, own // 4, own_rows, 0)

    kw = cols_adj.shape[1]
    w, o = iota((kw, LANES), 0), iota((kw, LANES), 1)

    def own_cols(b, carry):
        line = taps[b][0:1]
        for k in range(2):
            d = w - o - cols * k
            m = (d >= 0) & (d < TAPS) & (o < cols)
            t = jnp.where(m, staircase(line, kw, -HALO - cols * k), 0.0)
            cols_adj[b, :, LANES * k : LANES * (k + 1)] = t.astype(BF)
        return carry

    lax.fori_loop(0, own, own_cols, 0)

    spread = onehot(iota((comps, ck), 0) == (iota((comps, ck), 1) >> 3)).astype(BF)
    wide = mm(basis[...], spread)
    step = bands // 4
    er, el = iota((8 * step, ck), 0), iota((8 * step, ck), 1)
    for c in range(4):
        v = jnp.broadcast_to(wide[step * c : step * (c + 1)][:, None, :], (step, 8, ck)).reshape(8 * step, ck)
        e8[8 * step * c : 8 * step * (c + 1)] = jnp.where((er & 7) == (el & 7), v, 0.0).astype(BF)
    tall = onehot(iota((ck, comps), 1) == (iota((ck, comps), 0) >> 3)).astype(BF)
    tall = mm(tall, basis_t[...]).astype(BF)
    br, bl = iota((256, 256), 0), iota((256, 256), 1)
    same = (br & 7) == (bl & 7)

    def widen(start):
        return jnp.where(same, mm(tall, onehot(br == start + (bl >> 3)).astype(BF)), 0.0).astype(BF)

    for c in range(bands // 32):
        p8[:, 256 * c : 256 * (c + 1)] = widen(32 * c)
    p8_own[...] = widen(own * j)

    for c in line_copies:
        c.wait()
    for k in range(2):
        for jj in range(nbd):
            lines[k, own * jj : own * (jj + 1)] = line_in[jj, k][:own].astype(F32)
    groups = bands // 8
    wide_n = 16 * LANES

    def shifted(depth, hit, edge_hit):
        f, n = iota((depth, wide_n), 0), iota((depth, wide_n), 1)
        s = onehot(f == hit(n))
        if edge_hit is not None:
            s = s - onehot(f == edge_hit(n))
        return s.astype(BF)

    def unfold(k, depth, sel):
        res = mm(lines[k, :, :depth].astype(BF), sel)
        for t in range(16):
            work[:, 8 * t : 8 * (t + 1), :] = res[:, LANES * t : LANES * (t + 1)].reshape(groups, 8, LANES)

    def tt_pair(p, carry, depth):
        def hit(n):
            a, b = 16 * p + (n >> 7), n & 127
            return jnp.where((b < cols) & (a < cols + 2 * HALO) & (a - b <= 2 * HALO), a - b, -1)

        def edge_hit(n):
            a, b = 16 * p + (n >> 7) - HALO, n & 127
            a, b = jnp.where(last, cols - 1 - a, a), jnp.where(last, cols - 1 - b, b)
            ok = (first | last) & (a >= 0) & (a < RAD) & (b >= 0) & (b < RAD)
            return jnp.where(ok, SLOT + RAD * a + b, -1)

        unfold(0, depth, shifted(depth, hit, edge_hit if depth > SLOT else None))

        def place(g, c):
            for s in range(8):
                v = work[g, pl.ds(s, 16, stride=8), :]
                tt[8 * g + s, pl.ds(pl.multiple_of(16 * p, 16), 16), :] = v.astype(BF)
            return c

        lax.fori_loop(0, groups, place, 0)
        return carry

    third = rr.shape[0]
    lane16 = iota((16, LANES), 1)

    def rr_pair(p, carry):
        def hit(n):
            a, b = 16 * p + (n >> 7), n & 127
            return jnp.where((b < ext_r) & (b >= a) & (b - a <= 2 * HALO), b - a, -1)

        def edge_hit(n):
            a, b = 16 * p + (n >> 7), (n & 127) - HALO
            a, b = jnp.where(low_dev, rows - 1 - a, a), jnp.where(low_dev, rows - 1 - b, b)
            ok = (top_dev | low_dev) & (a >= 0) & (a < RAD) & (b >= 0) & (b < RAD)
            return jnp.where(ok, SLOT + RAD * a + b, -1)

        unfold(1, 256, shifted(256, hit, edge_hit))
        for q in range(3):
            lo = ext_r * q

            def place(g, c):
                for s in range(8):
                    v = work[g, pl.ds(s, 16, stride=8), :]
                    if lo % LANES:
                        v = pltpu.roll(v, lo % LANES, 1)
                    t0 = v if lo + ext_r <= LANES else jnp.where(lane16 >= lo, v, 0.0)
                    t1 = v if lo >= LANES else jnp.where(lane16 < lo + ext_r - LANES, v, 0.0)
                    at = (8 * g + s - third * q, pl.ds(pl.multiple_of(rows * q + 16 * p, 16), 16))
                    rr[at + (slice(0, LANES),)] = t0.astype(BF)
                    rr[at + (slice(LANES, 2 * LANES),)] = t1.astype(BF)
                return c

            lax.fori_loop(third * q // 8, min(third * (q + 1), bands) // 8, place, 0)
        return carry

    lax.fori_loop(0, rows // 16, rr_pair, 0)

    to_up.wait()
    to_down.wait()
    above_ok, below_ok = i_row > 0, i_row < nrow - 1

    def adjoint(g, carry):
        e = pl.ds(pl.multiple_of(4 * RAD * g, 16), 4 * RAD)
        above = edge_in[0, e]
        below = edge_in[1, e]
        mine = obs[pl.ds(4 * g, 4)].reshape(4 * rows, full)
        above = jnp.where(above_ok, above, jnp.zeros_like(above))
        below = jnp.where(below_ok, below, jnp.zeros_like(below))
        v = mm(rows_adj[g][:, : 4 * rows + 8 * RAD], jnp.concatenate([mine, above, below], axis=0))
        wins = []
        for k in range(ny):
            start = nc * cols * k - RAD
            wins.append(pltpu.roll(v, (full - start) % full, 1)[:, :256].astype(BF))
        for q in range(4):
            u = jnp.concatenate([t[rows * q : rows * (q + 1)] for t in wins], axis=0)
            u = mm(u[:, :kw], cols_adj[4 * g + q])
            for k in range(ny):
                zed[k, 4 * g + q] = u[rows * k : rows * (k + 1)]
        return carry

    lax.fori_loop(0, own // 4, adjoint, 0)

    offsets = [s for s in (2, 1, 3, 0) if s < ny]
    a_copies, b_copies = [], []

    def merge(idx):
        a_copies[idx].wait()
        done = idx == len(offsets) - 1

        def add(i, carry):
            v = keep[idx, i] + in_a[idx, i].astype(F32)
            if done:
                vec[0, i] = v
            else:
                out_b[idx, i] = v.astype(BF)
            return carry

        lax.fori_loop(0, nblk, add, 0)
        if not done:
            dest = (lax.rem(y + offsets[idx], ny), core, x, z)
            c = remote(out_b.at[idx], in_b.at[idx], b_sem.at[0, idx], b_sem.at[1, idx], dest)
            c.start()
            b_copies.append(c)

    for idx, off in enumerate(offsets):
        k = lax.rem(y + off, ny)

        def project(i, carry):
            v = zed[k, :, pl.ds(pl.multiple_of(8 * i, 8), 8), :].reshape(own * 8, 256).astype(BF)
            v = mm(p8_own[:, : own * 8], v)
            lo, hi = v[:, :LANES], v[:, LANES:]
            keep[idx, i] = jnp.where(core == 0, lo, hi)
            out_a[idx, i] = jnp.where(core == 0, hi, lo).astype(BF)
            return carry

        lax.fori_loop(0, nblk, project, 0)
        c = remote(out_a.at[idx], in_a.at[idx], a_sem.at[0, idx], a_sem.at[1, idx], partner)
        c.start()
        a_copies.append(c)
        if idx:
            merge(idx - 1)
    merge(len(offsets) - 1)
    lax.fori_loop(0, ku // 16, functools.partial(tt_pair, depth=SLOT), 0)

    @pl.when(first | last)
    def _():
        p0 = jnp.where(first, HALO // 16, (cols + RAD - 1) // 16)
        lax.fori_loop(p0, p0 + 2, functools.partial(tt_pair, depth=256), 0)

    mid[pl.ds(bands, mid.shape[0] - bands)] = jnp.zeros((mid.shape[0] - bands, ext_r, LANES), BF)
    for idx, c in enumerate(b_copies):
        c.wait()

        def collect(i, carry):
            vec[0, i] = vec[0, i] + in_b[idx, i].astype(F32)
            return carry

        lax.fori_loop(0, nblk, collect, 0)

    chunk = ck // 4
    per = next_ // 2
    lane_c = iota((chunk, LANES), 1)
    lane_k = iota((ck, LANES), 1)

    def normal(n, carry):
        def stage(i, c):
            ext[n, 3 + i] = vec[n, i].astype(BF)
            return c

        lax.fori_loop(0, nblk, stage, 0)
        r_up = remote(ext.at[n, pl.ds(3, 3)], ext.at[n, pl.ds(3 + nblk, 3)], row_sem.at[n, 0], row_sem.at[n, 2], up)
        r_down = remote(ext.at[n, pl.ds(nblk, 3)], ext.at[n, pl.ds(0, 3)], row_sem.at[n, 1], row_sem.at[n, 3], down)
        r_up.start()
        r_down.start()
        r_up.wait()
        r_down.wait()

        def packing(c, cc):
            t, part = c // 4, lax.rem(c, 4)
            sl = pl.ds(pl.multiple_of(chunk * part, chunk), chunk)
            a = jnp.zeros((chunk, LANES), F32)
            b = a
            for g in range(per):
                v = ext[n, per * t + g, sl, :].astype(F32)
                m = (lane_c >= HALO * g) & (lane_c < HALO * (g + 1))
                a = jnp.where(m, pltpu.roll(v, HALO * g, 1) if g else v, a)
                b = jnp.where(m, pltpu.roll(v, (HALO * g - cols + HALO) % LANES, 1), b)
            pack[n, 0, t, sl, :] = a.astype(BF)
            pack[n, 1, t, sl, :] = b.astype(BF)
            return cc

        lax.fori_loop(0, 8, packing, 0)
        c_left = remote(pack.at[n, 0], pack_in.at[n, 1], col_sem.at[n, 0], col_sem.at[n, 2], left)
        c_right = remote(pack.at[n, 1], pack_in.at[n, 0], col_sem.at[n, 1], col_sem.at[n, 3], right)
        c_left.start()
        c_right.start()
        c_left.wait()
        c_right.wait()

        def block(blk):
            t, g = blk // per, blk % per
            mine = pltpu.roll(ext[n, blk].astype(F32), HALO, 1)
            a = pltpu.roll(pack_in[n, 0, t].astype(F32), (LANES - HALO * g) % LANES, 1)
            b = pltpu.roll(pack_in[n, 1, t].astype(F32), (cols + HALO - HALO * g) % LANES, 1)
            inside = jnp.logical_not((top_dev if blk < 3 else False) | (low_dev if blk >= 3 + nblk else False))
            a_ok = inside & jnp.logical_not(first)
            b_ok = inside & jnp.logical_not(last)
            a = jnp.where(a_ok, a, 0.0)
            b = jnp.where(b_ok, b, 0.0)
            mine = jnp.where(inside, mine, 0.0)
            t0 = jnp.where(lane_k < HALO, a, jnp.where(lane_k < HALO + cols, mine, b))
            t1 = jnp.where(lane_k < cols + 2 * HALO - LANES, b, 0.0)
            return jnp.concatenate([t0, t1], axis=1).astype(BF)

        def expand(i, c):
            x0, x1 = block(2 * i), block(2 * i + 1)
            for m in range(4):
                e = e8[8 * step * m : 8 * step * (m + 1)]
                y0 = mm(e, x0).reshape(step, 8, 256)
                y1 = mm(e, x1).reshape(step, 8, 256)
                v = jnp.concatenate([y0, y1], axis=1).astype(BF)
                spec[step * m : step * (m + 1), 16 * i : 16 * (i + 1), :] = v
            return c

        for i in range(next_ // 2):
            expand(i, 0)

        def columns(g, c):
            for q in range(56):
                b = 56 * g + q
                mid[b] = mm(spec[b][:, :ku], tt[b]).astype(BF)
            return c

        lax.fori_loop(0, bands // 56, columns, 0)

        def along(g, c):
            for q in range(40):
                t = 40 * g + q
                v = jnp.concatenate([mid[t], mid[third + t], mid[2 * third + t]], axis=0)
                v = mm(rr[t][:, : 3 * ext_r], v)
                for k in range(3):
                    fin[third * k + t] = v[rows * k : rows * (k + 1)]
            return c

        lax.fori_loop(0, third // 40, along, 0)

        def project(i, c):
            v = fin[:bands, pl.ds(pl.multiple_of(8 * i, 8), 8), :].reshape(bands * 8, LANES).astype(BF)
            vec[n + 1, i] = mm(p8[...], v) + ridge[...] * vec[n, i]
            return c

        lax.fori_loop(0, nblk, project, 0)
        return carry

    lax.fori_loop(0, 2, normal, 0)

    def products(i, sums):
        a, b, c = vec[0, i], vec[1, i], vec[2, i]
        parts = [a * a, a * b, b * b, a * c, b * c]
        return tuple(s + jnp.sum(v.reshape(comps, 8, LANES), axis=0) for s, v in zip(sums, parts))

    zero = jnp.zeros((8, LANES), F32)
    sums = lax.fori_loop(0, nblk, products, (zero,) * 5)
    total = jnp.concatenate([jnp.sum(v, axis=0, keepdims=True) for v in sums] + [jnp.zeros((3, LANES), F32)], axis=0)
    at = 0
    for level, (group, place, count) in enumerate(((peers, j, nbd), (peers_r, i_row, nrow))):
        red_src[level] = total
        red_in[level, place] = total
        copies = []
        for d in group:
            c = remote(red_src.at[level], red_in.at[level, place], red_sem.at[0, at], red_sem.at[1, at], d)
            c.start()
            copies.append(c)
            at += 1
        for c in copies:
            c.wait()
        total = red_in[level, 0]
        for k in range(1, count):
            total = total + red_in[level, k]
    tot = jnp.sum(total, axis=1, keepdims=True)
    r00, r01, r11, r02, r12 = [tot[k : k + 1] for k in range(5)]
    alpha = r00 / r01
    new = r00 - 2.0 * alpha * r01 + alpha * alpha * r11
    gain = 1.0 + new / r00
    curve = gain * gain * r01 - alpha * gain * (r11 + r02) + alpha * alpha * r12
    alpha2 = new / curve

    def finish(i, carry):
        a, b, c = vec[0, i], vec[1, i], vec[2, i]
        xs = alpha * a + alpha2 * (gain * a - alpha * b)
        rs = (a - alpha * b) - alpha2 * (gain * b - alpha * c)
        sl = pl.ds(pl.multiple_of(8 * i, 8), 8)
        out_x[:, sl, :] = xs.reshape(comps, 8, LANES)[:, :, :cols]
        out_r[:, sl, :] = rs.reshape(comps, 8, LANES)[:, :, :cols]
        return carry

    lax.fori_loop(0, nblk, finish, 0)


def features(t):
    wide = jnp.pad(t, ((0, 0), (0, 0), (TAPS - 1, TAPS - 1)))
    auto = sum(t[:, :, m : m + 1] * wide[:, :, m : m + 2 * TAPS - 1] for m in range(TAPS))
    tail = jnp.pad(t[:, :, RAD + 1 :], ((0, 0), (0, 0), (0, RAD)))
    cut = 0.0
    for m in range(RAD):
        v = tail[:, :, m : m + RAD]
        cut = cut + v[:, :, :, None] * v[:, :, None, :]
    cut = cut.reshape(t.shape[0], t.shape[1], RAD * RAD)
    auto = jnp.pad(auto, ((0, 0), (0, 0), (0, SLOT - 2 * TAPS + 1)))
    both = jnp.concatenate([auto, cut], axis=2)
    return jnp.pad(both, ((0, 0), (0, -t.shape[1] % 16), (0, 256 - both.shape[2]))).astype(BF)


def local(height, width, sizes, observed, row_taps, col_taps, spectral_basis, ridge_weights):
    own, rows, _ = observed.shape
    bands, comps = spectral_basis.shape
    ny, nc, nx, nz = sizes
    nbd = ny * nc
    cols = width // nbd
    full = -(-width // LANES) * LANES
    ext_r = rows + 2 * HALO
    ck, nblk = comps * 8, rows // 8
    third = -(-bands // 24) * 8
    ku = -(-(cols + 2 * HALO) // 16) * 16
    kw = -(-(nc * cols + 2 * RAD) // 16) * 16

    obs = jnp.pad(observed, ((0, 0), (0, 0), (0, full - width)))
    edges = jnp.stack([obs[:, :RAD].reshape(own * RAD, full), obs[:, rows - RAD :].reshape(own * RAD, full)])
    feats = features(jnp.stack([col_taps, col_taps[:, ::-1], row_taps, row_taps[:, ::-1]]))
    taps = jnp.pad(jnp.stack([col_taps, row_taps[:, ::-1]], axis=1), ((0, 0), (0, 6), (0, LANES - TAPS)))
    basis_t = jnp.pad(spectral_basis.T, ((0, 0), (0, 256 - bands)))
    ridge = jnp.broadcast_to(jnp.repeat(ridge_weights, 8)[:, None], (ck, LANES))

    def vm(*shape, dtype=BF):
        return pltpu.VMEM(shape, dtype)

    dma = pltpu.SemaphoreType.DMA
    scratch = [
        vm(2, own * RAD, full),
        vm(nbd, 2, feats.shape[1], 256),
        vm(2, bands, 256, dtype=F32),
        vm(own // 4, 4 * rows, 256),
        vm(own, kw, 256),
        vm(ny, own, rows, 256, dtype=F32),
        vm(ny, nblk, ck, LANES, dtype=F32),
        vm(ny, nblk, ck, LANES),
        vm(ny, nblk, ck, LANES),
        vm(ny - 1, nblk, ck, LANES),
        vm(ny - 1, nblk, ck, LANES),
        vm(bands, ku, LANES),
        vm(third, 3 * rows, 256),
        vm(bands * 8, ck),
        vm(ck, bands * 8),
        vm(ck, 256),
        vm(bands, ext_r, 256),
        vm(3 * third, ext_r, LANES),
        vm(3 * third, rows, LANES, dtype=F32),
        vm(bands // 8, LANES, LANES, dtype=F32),
        vm(2, ext_r // 8, ck, LANES),
        vm(2, 2, 2, ck, LANES),
        vm(2, 2, 2, ck, LANES),
        vm(3, nblk, ck, LANES, dtype=F32),
        vm(2, 8, LANES, dtype=F32),
        vm(2, max(nbd, nx * nz), 8, LANES, dtype=F32),
        dma((4,)),
        dma((2, nbd - 1, 2)),
        dma((2, ny)),
        dma((2, ny - 1)),
        dma((2, 4)),
        dma((2, 4)),
        dma((2, nbd + nx * nz - 2)),
    ]
    shape = jax.ShapeDtypeStruct((comps, rows, cols), F32)
    vmem = pl.BlockSpec(memory_space=pltpu.VMEM)
    return pl.pallas_call(
        functools.partial(kernel, (cols, sizes)),
        out_shape=(shape, shape),
        in_specs=[vmem] * 7,
        out_specs=(vmem, vmem),
        scratch_shapes=scratch,
        compiler_params=pltpu.CompilerParams(
            collective_id=0, has_side_effects=True, vmem_limit_bytes=67043328
        ),
    )(obs, edges, feats, taps, spectral_basis, basis_t, ridge)


def solution(mesh):
    sizes = (4, 2, 4, 4)
    split = Mesh(mesh.devices.reshape(sizes), AXES)
    placed = (P(BAND, ROW, None), P(BAND, None), P(BAND, None), P(), P())

    def whole(observed, row_taps, col_taps, spectral_basis, ridge_weights):
        _, height, width = observed.shape
        return jax.shard_map(
            functools.partial(local, height, width, sizes),
            mesh=split,
            in_specs=placed,
            out_specs=(P(None, ROW, BAND), P(None, ROW, BAND)),
            check_vma=False,
        )(observed, row_taps, col_taps, spectral_basis, ridge_weights)

    return whole
```

```python
import functools

import jax
import jax.numpy as jnp
from jax import lax
from jax.experimental import pallas as pl
from jax.experimental.pallas import tpu as pltpu
from jax.sharding import Mesh
from jax.sharding import PartitionSpec as P

AXES = ("band_0", "band_1", "row_0", "row_1")
BAND = ("band_0", "band_1")
ROW = ("row_0", "row_1")
TAPS = 25
RAD = 12
HALO = 24
LANES = 128
SLOT = 64
BF = jnp.bfloat16
F32 = jnp.float32


def iota(shape, dim):
    return lax.broadcasted_iota(jnp.int32, shape, dim)


def mm(a, b):
    return lax.dot_general(a, b, (((1,), (0,)), ((), ())), preferred_element_type=F32)


def halves(v):
    hi = v.astype(BF)
    return hi, (v - hi.astype(F32)).astype(BF)


def onehot(mask):
    return jnp.where(mask, 1.0, 0.0)


def staircase(line, rows, shift):
    step = pltpu.roll(jnp.broadcast_to(line, (8, LANES)), 0, 1, stride=1, stride_axis=0)
    tiles = []
    for g in range(rows // 8):
        turn = (shift + 8 * g) % LANES
        tiles.append(pltpu.roll(step, turn, 1) if turn else step)
    return jnp.concatenate(tiles, axis=0)


def kernel(
    dims, obs, row_taps, col_taps, basis_t, ridge_in,
    out,
    edges, feats, taps, ridge, raw, vpad, edge_in, line_in, lines, rows_adj, cols_adj, zed, keep, out_a, in_a, out_b, in_b,
    tt, rr, e8, p8, p8_own, spec, mid, fin, work, ext, pack, pack_in, vec, red_src, red_in,
    edge_sem, line_sem, a_sem, b_sem, row_sem, col_sem, red_sem,
):
    cols, sizes = dims
    ny, nc, nx, nz = sizes
    nbd, nrow = ny * nc, nx * nz
    y, core = lax.axis_index("band_0"), lax.axis_index("band_1")
    x, z = lax.axis_index("row_0"), lax.axis_index("row_1")
    j, i_row = y * nc + core, x * nz + z
    own, rows, full = obs.shape
    comps, bands = basis_t.shape
    ext_r = rows + 2 * HALO
    nblk, next_ = rows // 8, ext_r // 8
    ck = comps * 8
    ku = tt.shape[1]
    first, last = j == 0, j == nbd - 1
    top_dev, low_dev = i_row == 0, i_row == nrow - 1

    def at_band(jj):
        return (jj // nc, lax.rem(jj, nc), x, z)

    def at_row(ii):
        return (y, core, ii // nz, lax.rem(ii, nz))

    up = at_row(lax.rem(i_row + nrow - 1, nrow))
    down = at_row(lax.rem(i_row + 1, nrow))
    left = at_band(lax.rem(j + nbd - 1, nbd))
    right = at_band(lax.rem(j + 1, nbd))
    partner = (y, 1 - core, x, z)
    peers = [at_band(lax.rem(j + s, nbd)) for s in range(1, nbd)]
    peers_r = [at_row(lax.rem(i_row + s, nrow)) for s in range(1, nrow)]

    barrier = pltpu.get_barrier_semaphore()
    everyone = peers + peers_r
    for d in everyone:
        pl.semaphore_signal(barrier, inc=1, device_id=d, device_id_type=pl.DeviceIdType.MESH)

    def pack_edges(g, carry):
        sl = pl.ds(pl.multiple_of(4 * RAD * g, 16), 4 * RAD)
        v = obs[pl.ds(4 * g, 4)].astype(F32)
        for k, lo in enumerate((0, rows - RAD)):
            slab = jnp.concatenate([v[q, lo : lo + RAD] for q in range(4)], axis=0)
            edges[k, sl, :] = slab.astype(BF)
        return carry

    lax.fori_loop(0, own // 4, pack_edges, 0)
    pl.semaphore_wait(barrier, len(everyone))

    def remote(src, dst, send, recv, device):
        return pltpu.make_async_remote_copy(
            src_ref=src, dst_ref=dst, send_sem=send, recv_sem=recv,
            device_id=device, device_id_type=pl.DeviceIdType.MESH,
        )

    to_up = remote(edges.at[0], edge_in.at[1], edge_sem.at[0], edge_sem.at[2], up)
    to_down = remote(edges.at[1], edge_in.at[0], edge_sem.at[1], edge_sem.at[3], down)
    to_up.start()
    to_down.start()

    pad_own = feats.shape[1]
    raw[...] = jnp.zeros_like(raw)
    raw[:own, :TAPS] = col_taps[...]
    raw[pad_own : pad_own + own, :TAPS] = row_taps[...]
    t = raw[...]
    t_hi, t_lo = halves(t)
    gr, gp = iota((LANES, 640), 0), iota((LANES, 640), 1)
    g1 = (gp * 5243) >> 17
    g1, g2 = onehot(gr == g1).astype(BF), onehot(gr == gp - TAPS * g1).astype(BF)
    prod = (mm(t_hi, g1) + mm(t_lo, g1)) * (mm(t_hi, g2) + mm(t_lo, g2))
    p_hi, p_lo = halves(prod)
    pp, f = iota((640, 256), 0), iota((640, 256), 1)
    m1 = (pp * 5243) >> 17
    m2 = pp - TAPS * m1
    fe = f - SLOT
    fx = (fe * 5462) >> 16
    fy = fe - RAD * fx
    lag = (f < 2 * TAPS - 1) & (m2 - m1 + TAPS - 1 == f)
    edge = (fe >= 0) & (fe < RAD * RAD)
    for k, cut in enumerate((
        (m1 - fx == m2 - fy) & (m1 - fx > RAD) & (m1 < TAPS),
        (m1 + fx == m2 + fy) & (m1 + fx < RAD),
    )):
        sel = onehot(lag | (edge & cut)).astype(BF)
        v = (mm(p_hi, sel) + mm(p_lo, sel)).astype(BF)
        feats[k] = v[:pad_own]
        feats[2 + k] = v[pad_own:]
    flip = onehot(iota((LANES, LANES), 0) + iota((LANES, LANES), 1) == TAPS - 1).astype(BF)
    taps[:, 0:1, :] = t[:own].reshape(own, 1, LANES)
    taps[:, 1:2, :] = mm(t_hi, flip)[pad_own : pad_own + own].reshape(own, 1, LANES)

    line_copies = []
    row_kind = jnp.where(low_dev, 3, 2)
    for s in range(1, nbd):
        dest = lax.rem(j + s, nbd)
        for k, kind in enumerate((jnp.where(dest == nbd - 1, 1, 0), row_kind)):
            c = remote(
                feats.at[kind], line_in.at[j, k], line_sem.at[0, s - 1, k], line_sem.at[1, s - 1, k], at_band(dest)
            )
            c.start()
            line_copies.append(c)
    line_in[j, 0] = feats[jnp.where(last, 1, 0)]
    line_in[j, 1] = feats[row_kind]

    r, l = iota((rows, LANES), 0), iota((rows, LANES), 1)

    def own_rows(g, carry):
        for q in range(4):
            line = taps[4 * g + q][1:2]
            d = l - rows * q + RAD - r
            m = (d >= 0) & (d < TAPS) & (l >= rows * q) & (l < rows * (q + 1))
            mine = jnp.where(m, staircase(line, rows, rows * q - RAD), 0.0)
            k = l - RAD * q
            d = k - r
            m = (d >= 0) & (d < TAPS) & (k >= 0) & (k < RAD)
            above = jnp.where(m, staircase(line, rows, RAD * q), 0.0)
            k = l - 4 * RAD - RAD * q
            d = k + rows + RAD - r
            m = (d >= 0) & (d < TAPS) & (k >= 0) & (k < RAD)
            below = jnp.where(m, staircase(line, rows, 4 * RAD + RAD * q - RAD - rows), 0.0)
            rows_adj[g, rows * q : rows * (q + 1), :LANES] = mine.astype(BF)
            rows_adj[g, rows * q : rows * (q + 1), LANES:] = (above + below).astype(BF)
        return carry

    lax.fori_loop(0, own // 4, own_rows, 0)

    kw = cols_adj.shape[1]
    w, o = iota((kw, LANES), 0), iota((kw, LANES), 1)

    def own_cols(b, carry):
        line = taps[b][0:1]
        for k in range(2):
            d = w - o - cols * k
            m = (d >= 0) & (d < TAPS) & (o < cols)
            t = jnp.where(m, staircase(line, kw, -HALO - cols * k), 0.0)
            cols_adj[b, :, LANES * k : LANES * (k + 1)] = t.astype(BF)
        return carry

    lax.fori_loop(0, own, own_cols, 0)

    spread = onehot(iota((comps, ck), 0) == (iota((comps, ck), 1) >> 3)).astype(BF)
    wide = lax.dot_general(basis_t[...], spread, (((0,), (0,)), ((), ())), preferred_element_type=F32)
    step = bands // 4
    er, el = iota((8 * step, ck), 0), iota((8 * step, ck), 1)
    for c in range(4):
        v = jnp.broadcast_to(wide[step * c : step * (c + 1)][:, None, :], (step, 8, ck)).reshape(8 * step, ck)
        e8[8 * step * c : 8 * step * (c + 1)] = jnp.where((er & 7) == (el & 7), v, 0.0).astype(BF)
    tall = onehot(iota((ck, comps), 1) == (iota((ck, comps), 0) >> 3)).astype(BF)
    tall = mm(tall, basis_t[...]).astype(BF)
    br, bl = iota((bands, 256), 0), iota((bands, 256), 1)
    same = (iota((ck, 256), 0) & 7) == (iota((ck, 256), 1) & 7)
    kr, kl = iota((ck, comps), 0), iota((ck, comps), 1)
    ridge_col = jnp.sum(jnp.where(kl == (kr >> 3), ridge_in[...], 0.0), axis=1, keepdims=True)
    ridge[...] = jnp.broadcast_to(ridge_col, (ck, LANES))
    vpad[...] = jnp.zeros_like(vpad)

    def widen(start):
        return jnp.where(same, mm(tall, onehot(br == start + (bl >> 3)).astype(BF)), 0.0).astype(BF)

    for c in range(bands // 32):
        p8[:, 256 * c : 256 * (c + 1)] = widen(32 * c)
    p8_own[...] = widen(own * j)

    for c in line_copies:
        c.wait()
    for k in range(2):
        for jj in range(nbd):
            lines[k, own * jj : own * (jj + 1)] = line_in[jj, k][:own].astype(F32)
    groups = bands // 8
    wide_n = 16 * LANES

    def shifted(depth, hit, edge_hit):
        f, n = iota((depth, wide_n), 0), iota((depth, wide_n), 1)
        s = onehot(f == hit(n))
        if edge_hit is not None:
            s = s - onehot(f == edge_hit(n))
        return s.astype(BF)

    def unfold(k, depth, sel):
        res = mm(lines[k, :, :depth].astype(BF), sel)
        for t in range(16):
            work[:, 8 * t : 8 * (t + 1), :] = res[:, LANES * t : LANES * (t + 1)].reshape(groups, 8, LANES)

    def tt_pair(p, carry, depth):
        def hit(n):
            a, b = 16 * p + (n >> 7), n & 127
            return jnp.where((b < cols) & (a < cols + 2 * HALO) & (a - b <= 2 * HALO), a - b, -1)

        def edge_hit(n):
            a, b = 16 * p + (n >> 7) - HALO, n & 127
            a, b = jnp.where(last, cols - 1 - a, a), jnp.where(last, cols - 1 - b, b)
            ok = (first | last) & (a >= 0) & (a < RAD) & (b >= 0) & (b < RAD)
            return jnp.where(ok, SLOT + RAD * a + b, -1)

        unfold(0, depth, shifted(depth, hit, edge_hit if depth > SLOT else None))

        def place(g, c):
            for s in range(8):
                v = work[g, pl.ds(s, 16, stride=8), :]
                tt[8 * g + s, pl.ds(pl.multiple_of(16 * p, 16), 16), :] = v.astype(BF)
            return c

        lax.fori_loop(0, groups, place, 0)
        return carry

    third = rr.shape[0]
    lane16 = iota((16, LANES), 1)

    def rr_pair(p, carry):
        def hit(n):
            a, b = 16 * p + (n >> 7), n & 127
            return jnp.where((b < ext_r) & (b >= a) & (b - a <= 2 * HALO), b - a, -1)

        def edge_hit(n):
            a, b = 16 * p + (n >> 7), (n & 127) - HALO
            a, b = jnp.where(low_dev, rows - 1 - a, a), jnp.where(low_dev, rows - 1 - b, b)
            ok = (top_dev | low_dev) & (a >= 0) & (a < RAD) & (b >= 0) & (b < RAD)
            return jnp.where(ok, SLOT + RAD * a + b, -1)

        unfold(1, 256, shifted(256, hit, edge_hit))
        for q in range(3):
            lo = ext_r * q

            def place(g, c):
                for s in range(8):
                    v = work[g, pl.ds(s, 16, stride=8), :]
                    if lo % LANES:
                        v = pltpu.roll(v, lo % LANES, 1)
                    t0 = v if lo + ext_r <= LANES else jnp.where(lane16 >= lo, v, 0.0)
                    t1 = v if lo >= LANES else jnp.where(lane16 < lo + ext_r - LANES, v, 0.0)
                    at = (8 * g + s - third * q, pl.ds(pl.multiple_of(rows * q + 16 * p, 16), 16))
                    rr[at + (slice(0, LANES),)] = t0.astype(BF)
                    rr[at + (slice(LANES, 2 * LANES),)] = t1.astype(BF)
                return c

            lax.fori_loop(third * q // 8, min(third * (q + 1), bands) // 8, place, 0)
        return carry

    lax.fori_loop(0, rows // 16, rr_pair, 0)

    to_up.wait()
    to_down.wait()
    above_ok, below_ok = i_row > 0, i_row < nrow - 1

    def adjoint(g, carry):
        e = pl.ds(pl.multiple_of(4 * RAD * g, 16), 4 * RAD)
        above = edge_in[0, e]
        below = edge_in[1, e]
        mine = obs[pl.ds(4 * g, 4)].reshape(4 * rows, full)
        above = jnp.where(above_ok, above, jnp.zeros_like(above))
        below = jnp.where(below_ok, below, jnp.zeros_like(below))
        v = mm(rows_adj[g][:, : 4 * rows + 8 * RAD], jnp.concatenate([mine, above, below], axis=0))
        vpad[:, :full] = v
        v = vpad[...]
        wins = []
        for k in range(ny):
            start = nc * cols * k - RAD
            wins.append(pltpu.roll(v, (v.shape[1] - start) % v.shape[1], 1)[:, :256].astype(BF))
        for q in range(4):
            u = jnp.concatenate([t[rows * q : rows * (q + 1)] for t in wins], axis=0)
            u = mm(u[:, :kw], cols_adj[4 * g + q])
            for k in range(ny):
                zed[k, 4 * g + q] = u[rows * k : rows * (k + 1)]
        return carry

    lax.fori_loop(0, own // 4, adjoint, 0)

    offsets = [s for s in (2, 1, 3, 0) if s < ny]
    a_copies, b_copies = [], []

    def merge(idx):
        a_copies[idx].wait()
        done = idx == len(offsets) - 1

        def add(i, carry):
            v = keep[idx, i] + in_a[idx, i].astype(F32)
            if done:
                vec[0, i] = v
            else:
                out_b[idx, i] = v.astype(BF)
            return carry

        lax.fori_loop(0, nblk, add, 0)
        if not done:
            dest = (lax.rem(y + offsets[idx], ny), core, x, z)
            c = remote(out_b.at[idx], in_b.at[idx], b_sem.at[0, idx], b_sem.at[1, idx], dest)
            c.start()
            b_copies.append(c)

    for idx, off in enumerate(offsets):
        k = lax.rem(y + off, ny)

        def project(i, carry):
            v = zed[k, :, pl.ds(pl.multiple_of(8 * i, 8), 8), :].reshape(own * 8, 256).astype(BF)
            v = mm(p8_own[:, : own * 8], v)
            lo, hi = v[:, :LANES], v[:, LANES:]
            keep[idx, i] = jnp.where(core == 0, lo, hi)
            out_a[idx, i] = jnp.where(core == 0, hi, lo).astype(BF)
            return carry

        lax.fori_loop(0, nblk, project, 0)
        c = remote(out_a.at[idx], in_a.at[idx], a_sem.at[0, idx], a_sem.at[1, idx], partner)
        c.start()
        a_copies.append(c)
        if idx:
            merge(idx - 1)
    merge(len(offsets) - 1)
    lax.fori_loop(0, ku // 16, functools.partial(tt_pair, depth=SLOT), 0)

    @pl.when(first | last)
    def _():
        p0 = jnp.where(first, HALO // 16, (cols + RAD - 1) // 16)
        lax.fori_loop(p0, p0 + 2, functools.partial(tt_pair, depth=256), 0)

    mid[pl.ds(bands, mid.shape[0] - bands)] = jnp.zeros((mid.shape[0] - bands, ext_r, LANES), BF)
    for idx, c in enumerate(b_copies):
        c.wait()

        def collect(i, carry):
            vec[0, i] = vec[0, i] + in_b[idx, i].astype(F32)
            return carry

        lax.fori_loop(0, nblk, collect, 0)

    chunk = ck // 4
    per = next_ // 2
    lane_c = iota((chunk, LANES), 1)
    lane_k = iota((ck, LANES), 1)

    def normal(n, carry):
        def stage(i, c):
            ext[n, 3 + i] = vec[n, i].astype(BF)
            return c

        lax.fori_loop(0, nblk, stage, 0)
        r_up = remote(ext.at[n, pl.ds(3, 3)], ext.at[n, pl.ds(3 + nblk, 3)], row_sem.at[n, 0], row_sem.at[n, 2], up)
        r_down = remote(ext.at[n, pl.ds(nblk, 3)], ext.at[n, pl.ds(0, 3)], row_sem.at[n, 1], row_sem.at[n, 3], down)
        r_up.start()
        r_down.start()
        r_up.wait()
        r_down.wait()

        def packing(c, cc):
            t, part = c // 4, lax.rem(c, 4)
            sl = pl.ds(pl.multiple_of(chunk * part, chunk), chunk)
            a = jnp.zeros((chunk, LANES), F32)
            b = a
            for g in range(per):
                v = ext[n, per * t + g, sl, :].astype(F32)
                m = (lane_c >= HALO * g) & (lane_c < HALO * (g + 1))
                a = jnp.where(m, pltpu.roll(v, HALO * g, 1) if g else v, a)
                b = jnp.where(m, pltpu.roll(v, (HALO * g - cols + HALO) % LANES, 1), b)
            pack[n, 0, t, sl, :] = a.astype(BF)
            pack[n, 1, t, sl, :] = b.astype(BF)
            return cc

        lax.fori_loop(0, 8, packing, 0)
        c_left = remote(pack.at[n, 0], pack_in.at[n, 1], col_sem.at[n, 0], col_sem.at[n, 2], left)
        c_right = remote(pack.at[n, 1], pack_in.at[n, 0], col_sem.at[n, 1], col_sem.at[n, 3], right)
        c_left.start()
        c_right.start()
        c_left.wait()
        c_right.wait()

        def block(blk):
            t, g = blk // per, blk % per
            mine = pltpu.roll(ext[n, blk].astype(F32), HALO, 1)
            a = pltpu.roll(pack_in[n, 0, t].astype(F32), (LANES - HALO * g) % LANES, 1)
            b = pltpu.roll(pack_in[n, 1, t].astype(F32), (cols + HALO - HALO * g) % LANES, 1)
            inside = jnp.logical_not((top_dev if blk < 3 else False) | (low_dev if blk >= 3 + nblk else False))
            a_ok = inside & jnp.logical_not(first)
            b_ok = inside & jnp.logical_not(last)
            a = jnp.where(a_ok, a, 0.0)
            b = jnp.where(b_ok, b, 0.0)
            mine = jnp.where(inside, mine, 0.0)
            t0 = jnp.where(lane_k < HALO, a, jnp.where(lane_k < HALO + cols, mine, b))
            t1 = jnp.where(lane_k < cols + 2 * HALO - LANES, b, 0.0)
            return jnp.concatenate([t0, t1], axis=1).astype(BF)

        def expand(i, c):
            x0, x1 = block(2 * i), block(2 * i + 1)
            for m in range(4):
                e = e8[8 * step * m : 8 * step * (m + 1)]
                y0 = mm(e, x0).reshape(step, 8, 256)
                y1 = mm(e, x1).reshape(step, 8, 256)
                v = jnp.concatenate([y0, y1], axis=1).astype(BF)
                spec[step * m : step * (m + 1), 16 * i : 16 * (i + 1), :] = v
            return c

        for i in range(next_ // 2):
            expand(i, 0)

        def columns(g, c):
            for q in range(56):
                b = 56 * g + q
                mid[b] = mm(spec[b][:, :ku], tt[b]).astype(BF)
            return c

        lax.fori_loop(0, bands // 56, columns, 0)

        def along(g, c):
            for q in range(40):
                t = 40 * g + q
                v = jnp.concatenate([mid[t], mid[third + t], mid[2 * third + t]], axis=0)
                v = mm(rr[t][:, : 3 * ext_r], v)
                for k in range(3):
                    fin[third * k + t] = v[rows * k : rows * (k + 1)]
            return c

        lax.fori_loop(0, third // 40, along, 0)

        def project(i, c):
            v = fin[:bands, pl.ds(pl.multiple_of(8 * i, 8), 8), :].reshape(bands * 8, LANES).astype(BF)
            vec[n + 1, i] = mm(p8[...], v) + ridge[...] * vec[n, i]
            return c

        lax.fori_loop(0, nblk, project, 0)
        return carry

    lax.fori_loop(0, 2, normal, 0)

    def products(i, sums):
        a, b, c = vec[0, i], vec[1, i], vec[2, i]
        parts = [a * a, a * b, b * b, a * c, b * c]
        return tuple(s + jnp.sum(v.reshape(comps, 8, LANES), axis=0) for s, v in zip(sums, parts))

    zero = jnp.zeros((8, LANES), F32)
    sums = lax.fori_loop(0, nblk, products, (zero,) * 5)
    total = jnp.concatenate([jnp.sum(v, axis=0, keepdims=True) for v in sums] + [jnp.zeros((3, LANES), F32)], axis=0)
    at = 0
    for level, (group, place, count) in enumerate(((peers, j, nbd), (peers_r, i_row, nrow))):
        red_src[level] = total
        red_in[level, place] = total
        copies = []
        for d in group:
            c = remote(red_src.at[level], red_in.at[level, place], red_sem.at[0, at], red_sem.at[1, at], d)
            c.start()
            copies.append(c)
            at += 1
        for c in copies:
            c.wait()
        total = red_in[level, 0]
        for k in range(1, count):
            total = total + red_in[level, k]
    tot = jnp.sum(total, axis=1, keepdims=True)
    r00, r01, r11, r02, r12 = [tot[k : k + 1] for k in range(5)]
    alpha = r00 / r01
    new = r00 - 2.0 * alpha * r01 + alpha * alpha * r11
    gain = 1.0 + new / r00
    curve = gain * gain * r01 - alpha * gain * (r11 + r02) + alpha * alpha * r12
    alpha2 = new / curve

    def finish(i, carry):
        a, b, c = vec[0, i], vec[1, i], vec[2, i]
        xs = alpha * a + alpha2 * (gain * a - alpha * b)
        rs = (a - alpha * b) - alpha2 * (gain * b - alpha * c)
        sl = pl.ds(pl.multiple_of(8 * i, 8), 8)
        out[0, :, sl, :] = xs.reshape(comps, 8, LANES)
        out[1, :, sl, :] = rs.reshape(comps, 8, LANES)
        return carry

    lax.fori_loop(0, nblk, finish, 0)


def local(height, width, sizes, observed, row_taps, col_taps, spectral_basis, ridge_weights):
    own, rows, _ = observed.shape
    bands, comps = spectral_basis.shape
    ny, nc, nx, nz = sizes
    nbd = ny * nc
    cols = width // nbd
    full = -(-width // LANES) * LANES
    ext_r = rows + 2 * HALO
    ck, nblk = comps * 8, rows // 8
    third = -(-bands // 24) * 8
    ku = -(-(cols + 2 * HALO) // 16) * 16
    kw = -(-(nc * cols + 2 * RAD) // 16) * 16

    pad_own = -(-own // 16) * 16

    def vm(*shape, dtype=BF):
        return pltpu.VMEM(shape, dtype)

    dma = pltpu.SemaphoreType.DMA
    scratch = [
        vm(2, own * RAD, width),
        vm(4, pad_own, 256),
        vm(own, 8, LANES, dtype=F32),
        vm(ck, LANES, dtype=F32),
        vm(2 * pad_own, LANES, dtype=F32),
        vm(4 * rows, full, dtype=F32),
        vm(2, own * RAD, width),
        vm(nbd, 2, pad_own, 256),
        vm(2, bands, 256, dtype=F32),
        vm(own // 4, 4 * rows, 256),
        vm(own, kw, 256),
        vm(ny, own, rows, 256, dtype=F32),
        vm(ny, nblk, ck, LANES, dtype=F32),
        vm(ny, nblk, ck, LANES),
        vm(ny, nblk, ck, LANES),
        vm(ny - 1, nblk, ck, LANES),
        vm(ny - 1, nblk, ck, LANES),
        vm(bands, ku, LANES),
        vm(third, 3 * rows, 256),
        vm(bands * 8, ck),
        vm(ck, bands * 8),
        vm(ck, 256),
        vm(bands, ext_r, 256),
        vm(3 * third, ext_r, LANES),
        vm(3 * third, rows, LANES, dtype=F32),
        vm(bands // 8, LANES, LANES, dtype=F32),
        vm(2, ext_r // 8, ck, LANES),
        vm(2, 2, 2, ck, LANES),
        vm(2, 2, 2, ck, LANES),
        vm(3, nblk, ck, LANES, dtype=F32),
        vm(2, 8, LANES, dtype=F32),
        vm(2, max(nbd, nx * nz), 8, LANES, dtype=F32),
        dma((4,)),
        dma((2, nbd - 1, 2)),
        dma((2, ny)),
        dma((2, ny - 1)),
        dma((2, 4)),
        dma((2, 4)),
        dma((2, nbd + nx * nz - 2)),
    ]
    vmem = pl.BlockSpec(memory_space=pltpu.VMEM)
    both = pl.pallas_call(
        functools.partial(kernel, (cols, sizes)),
        out_shape=jax.ShapeDtypeStruct((2, comps, rows, LANES), F32),
        in_specs=[vmem] * 5,
        out_specs=vmem,
        scratch_shapes=scratch,
        compiler_params=pltpu.CompilerParams(
            collective_id=0, has_side_effects=True, vmem_limit_bytes=67043328
        ),
    )(observed, row_taps, col_taps, spectral_basis.T, ridge_weights[None, :])
    return both[0, :, :, :cols], both[1, :, :, :cols]


def solution(mesh):
    sizes = (4, 2, 4, 4)
    split = Mesh(mesh.devices.reshape(sizes), AXES)
    placed = (P(BAND, ROW, None), P(BAND, None), P(BAND, None), P(), P())

    def whole(observed, row_taps, col_taps, spectral_basis, ridge_weights):
        _, height, width = observed.shape
        return jax.shard_map(
            functools.partial(local, height, width, sizes),
            mesh=split,
            in_specs=placed,
            out_specs=(P(None, ROW, BAND), P(None, ROW, BAND)),
            check_vma=False,
        )(observed, row_taps, col_taps, spectral_basis, ridge_weights)

    return whole
```

```python
import functools

import jax
import jax.numpy as jnp
from jax import lax
from jax.experimental import pallas as pl
from jax.experimental.pallas import tpu as pltpu
from jax.sharding import Mesh
from jax.sharding import PartitionSpec as P

AXES = ("band_0", "band_1", "row_0", "row_1")
BAND = ("band_0", "band_1")
ROW = ("row_0", "row_1")
TAPS = 25
RAD = 12
HALO = 24
LANES = 128
SLOT = 64
BF = jnp.bfloat16
F32 = jnp.float32


def iota(shape, dim):
    return lax.broadcasted_iota(jnp.int32, shape, dim)


def mm(a, b):
    return lax.dot_general(a, b, (((1,), (0,)), ((), ())), preferred_element_type=F32)


def halves(v):
    hi = v.astype(BF)
    return hi, (v - hi.astype(F32)).astype(BF)


def onehot(mask):
    return jnp.where(mask, 1.0, 0.0)


def staircase(line, rows, shift):
    step = pltpu.roll(jnp.broadcast_to(line, (8, LANES)), 0, 1, stride=1, stride_axis=0)
    tiles = []
    for g in range(rows // 8):
        turn = (shift + 8 * g) % LANES
        tiles.append(pltpu.roll(step, turn, 1) if turn else step)
    return jnp.concatenate(tiles, axis=0)


def kernel(
    dims, obs, row_taps, col_taps, basis_t, ridge_in,
    out,
    edges, feats, taps, ridge, raw, vpad, edge_in, line_in, lines, rows_adj, cols_adj, zed, keep, out_a, in_a, out_b, in_b,
    tt, rr, e8, p8, p8_own, spec, mid, fin, work, ext, pack, pack_in, vec, red_src, red_in,
    edge_sem, line_sem, a_sem, b_sem, row_sem, col_sem, red_sem,
):
    cols, sizes = dims
    ny, nc, nx, nz = sizes
    nbd, nrow = ny * nc, nx * nz
    y, core = lax.axis_index("band_0"), lax.axis_index("band_1")
    x, z = lax.axis_index("row_0"), lax.axis_index("row_1")
    j, i_row = y * nc + core, x * nz + z
    own, rows, full = obs.shape
    comps, bands = basis_t.shape
    ext_r = rows + 2 * HALO
    nblk = rows // 8
    ck = comps * 8
    ku = tt.shape[1]
    first, last = j == 0, j == nbd - 1
    top_dev, low_dev = i_row == 0, i_row == nrow - 1

    def at_band(jj):
        return (jj // nc, lax.rem(jj, nc), x, z)

    def at_row(ii):
        return (y, core, ii // nz, lax.rem(ii, nz))

    up = at_row(lax.rem(i_row + nrow - 1, nrow))
    down = at_row(lax.rem(i_row + 1, nrow))
    left = at_band(lax.rem(j + nbd - 1, nbd))
    right = at_band(lax.rem(j + 1, nbd))
    partner = (y, 1 - core, x, z)
    peers = [at_band(lax.rem(j + s, nbd)) for s in range(1, nbd)]
    peers_r = [at_row(lax.rem(i_row + s, nrow)) for s in range(1, nrow)]

    barrier = pltpu.get_barrier_semaphore()
    everyone = peers + peers_r
    for d in everyone:
        pl.semaphore_signal(barrier, inc=1, device_id=d, device_id_type=pl.DeviceIdType.MESH)

    def pack_edges(g, carry):
        sl = pl.ds(pl.multiple_of(4 * RAD * g, 16), 4 * RAD)
        v = obs[pl.ds(4 * g, 4)].astype(F32)
        for k, lo in enumerate((0, rows - RAD)):
            slab = jnp.concatenate([v[q, lo : lo + RAD] for q in range(4)], axis=0)
            edges[k, sl, :] = slab.astype(BF)
        return carry

    lax.fori_loop(0, own // 4, pack_edges, 0)
    pl.semaphore_wait(barrier, len(everyone))

    def remote(src, dst, send, recv, device):
        return pltpu.make_async_remote_copy(
            src_ref=src, dst_ref=dst, send_sem=send, recv_sem=recv,
            device_id=device, device_id_type=pl.DeviceIdType.MESH,
        )

    to_up = remote(edges.at[0], edge_in.at[1], edge_sem.at[0], edge_sem.at[2], up)
    to_down = remote(edges.at[1], edge_in.at[0], edge_sem.at[1], edge_sem.at[3], down)
    to_up.start()
    to_down.start()

    pad_own = feats.shape[1]
    raw[...] = jnp.zeros_like(raw)
    raw[:own, :TAPS] = col_taps[...]
    raw[pad_own : pad_own + own, :TAPS] = row_taps[...]
    t = raw[...]
    t_hi, t_lo = halves(t)
    gr, gp = iota((LANES, 640), 0), iota((LANES, 640), 1)
    g1 = (gp * 5243) >> 17
    g1, g2 = onehot(gr == g1).astype(BF), onehot(gr == gp - TAPS * g1).astype(BF)
    prod = (mm(t_hi, g1) + mm(t_lo, g1)) * (mm(t_hi, g2) + mm(t_lo, g2))
    p_hi, p_lo = halves(prod)
    pp, f = iota((640, 256), 0), iota((640, 256), 1)
    m1 = (pp * 5243) >> 17
    m2 = pp - TAPS * m1
    fe = f - SLOT
    fx = (fe * 5462) >> 16
    fy = fe - RAD * fx
    lag = (f < 2 * TAPS - 1) & (m2 - m1 + TAPS - 1 == f)
    edge = (fe >= 0) & (fe < RAD * RAD)
    for k, cut in enumerate((
        (m1 - fx == m2 - fy) & (m1 - fx > RAD) & (m1 < TAPS),
        (m1 + fx == m2 + fy) & (m1 + fx < RAD),
    )):
        sel = onehot(lag | (edge & cut)).astype(BF)
        v = (mm(p_hi, sel) + mm(p_lo, sel)).astype(BF)
        feats[k] = v[:pad_own]
        feats[2 + k] = v[pad_own:]
    flip = onehot(iota((LANES, LANES), 0) + iota((LANES, LANES), 1) == TAPS - 1).astype(BF)
    taps[:, 0:1, :] = t[:own].reshape(own, 1, LANES)
    taps[:, 1:2, :] = mm(t_hi, flip)[pad_own : pad_own + own].reshape(own, 1, LANES)

    line_copies = []
    row_kind = jnp.where(low_dev, 3, 2)
    for s in range(1, nbd):
        dest = lax.rem(j + s, nbd)
        for k, kind in enumerate((jnp.where(dest == nbd - 1, 1, 0), row_kind)):
            c = remote(
                feats.at[kind], line_in.at[j, k], line_sem.at[0, s - 1, k], line_sem.at[1, s - 1, k], at_band(dest)
            )
            c.start()
            line_copies.append(c)
    line_in[j, 0] = feats[jnp.where(last, 1, 0)]
    line_in[j, 1] = feats[row_kind]

    r, l = iota((rows, LANES), 0), iota((rows, LANES), 1)

    def own_rows(g, carry):
        for q in range(4):
            line = taps[4 * g + q][1:2]
            d = l - rows * q + RAD - r
            m = (d >= 0) & (d < TAPS) & (l >= rows * q) & (l < rows * (q + 1))
            mine = jnp.where(m, staircase(line, rows, rows * q - RAD), 0.0)
            k = l - RAD * q
            d = k - r
            m = (d >= 0) & (d < TAPS) & (k >= 0) & (k < RAD)
            above = jnp.where(m, staircase(line, rows, RAD * q), 0.0)
            k = l - 4 * RAD - RAD * q
            d = k + rows + RAD - r
            m = (d >= 0) & (d < TAPS) & (k >= 0) & (k < RAD)
            below = jnp.where(m, staircase(line, rows, 4 * RAD + RAD * q - RAD - rows), 0.0)
            rows_adj[g, rows * q : rows * (q + 1), :LANES] = mine.astype(BF)
            rows_adj[g, rows * q : rows * (q + 1), LANES:] = (above + below).astype(BF)
        return carry

    lax.fori_loop(0, own // 4, own_rows, 0)

    kw = cols_adj.shape[1]
    w, o = iota((kw, LANES), 0), iota((kw, LANES), 1)

    def own_cols(b, carry):
        line = taps[b][0:1]
        for k in range(2):
            d = w - o - cols * k
            m = (d >= 0) & (d < TAPS) & (o < cols)
            t = jnp.where(m, staircase(line, kw, -HALO - cols * k), 0.0)
            cols_adj[b, :, LANES * k : LANES * (k + 1)] = t.astype(BF)
        return carry

    lax.fori_loop(0, own, own_cols, 0)

    spread = onehot(iota((comps, ck), 0) == (iota((comps, ck), 1) >> 3)).astype(BF)
    wide = lax.dot_general(basis_t[...], spread, (((0,), (0,)), ((), ())), preferred_element_type=F32)
    step = bands // 4
    er, el = iota((8 * step, ck), 0), iota((8 * step, ck), 1)
    for c in range(4):
        v = jnp.broadcast_to(wide[step * c : step * (c + 1)][:, None, :], (step, 8, ck)).reshape(8 * step, ck)
        e8[8 * step * c : 8 * step * (c + 1)] = jnp.where((er & 7) == (el & 7), v, 0.0).astype(BF)
    tall = onehot(iota((ck, comps), 1) == (iota((ck, comps), 0) >> 3)).astype(BF)
    tall = mm(tall, basis_t[...]).astype(BF)
    br, bl = iota((bands, 256), 0), iota((bands, 256), 1)
    same = (iota((ck, 256), 0) & 7) == (iota((ck, 256), 1) & 7)
    kr, kl = iota((ck, comps), 0), iota((ck, comps), 1)
    ridge_col = jnp.sum(jnp.where(kl == (kr >> 3), ridge_in[...], 0.0), axis=1, keepdims=True)
    ridge[...] = jnp.broadcast_to(ridge_col, (ck, LANES))
    vpad[...] = jnp.zeros_like(vpad)

    def widen(start):
        return jnp.where(same, mm(tall, onehot(br == start + (bl >> 3)).astype(BF)), 0.0).astype(BF)

    for c in range(bands // 32):
        p8[:, 256 * c : 256 * (c + 1)] = widen(32 * c)
    p8_own[...] = widen(own * j)

    for c in line_copies:
        c.wait()
    for k in range(2):
        for jj in range(nbd):
            lines[k, own * jj : own * (jj + 1)] = line_in[jj, k][:own].astype(F32)
    groups = bands // 8
    wide_n = 16 * LANES

    def shifted(depth, hit, edge_hit):
        f, n = iota((depth, wide_n), 0), iota((depth, wide_n), 1)
        s = onehot(f == hit(n))
        if edge_hit is not None:
            s = s - onehot(f == edge_hit(n))
        return s.astype(BF)

    def unfold(k, depth, sel):
        res = mm(lines[k, :, :depth].astype(BF), sel)
        for t in range(16):
            work[:, 8 * t : 8 * (t + 1), :] = res[:, LANES * t : LANES * (t + 1)].reshape(groups, 8, LANES)

    def tt_pair(p, carry, depth):
        def hit(n):
            a, b = 16 * p + (n >> 7), n & 127
            return jnp.where((b < cols) & (a < cols + 2 * HALO) & (a - b <= 2 * HALO), a - b, -1)

        def edge_hit(n):
            a, b = 16 * p + (n >> 7) - HALO, n & 127
            a, b = jnp.where(last, cols - 1 - a, a), jnp.where(last, cols - 1 - b, b)
            ok = (first | last) & (a >= 0) & (a < RAD) & (b >= 0) & (b < RAD)
            return jnp.where(ok, SLOT + RAD * a + b, -1)

        unfold(0, depth, shifted(depth, hit, edge_hit if depth > SLOT else None))

        def place(g, c):
            for s in range(8):
                v = work[g, pl.ds(s, 16, stride=8), :]
                tt[8 * g + s, pl.ds(pl.multiple_of(16 * p, 16), 16), :] = v.astype(BF)
            return c

        lax.fori_loop(0, groups, place, 0)
        return carry

    third = rr.shape[0]
    lane16 = iota((16, LANES), 1)

    def rr_pair(p, carry):
        def row_of(n):
            b = n & 127
            return jnp.where(b < rows, b + HALO, jnp.where(b < rows + HALO, b - rows, b))

        def hit(n):
            a, b = 16 * p + (n >> 7), row_of(n)
            return jnp.where((b < ext_r) & (b >= a) & (b - a <= 2 * HALO), b - a, -1)

        def edge_hit(n):
            a, b = 16 * p + (n >> 7), row_of(n) - HALO
            a, b = jnp.where(low_dev, rows - 1 - a, a), jnp.where(low_dev, rows - 1 - b, b)
            ok = (top_dev | low_dev) & (a >= 0) & (a < RAD) & (b >= 0) & (b < RAD)
            return jnp.where(ok, SLOT + RAD * a + b, -1)

        unfold(1, 256, shifted(256, hit, edge_hit))
        for q in range(3):
            lo = ext_r * q

            def place(g, c):
                for s in range(8):
                    v = work[g, pl.ds(s, 16, stride=8), :]
                    if lo % LANES:
                        v = pltpu.roll(v, lo % LANES, 1)
                    t0 = v if lo + ext_r <= LANES else jnp.where(lane16 >= lo, v, 0.0)
                    t1 = v if lo >= LANES else jnp.where(lane16 < lo + ext_r - LANES, v, 0.0)
                    at = (8 * g + s - third * q, pl.ds(pl.multiple_of(rows * q + 16 * p, 16), 16))
                    rr[at + (slice(0, LANES),)] = t0.astype(BF)
                    rr[at + (slice(LANES, 2 * LANES),)] = t1.astype(BF)
                return c

            lax.fori_loop(third * q // 8, min(third * (q + 1), bands) // 8, place, 0)
        return carry

    lax.fori_loop(0, rows // 16, rr_pair, 0)

    to_up.wait()
    to_down.wait()
    above_ok, below_ok = i_row > 0, i_row < nrow - 1

    def adjoint(g, carry):
        e = pl.ds(pl.multiple_of(4 * RAD * g, 16), 4 * RAD)
        above = edge_in[0, e]
        below = edge_in[1, e]
        mine = obs[pl.ds(4 * g, 4)].reshape(4 * rows, full)
        above = jnp.where(above_ok, above, jnp.zeros_like(above))
        below = jnp.where(below_ok, below, jnp.zeros_like(below))
        v = mm(rows_adj[g][:, : 4 * rows + 8 * RAD], jnp.concatenate([mine, above, below], axis=0))
        vpad[:, :full] = v
        v = vpad[...]
        wins = []
        for k in range(ny):
            start = nc * cols * k - RAD
            wins.append(pltpu.roll(v, (v.shape[1] - start) % v.shape[1], 1)[:, :256].astype(BF))
        for q in range(4):
            u = jnp.concatenate([t[rows * q : rows * (q + 1)] for t in wins], axis=0)
            u = mm(u[:, :kw], cols_adj[4 * g + q])
            for k in range(ny):
                zed[k, 4 * g + q] = u[rows * k : rows * (k + 1)]
        return carry

    lax.fori_loop(0, own // 4, adjoint, 0)

    offsets = [s for s in (2, 1, 3, 0) if s < ny]
    a_copies, b_copies = [], []

    def merge(idx):
        a_copies[idx].wait()
        done = idx == len(offsets) - 1

        def add(i, carry):
            v = keep[idx, i] + in_a[idx, i].astype(F32)
            if done:
                vec[0, i] = v
            else:
                out_b[idx, i] = v.astype(BF)
            return carry

        lax.fori_loop(0, nblk, add, 0)
        if not done:
            dest = (lax.rem(y + offsets[idx], ny), core, x, z)
            c = remote(out_b.at[idx], in_b.at[idx], b_sem.at[0, idx], b_sem.at[1, idx], dest)
            c.start()
            b_copies.append(c)

    for idx, off in enumerate(offsets):
        k = lax.rem(y + off, ny)

        def project(i, carry):
            v = zed[k, :, pl.ds(pl.multiple_of(8 * i, 8), 8), :].reshape(own * 8, 256).astype(BF)
            v = mm(p8_own[:, : own * 8], v)
            lo, hi = v[:, :LANES], v[:, LANES:]
            keep[idx, i] = jnp.where(core == 0, lo, hi)
            out_a[idx, i] = jnp.where(core == 0, hi, lo).astype(BF)
            return carry

        lax.fori_loop(0, nblk, project, 0)
        c = remote(out_a.at[idx], in_a.at[idx], a_sem.at[0, idx], a_sem.at[1, idx], partner)
        c.start()
        a_copies.append(c)
        if idx:
            merge(idx - 1)
    merge(len(offsets) - 1)
    lax.fori_loop(0, ku // 16, functools.partial(tt_pair, depth=SLOT), 0)

    @pl.when(first | last)
    def _():
        p0 = jnp.where(first, HALO // 16, (cols + RAD - 1) // 16)
        lax.fori_loop(p0, p0 + 2, functools.partial(tt_pair, depth=256), 0)

    mid[pl.ds(bands, mid.shape[0] - bands)] = jnp.zeros((mid.shape[0] - bands, ext_r, LANES), BF)
    for idx, c in enumerate(b_copies):
        c.wait()

        def collect(i, carry):
            vec[0, i] = vec[0, i] + in_b[idx, i].astype(F32)
            return carry

        lax.fori_loop(0, nblk, collect, 0)

    chunk = ck // 4
    lane_c = iota((chunk, LANES), 1)
    lane_k = iota((ck, LANES), 1)

    def normal(n, carry):
        def stage(i, c):
            ext[n, i] = vec[n, i].astype(BF)
            return c

        lax.fori_loop(0, nblk, stage, 0)
        r_up = remote(ext.at[n, pl.ds(0, 3)], ext.at[n, pl.ds(nblk + 3, 3)], row_sem.at[n, 0], row_sem.at[n, 2], up)
        r_down = remote(ext.at[n, pl.ds(nblk - 3, 3)], ext.at[n, pl.ds(nblk, 3)], row_sem.at[n, 1], row_sem.at[n, 3], down)
        r_up.start()
        r_down.start()

        def packing(t, blocks):
            def part(c, cc):
                sl = pl.ds(pl.multiple_of(chunk * c, chunk), chunk)
                a = jnp.zeros((chunk, LANES), F32)
                b = a
                for g, blk in enumerate(blocks):
                    v = ext[n, blk, sl, :].astype(F32)
                    m = (lane_c >= HALO * g) & (lane_c < HALO * (g + 1))
                    a = jnp.where(m, pltpu.roll(v, HALO * g, 1) if g else v, a)
                    b = jnp.where(m, pltpu.roll(v, (HALO * g - cols + HALO) % LANES, 1), b)
                pack[n, 0, t, sl, :] = a.astype(BF)
                pack[n, 1, t, sl, :] = b.astype(BF)
                return cc

            lax.fori_loop(0, ck // chunk, part, 0)

        def swap(first_t, count, k):
            sl = pl.ds(first_t, count)
            a = remote(pack.at[n, 0, sl], pack_in.at[n, 1, sl], col_sem.at[n, k], col_sem.at[n, k + 2], left)
            b = remote(pack.at[n, 1, sl], pack_in.at[n, 0, sl], col_sem.at[n, k + 1], col_sem.at[n, k + 3], right)
            a.start()
            b.start()
            return a, b

        def block(blk, t, g):
            mine = pltpu.roll(ext[n, blk].astype(F32), HALO, 1)
            a = pltpu.roll(pack_in[n, 0, t].astype(F32), (LANES - HALO * g) % LANES, 1)
            b = pltpu.roll(pack_in[n, 1, t].astype(F32), (cols + HALO - HALO * g) % LANES, 1)
            a_ok, b_ok = jnp.logical_not(first), jnp.logical_not(last)
            if blk >= nblk:
                inside = jnp.logical_not(top_dev if blk < nblk + 3 else low_dev)
                a_ok, b_ok = a_ok & inside, b_ok & inside
                mine = jnp.where(inside, mine, 0.0)
            a = jnp.where(a_ok, a, 0.0)
            b = jnp.where(b_ok, b, 0.0)
            t0 = jnp.where(lane_k < HALO, a, jnp.where(lane_k < HALO + cols, mine, b))
            t1 = jnp.where(lane_k < cols + 2 * HALO - LANES, b, 0.0)
            return jnp.concatenate([t0, t1], axis=1).astype(BF)

        def expand(row, x0, x1):
            for m in range(4):
                e = e8[8 * step * m : 8 * step * (m + 1)]
                y0 = mm(e, x0).reshape(step, 8, 256)
                y1 = mm(e, x1).reshape(step, 8, 256)
                v = jnp.concatenate([y0, y1], axis=1).astype(BF)
                spec[step * m : step * (m + 1), row : row + 16, :] = v

        def columns(lo, count):
            def body(g, c):
                for q in range(56):
                    b = 56 * g + q
                    mid[b, lo : lo + count] = mm(spec[b, lo : lo + count][:, :ku], tt[b]).astype(BF)
                return c

            lax.fori_loop(0, bands // 56, body, 0)

        packing(0, range(nblk))
        own_edges = swap(0, 1, 0)
        for c in own_edges:
            c.wait()
        for i in range(nblk // 2):
            expand(16 * i, block(2 * i, 0, 2 * i), block(2 * i + 1, 0, 2 * i + 1))
        r_up.wait()
        r_down.wait()
        packing(1, range(nblk, nblk + 3))
        packing(2, range(nblk + 3, nblk + 6))
        halo_edges = swap(1, 2, 4)
        columns(0, rows)
        for c in halo_edges:
            c.wait()
        for i in range(3):
            k0, k1 = 2 * i, 2 * i + 1
            expand(
                rows + 16 * i,
                block(nblk + k0, 1 + k0 // 3, k0 % 3),
                block(nblk + k1, 1 + k1 // 3, k1 % 3),
            )
        columns(rows, ext_r - rows)

        def along(g, c):
            for q in range(40):
                t = 40 * g + q
                v = jnp.concatenate([mid[t], mid[third + t], mid[2 * third + t]], axis=0)
                v = mm(rr[t][:, : 3 * ext_r], v)
                for k in range(3):
                    fin[third * k + t] = v[rows * k : rows * (k + 1)]
            return c

        lax.fori_loop(0, third // 40, along, 0)

        def project(i, c):
            v = fin[:bands, pl.ds(pl.multiple_of(8 * i, 8), 8), :].reshape(bands * 8, LANES).astype(BF)
            vec[n + 1, i] = mm(p8[...], v) + ridge[...] * vec[n, i]
            return c

        lax.fori_loop(0, nblk, project, 0)
        return carry

    lax.fori_loop(0, 2, normal, 0)

    def products(i, sums):
        a, b, c = vec[0, i], vec[1, i], vec[2, i]
        parts = [a * a, a * b, b * b, a * c, b * c]
        return tuple(s + jnp.sum(v.reshape(comps, 8, LANES), axis=0) for s, v in zip(sums, parts))

    zero = jnp.zeros((8, LANES), F32)
    sums = lax.fori_loop(0, nblk, products, (zero,) * 5)
    total = jnp.concatenate([jnp.sum(v, axis=0, keepdims=True) for v in sums] + [jnp.zeros((3, LANES), F32)], axis=0)
    at = 0
    for level, (group, place, count) in enumerate(((peers, j, nbd), (peers_r, i_row, nrow))):
        red_src[level] = total
        red_in[level, place] = total
        copies = []
        for d in group:
            c = remote(red_src.at[level], red_in.at[level, place], red_sem.at[0, at], red_sem.at[1, at], d)
            c.start()
            copies.append(c)
            at += 1
        for c in copies:
            c.wait()
        total = red_in[level, 0]
        for k in range(1, count):
            total = total + red_in[level, k]
    tot = jnp.sum(total, axis=1, keepdims=True)
    r00, r01, r11, r02, r12 = [tot[k : k + 1] for k in range(5)]
    alpha = r00 / r01
    new = r00 - 2.0 * alpha * r01 + alpha * alpha * r11
    gain = 1.0 + new / r00
    curve = gain * gain * r01 - alpha * gain * (r11 + r02) + alpha * alpha * r12
    alpha2 = new / curve

    def finish(i, carry):
        a, b, c = vec[0, i], vec[1, i], vec[2, i]
        xs = alpha * a + alpha2 * (gain * a - alpha * b)
        rs = (a - alpha * b) - alpha2 * (gain * b - alpha * c)
        sl = pl.ds(pl.multiple_of(8 * i, 8), 8)
        out[0, :, sl, :] = xs.reshape(comps, 8, LANES)
        out[1, :, sl, :] = rs.reshape(comps, 8, LANES)
        return carry

    lax.fori_loop(0, nblk, finish, 0)


def local(height, width, sizes, observed, row_taps, col_taps, spectral_basis, ridge_weights):
    own, rows, _ = observed.shape
    bands, comps = spectral_basis.shape
    ny, nc, nx, nz = sizes
    nbd = ny * nc
    cols = width // nbd
    full = -(-width // LANES) * LANES
    ext_r = rows + 2 * HALO
    ck, nblk = comps * 8, rows // 8
    third = -(-bands // 24) * 8
    ku = -(-(cols + 2 * HALO) // 16) * 16
    kw = -(-(nc * cols + 2 * RAD) // 16) * 16

    pad_own = -(-own // 16) * 16

    def vm(*shape, dtype=BF):
        return pltpu.VMEM(shape, dtype)

    dma = pltpu.SemaphoreType.DMA
    scratch = [
        vm(2, own * RAD, width),
        vm(4, pad_own, 256),
        vm(own, 8, LANES, dtype=F32),
        vm(ck, LANES, dtype=F32),
        vm(2 * pad_own, LANES, dtype=F32),
        vm(4 * rows, full, dtype=F32),
        vm(2, own * RAD, width),
        vm(nbd, 2, pad_own, 256),
        vm(2, bands, 256, dtype=F32),
        vm(own // 4, 4 * rows, 256),
        vm(own, kw, 256),
        vm(ny, own, rows, 256, dtype=F32),
        vm(ny, nblk, ck, LANES, dtype=F32),
        vm(ny, nblk, ck, LANES),
        vm(ny, nblk, ck, LANES),
        vm(ny - 1, nblk, ck, LANES),
        vm(ny - 1, nblk, ck, LANES),
        vm(bands, ku, LANES),
        vm(third, 3 * rows, 256),
        vm(bands * 8, ck),
        vm(ck, bands * 8),
        vm(ck, 256),
        vm(bands, ext_r, 256),
        vm(3 * third, ext_r, LANES),
        vm(3 * third, rows, LANES, dtype=F32),
        vm(bands // 8, LANES, LANES, dtype=F32),
        vm(2, ext_r // 8, ck, LANES),
        vm(2, 2, 3, ck, LANES),
        vm(2, 2, 3, ck, LANES),
        vm(3, nblk, ck, LANES, dtype=F32),
        vm(2, 8, LANES, dtype=F32),
        vm(2, max(nbd, nx * nz), 8, LANES, dtype=F32),
        dma((4,)),
        dma((2, nbd - 1, 2)),
        dma((2, ny)),
        dma((2, ny - 1)),
        dma((2, 4)),
        dma((2, 8)),
        dma((2, nbd + nx * nz - 2)),
    ]
    vmem = pl.BlockSpec(memory_space=pltpu.VMEM)
    both = pl.pallas_call(
        functools.partial(kernel, (cols, sizes)),
        out_shape=jax.ShapeDtypeStruct((2, comps, rows, LANES), F32),
        in_specs=[vmem] * 5,
        out_specs=vmem,
        scratch_shapes=scratch,
        compiler_params=pltpu.CompilerParams(
            collective_id=0, has_side_effects=True, vmem_limit_bytes=67043328
        ),
    )(observed, row_taps, col_taps, spectral_basis.T, ridge_weights[None, :])
    return both[0, :, :, :cols], both[1, :, :, :cols]


def solution(mesh):
    sizes = (4, 2, 4, 4)
    split = Mesh(mesh.devices.reshape(sizes), AXES)
    placed = (P(BAND, ROW, None), P(BAND, None), P(BAND, None), P(), P())

    def whole(observed, row_taps, col_taps, spectral_basis, ridge_weights):
        _, height, width = observed.shape
        return jax.shard_map(
            functools.partial(local, height, width, sizes),
            mesh=split,
            in_specs=placed,
            out_specs=(P(None, ROW, BAND), P(None, ROW, BAND)),
            check_vma=False,
        )(observed, row_taps, col_taps, spectral_basis, ridge_weights)

    return whole
```

```python
import functools

import jax
import jax.numpy as jnp
from jax import lax
from jax.experimental import pallas as pl
from jax.experimental.pallas import tpu as pltpu
from jax.sharding import Mesh
from jax.sharding import PartitionSpec as P

AXES = ("band_0", "band_1", "row_0", "row_1")
BAND = ("band_0", "band_1")
ROW = ("row_0", "row_1")
TAPS = 25
RAD = 12
HALO = 24
LANES = 128
SLOT = 64
BF = jnp.bfloat16
F32 = jnp.float32


def iota(shape, dim):
    return lax.broadcasted_iota(jnp.int32, shape, dim)


def mm(a, b):
    return lax.dot_general(a, b, (((1,), (0,)), ((), ())), preferred_element_type=F32)


def halves(v):
    hi = v.astype(BF)
    return hi, (v - hi.astype(F32)).astype(BF)


def onehot(mask):
    return jnp.where(mask, 1.0, 0.0)


def staircase(line, rows, shift):
    step = pltpu.roll(jnp.broadcast_to(line, (8, LANES)), 0, 1, stride=1, stride_axis=0)
    tiles = []
    for g in range(rows // 8):
        turn = (shift + 8 * g) % LANES
        tiles.append(pltpu.roll(step, turn, 1) if turn else step)
    return jnp.concatenate(tiles, axis=0)


def kernel(
    dims, obs, row_taps, col_taps, basis_t, ridge_in,
    out,
    edges, feats, taps, ridge, raw, vpad, edge_in, line_in, lines, rows_adj, cols_adj, zed, keep, out_a, in_a, out_b, in_b,
    tt, rr, e8, p8, p8_own, spec, mid, fin, work, ext, pack, pack_in, vec, red_src, red_in, tight, tight_in,
    edge_sem, line_sem, a_sem, b_sem, row_sem, col_sem, red_sem,
):
    cols, sizes = dims
    ny, nc, nx, nz = sizes
    nbd, nrow = ny * nc, nx * nz
    y, core = lax.axis_index("band_0"), lax.axis_index("band_1")
    x, z = lax.axis_index("row_0"), lax.axis_index("row_1")
    j, i_row = y * nc + core, x * nz + z
    own, rows, full = obs.shape
    comps, bands = basis_t.shape
    ext_r = rows + 2 * HALO
    nblk = rows // 8
    ck = comps * 8
    ku = tt.shape[1]
    first, last = j == 0, j == nbd - 1
    top_dev, low_dev = i_row == 0, i_row == nrow - 1

    def at_band(jj):
        return (jj // nc, lax.rem(jj, nc), x, z)

    def at_row(ii):
        return (y, core, ii // nz, lax.rem(ii, nz))

    up = at_row(lax.rem(i_row + nrow - 1, nrow))
    down = at_row(lax.rem(i_row + 1, nrow))
    left = at_band(lax.rem(j + nbd - 1, nbd))
    right = at_band(lax.rem(j + 1, nbd))
    partner = (y, 1 - core, x, z)
    peers = [at_band(lax.rem(j + s, nbd)) for s in range(1, nbd)]
    peers_r = [at_row(lax.rem(i_row + s, nrow)) for s in range(1, nrow)]


    def corner(di, dj):
        ii, jj = lax.rem(i_row + nrow + di, nrow), lax.rem(j + nbd + dj, nbd)
        return (jj // nc, lax.rem(jj, nc), ii // nz, lax.rem(ii, nz))

    corners = {(di, dj): corner(di, dj) for di in (-1, 1) for dj in (-1, 1)}

    barrier = pltpu.get_barrier_semaphore()
    everyone = peers + peers_r + list(corners.values())
    for d in everyone:
        pl.semaphore_signal(barrier, inc=1, device_id=d, device_id_type=pl.DeviceIdType.MESH)

    def pack_edges(g, carry):
        sl = pl.ds(pl.multiple_of(4 * RAD * g, 16), 4 * RAD)
        v = obs[pl.ds(4 * g, 4)].astype(F32)
        for k, lo in enumerate((0, rows - RAD)):
            slab = jnp.concatenate([v[q, lo : lo + RAD] for q in range(4)], axis=0)
            edges[k, sl, :] = slab.astype(BF)
        return carry

    lax.fori_loop(0, own // 4, pack_edges, 0)
    pl.semaphore_wait(barrier, len(everyone))

    def remote(src, dst, send, recv, device):
        return pltpu.make_async_remote_copy(
            src_ref=src, dst_ref=dst, send_sem=send, recv_sem=recv,
            device_id=device, device_id_type=pl.DeviceIdType.MESH,
        )

    to_up = remote(edges.at[0], edge_in.at[1], edge_sem.at[0], edge_sem.at[2], up)
    to_down = remote(edges.at[1], edge_in.at[0], edge_sem.at[1], edge_sem.at[3], down)
    to_up.start()
    to_down.start()

    pad_own = feats.shape[1]
    raw[...] = jnp.zeros_like(raw)
    raw[:own, :TAPS] = col_taps[...]
    raw[pad_own : pad_own + own, :TAPS] = row_taps[...]
    t = raw[...]
    t_hi, t_lo = halves(t)
    gr, gp = iota((LANES, 640), 0), iota((LANES, 640), 1)
    g1 = (gp * 5243) >> 17
    g1, g2 = onehot(gr == g1).astype(BF), onehot(gr == gp - TAPS * g1).astype(BF)
    prod = (mm(t_hi, g1) + mm(t_lo, g1)) * (mm(t_hi, g2) + mm(t_lo, g2))
    p_hi, p_lo = halves(prod)
    pp, f = iota((640, 256), 0), iota((640, 256), 1)
    m1 = (pp * 5243) >> 17
    m2 = pp - TAPS * m1
    fe = f - SLOT
    fx = (fe * 5462) >> 16
    fy = fe - RAD * fx
    lag = (f < 2 * TAPS - 1) & (m2 - m1 + TAPS - 1 == f)
    edge = (fe >= 0) & (fe < RAD * RAD)
    for k, cut in enumerate((
        (m1 - fx == m2 - fy) & (m1 - fx > RAD) & (m1 < TAPS),
        (m1 + fx == m2 + fy) & (m1 + fx < RAD),
    )):
        sel = onehot(lag | (edge & cut)).astype(BF)
        v = (mm(p_hi, sel) + mm(p_lo, sel)).astype(BF)
        feats[k] = v[:pad_own]
        feats[2 + k] = v[pad_own:]
    flip = onehot(iota((LANES, LANES), 0) + iota((LANES, LANES), 1) == TAPS - 1).astype(BF)
    taps[:, 0:1, :] = t[:own].reshape(own, 1, LANES)
    taps[:, 1:2, :] = mm(t_hi, flip)[pad_own : pad_own + own].reshape(own, 1, LANES)

    line_copies = []
    row_kind = jnp.where(low_dev, 3, 2)
    for s in range(1, nbd):
        dest = lax.rem(j + s, nbd)
        for k, kind in enumerate((jnp.where(dest == nbd - 1, 1, 0), row_kind)):
            c = remote(
                feats.at[kind], line_in.at[j, k], line_sem.at[0, s - 1, k], line_sem.at[1, s - 1, k], at_band(dest)
            )
            c.start()
            line_copies.append(c)
    line_in[j, 0] = feats[jnp.where(last, 1, 0)]
    line_in[j, 1] = feats[row_kind]

    r, l = iota((rows, LANES), 0), iota((rows, LANES), 1)

    def own_rows(g, carry):
        for q in range(4):
            line = taps[4 * g + q][1:2]
            d = l - rows * q + RAD - r
            m = (d >= 0) & (d < TAPS) & (l >= rows * q) & (l < rows * (q + 1))
            mine = jnp.where(m, staircase(line, rows, rows * q - RAD), 0.0)
            k = l - RAD * q
            d = k - r
            m = (d >= 0) & (d < TAPS) & (k >= 0) & (k < RAD)
            above = jnp.where(m, staircase(line, rows, RAD * q), 0.0)
            k = l - 4 * RAD - RAD * q
            d = k + rows + RAD - r
            m = (d >= 0) & (d < TAPS) & (k >= 0) & (k < RAD)
            below = jnp.where(m, staircase(line, rows, 4 * RAD + RAD * q - RAD - rows), 0.0)
            rows_adj[g, rows * q : rows * (q + 1), :LANES] = mine.astype(BF)
            rows_adj[g, rows * q : rows * (q + 1), LANES:] = (above + below).astype(BF)
        return carry

    lax.fori_loop(0, own // 4, own_rows, 0)

    kw = cols_adj.shape[1]
    w, o = iota((kw, LANES), 0), iota((kw, LANES), 1)

    def own_cols(b, carry):
        line = taps[b][0:1]
        for k in range(2):
            d = w - o - cols * k
            m = (d >= 0) & (d < TAPS) & (o < cols)
            t = jnp.where(m, staircase(line, kw, -HALO - cols * k), 0.0)
            cols_adj[b, :, LANES * k : LANES * (k + 1)] = t.astype(BF)
        return carry

    lax.fori_loop(0, own, own_cols, 0)

    spread = onehot(iota((comps, ck), 0) == (iota((comps, ck), 1) >> 3)).astype(BF)
    wide = lax.dot_general(basis_t[...], spread, (((0,), (0,)), ((), ())), preferred_element_type=F32)
    step = bands // 4
    er, el = iota((8 * step, ck), 0), iota((8 * step, ck), 1)
    for c in range(4):
        v = jnp.broadcast_to(wide[step * c : step * (c + 1)][:, None, :], (step, 8, ck)).reshape(8 * step, ck)
        e8[8 * step * c : 8 * step * (c + 1)] = jnp.where((er & 7) == (el & 7), v, 0.0).astype(BF)
    tall = onehot(iota((ck, comps), 1) == (iota((ck, comps), 0) >> 3)).astype(BF)
    tall = mm(tall, basis_t[...]).astype(BF)
    br, bl = iota((bands, 256), 0), iota((bands, 256), 1)
    same = (iota((ck, 256), 0) & 7) == (iota((ck, 256), 1) & 7)
    kr, kl = iota((ck, comps), 0), iota((ck, comps), 1)
    ridge_col = jnp.sum(jnp.where(kl == (kr >> 3), ridge_in[...], 0.0), axis=1, keepdims=True)
    ridge[...] = jnp.broadcast_to(ridge_col, (ck, LANES))
    vpad[...] = jnp.zeros_like(vpad)

    def widen(start):
        return jnp.where(same, mm(tall, onehot(br == start + (bl >> 3)).astype(BF)), 0.0).astype(BF)

    for c in range(bands // 32):
        p8[:, 256 * c : 256 * (c + 1)] = widen(32 * c)
    p8_own[...] = widen(own * j)

    for c in line_copies:
        c.wait()
    for k in range(2):
        for jj in range(nbd):
            lines[k, own * jj : own * (jj + 1)] = line_in[jj, k][:own].astype(F32)
    groups = bands // 8
    wide_n = 16 * LANES

    def shifted(depth, hit, edge_hit):
        f, n = iota((depth, wide_n), 0), iota((depth, wide_n), 1)
        s = onehot(f == hit(n))
        if edge_hit is not None:
            s = s - onehot(f == edge_hit(n))
        return s.astype(BF)

    def unfold(k, depth, sel):
        res = mm(lines[k, :, :depth].astype(BF), sel)
        for t in range(16):
            work[:, 8 * t : 8 * (t + 1), :] = res[:, LANES * t : LANES * (t + 1)].reshape(groups, 8, LANES)

    def tt_pair(p, carry, depth):
        def hit(n):
            a, b = 16 * p + (n >> 7), n & 127
            return jnp.where((b < cols) & (a < cols + 2 * HALO) & (a - b <= 2 * HALO), a - b, -1)

        def edge_hit(n):
            a, b = 16 * p + (n >> 7) - HALO, n & 127
            a, b = jnp.where(last, cols - 1 - a, a), jnp.where(last, cols - 1 - b, b)
            ok = (first | last) & (a >= 0) & (a < RAD) & (b >= 0) & (b < RAD)
            return jnp.where(ok, SLOT + RAD * a + b, -1)

        unfold(0, depth, shifted(depth, hit, edge_hit if depth > SLOT else None))

        def place(g, c):
            for s in range(8):
                v = work[g, pl.ds(s, 16, stride=8), :]
                tt[8 * g + s, pl.ds(pl.multiple_of(16 * p, 16), 16), :] = v.astype(BF)
            return c

        lax.fori_loop(0, groups, place, 0)
        return carry

    third = rr.shape[0]
    lane16 = iota((16, LANES), 1)

    def rr_pair(p, carry):
        def row_of(n):
            b = n & 127
            return jnp.where(b < rows, b + HALO, jnp.where(b < rows + HALO, b - rows, b))

        def hit(n):
            a, b = 16 * p + (n >> 7), row_of(n)
            return jnp.where((b < ext_r) & (b >= a) & (b - a <= 2 * HALO), b - a, -1)

        def edge_hit(n):
            a, b = 16 * p + (n >> 7), row_of(n) - HALO
            a, b = jnp.where(low_dev, rows - 1 - a, a), jnp.where(low_dev, rows - 1 - b, b)
            ok = (top_dev | low_dev) & (a >= 0) & (a < RAD) & (b >= 0) & (b < RAD)
            return jnp.where(ok, SLOT + RAD * a + b, -1)

        unfold(1, 256, shifted(256, hit, edge_hit))
        for q in range(3):
            lo = ext_r * q

            def place(g, c):
                for s in range(8):
                    v = work[g, pl.ds(s, 16, stride=8), :]
                    if lo % LANES:
                        v = pltpu.roll(v, lo % LANES, 1)
                    t0 = v if lo + ext_r <= LANES else jnp.where(lane16 >= lo, v, 0.0)
                    t1 = v if lo >= LANES else jnp.where(lane16 < lo + ext_r - LANES, v, 0.0)
                    at = (8 * g + s - third * q, pl.ds(pl.multiple_of(rows * q + 16 * p, 16), 16))
                    rr[at + (slice(0, LANES),)] = t0.astype(BF)
                    rr[at + (slice(LANES, 2 * LANES),)] = t1.astype(BF)
                return c

            lax.fori_loop(third * q // 8, min(third * (q + 1), bands) // 8, place, 0)
        return carry

    lax.fori_loop(0, rows // 16, rr_pair, 0)

    to_up.wait()
    to_down.wait()
    above_ok, below_ok = i_row > 0, i_row < nrow - 1

    def adjoint(g, carry):
        e = pl.ds(pl.multiple_of(4 * RAD * g, 16), 4 * RAD)
        above = edge_in[0, e]
        below = edge_in[1, e]
        mine = obs[pl.ds(4 * g, 4)].reshape(4 * rows, full)
        above = jnp.where(above_ok, above, jnp.zeros_like(above))
        below = jnp.where(below_ok, below, jnp.zeros_like(below))
        v = mm(rows_adj[g][:, : 4 * rows + 8 * RAD], jnp.concatenate([mine, above, below], axis=0))
        vpad[:, :full] = v
        v = vpad[...]
        wins = []
        for k in range(ny):
            start = nc * cols * k - RAD
            wins.append(pltpu.roll(v, (v.shape[1] - start) % v.shape[1], 1)[:, :256].astype(BF))
        for q in range(4):
            u = jnp.concatenate([t[rows * q : rows * (q + 1)] for t in wins], axis=0)
            u = mm(u[:, :kw], cols_adj[4 * g + q])
            for k in range(ny):
                zed[k, 4 * g + q] = u[rows * k : rows * (k + 1)]
        return carry

    lax.fori_loop(0, own // 4, adjoint, 0)

    offsets = [s for s in (2, 1, 3, 0) if s < ny]
    a_copies, b_copies = [], []

    def merge(idx):
        a_copies[idx].wait()
        done = idx == len(offsets) - 1

        def add(i, carry):
            v = keep[idx, i] + in_a[idx, i].astype(F32)
            if done:
                vec[0, i] = v
            else:
                out_b[idx, i] = v.astype(BF)
            return carry

        lax.fori_loop(0, nblk, add, 0)
        if not done:
            dest = (lax.rem(y + offsets[idx], ny), core, x, z)
            c = remote(out_b.at[idx], in_b.at[idx], b_sem.at[0, idx], b_sem.at[1, idx], dest)
            c.start()
            b_copies.append(c)

    for idx, off in enumerate(offsets):
        k = lax.rem(y + off, ny)

        for i in range(nblk):
            v = zed[k, :, 8 * i : 8 * (i + 1), :].reshape(own * 8, 256).astype(BF)
            v = mm(p8_own[:, : own * 8], v)
            lo, hi = v[:, :LANES], v[:, LANES:]
            keep[idx, i] = jnp.where(core == 0, lo, hi)
            out_a[idx, i] = jnp.where(core == 0, hi, lo).astype(BF)
        c = remote(out_a.at[idx], in_a.at[idx], a_sem.at[0, idx], a_sem.at[1, idx], partner)
        c.start()
        a_copies.append(c)
        if idx:
            merge(idx - 1)
    merge(len(offsets) - 1)
    lax.fori_loop(0, ku // 16, functools.partial(tt_pair, depth=SLOT), 0)

    @pl.when(first | last)
    def _():
        p0 = jnp.where(first, HALO // 16, (cols + RAD - 1) // 16)
        lax.fori_loop(p0, p0 + 2, functools.partial(tt_pair, depth=256), 0)

    mid[pl.ds(bands, mid.shape[0] - bands)] = jnp.zeros((mid.shape[0] - bands, ext_r, LANES), BF)
    for idx, c in enumerate(b_copies):
        c.wait()

        def collect(i, carry):
            vec[0, i] = vec[0, i] + in_b[idx, i].astype(F32)
            return carry

        lax.fori_loop(0, nblk, collect, 0)

    chunk = ck // 4
    lane_c = iota((chunk, LANES), 1)
    lane_k = iota((ck, LANES), 1)

    def normal(n, carry):
        def stage(i, c):
            ext[n, i] = vec[n, i].astype(BF)
            return c

        lax.fori_loop(0, nblk, stage, 0)
        cut = LANES - cols
        for k, lo in enumerate((0, nblk - 3)):
            a, b, c = (vec[n, lo + q] for q in range(3))
            b = pltpu.roll(b, cols, 1)
            c = pltpu.roll(c, cols - cut, 1)
            tight[n, k, 0] = jnp.where(lane_k < cols, a, b).astype(BF)
            tight[n, k, 1] = jnp.where(lane_k < cols - cut, b, c).astype(BF)
        r_up = remote(tight.at[n, 0], tight_in.at[n, 1], row_sem.at[n, 0], row_sem.at[n, 2], up)
        r_down = remote(tight.at[n, 1], tight_in.at[n, 0], row_sem.at[n, 1], row_sem.at[n, 3], down)

        def packing(t, blocks):
            def part(c, cc):
                sl = pl.ds(pl.multiple_of(chunk * c, chunk), chunk)
                a = jnp.zeros((chunk, LANES), F32)
                b = a
                for g, blk in enumerate(blocks):
                    v = ext[n, blk, sl, :].astype(F32)
                    m = (lane_c >= HALO * g) & (lane_c < HALO * (g + 1))
                    a = jnp.where(m, pltpu.roll(v, HALO * g, 1) if g else v, a)
                    b = jnp.where(m, pltpu.roll(v, (HALO * g - cols + HALO) % LANES, 1), b)
                pack[n, 0, t, sl, :] = a.astype(BF)
                pack[n, 1, t, sl, :] = b.astype(BF)
                return cc

            lax.fori_loop(0, ck // chunk, part, 0)

        def to(src, dst, k, device):
            c = remote(pack.at[(n,) + src], pack_in.at[(n,) + dst], col_sem.at[n, 0, k], col_sem.at[n, 1, k], device)
            c.start()
            return c

        def block(blk, t, g):
            mine = pltpu.roll(ext[n, blk].astype(F32), HALO, 1)
            a = pltpu.roll(pack_in[n, 0, t].astype(F32), (LANES - HALO * g) % LANES, 1)
            b = pltpu.roll(pack_in[n, 1, t].astype(F32), (cols + HALO - HALO * g) % LANES, 1)
            a_ok, b_ok = jnp.logical_not(first), jnp.logical_not(last)
            if blk >= nblk:
                inside = jnp.logical_not(top_dev if blk < nblk + 3 else low_dev)
                a_ok, b_ok = a_ok & inside, b_ok & inside
                mine = jnp.where(inside, mine, 0.0)
            a = jnp.where(a_ok, a, 0.0)
            b = jnp.where(b_ok, b, 0.0)
            t0 = jnp.where(lane_k < HALO, a, jnp.where(lane_k < HALO + cols, mine, b))
            t1 = jnp.where(lane_k < cols + 2 * HALO - LANES, b, 0.0)
            return jnp.concatenate([t0, t1], axis=1).astype(BF)

        def expand(row, x0, x1):
            for m in range(4):
                e = e8[8 * step * m : 8 * step * (m + 1)]
                y0 = mm(e, x0).reshape(step, 8, 256)
                y1 = mm(e, x1).reshape(step, 8, 256)
                v = jnp.concatenate([y0, y1], axis=1).astype(BF)
                spec[step * m : step * (m + 1), row : row + 16, :] = v

        def columns(lo, count):
            def body(g, c):
                for q in range(56):
                    b = 56 * g + q
                    mid[b, lo : lo + count] = mm(spec[b, lo : lo + count][:, :ku], tt[b]).astype(BF)
                return c

            lax.fori_loop(0, bands // 56, body, 0)

        packing(0, range(nblk))
        own_edges = [to((0, 0), (1, 0), 0, left), to((1, 0), (0, 0), 1, right)]
        r_up.start()
        r_down.start()
        packing(1, range(nblk - 3, nblk))
        packing(2, range(3))
        halo_edges = [
            to((1, 1), (0, 1), 2, corners[1, 1]),
            to((0, 1), (1, 1), 3, corners[1, -1]),
            to((1, 2), (0, 2), 4, corners[-1, 1]),
            to((0, 2), (1, 2), 5, corners[-1, -1]),
        ]
        for c in own_edges:
            c.wait()
        for i in range(nblk // 2):
            expand(16 * i, block(2 * i, 0, 2 * i), block(2 * i + 1, 0, 2 * i + 1))
        columns(0, rows)
        r_up.wait()
        r_down.wait()
        for k in range(2):
            a, b = tight_in[n, k, 0].astype(F32), tight_in[n, k, 1].astype(F32)
            ext[n, nblk + 3 * k] = tight_in[n, k, 0]
            b1 = jnp.where(lane_k < cut, pltpu.roll(a, cut, 1), pltpu.roll(b, cut, 1))
            ext[n, nblk + 3 * k + 1] = b1.astype(BF)
            ext[n, nblk + 3 * k + 2] = pltpu.roll(b, 2 * cut, 1).astype(BF)
        for c in halo_edges:
            c.wait()
        for i in range(3):
            k0, k1 = 2 * i, 2 * i + 1
            expand(
                rows + 16 * i,
                block(nblk + k0, 1 + k0 // 3, k0 % 3),
                block(nblk + k1, 1 + k1 // 3, k1 % 3),
            )
        columns(rows, ext_r - rows)

        def along(g, c):
            for q in range(40):
                t = 40 * g + q
                v = jnp.concatenate([mid[t], mid[third + t], mid[2 * third + t]], axis=0)
                v = mm(rr[t][:, : 3 * ext_r], v)
                for k in range(3):
                    fin[third * k + t] = v[rows * k : rows * (k + 1)]
            return c

        lax.fori_loop(0, third // 40, along, 0)

        for i in range(nblk):
            v = fin[:bands, 8 * i : 8 * (i + 1), :].reshape(bands * 8, LANES).astype(BF)
            vec[n + 1, i] = mm(p8[...], v) + ridge[...] * vec[n, i]
        return carry

    lax.fori_loop(0, 2, normal, 0)

    def products(i, sums):
        a, b, c = vec[0, i], vec[1, i], vec[2, i]
        parts = [a * a, a * b, b * b, a * c, b * c]
        return tuple(s + jnp.sum(v.reshape(comps, 8, LANES), axis=0) for s, v in zip(sums, parts))

    zero = jnp.zeros((8, LANES), F32)
    sums = lax.fori_loop(0, nblk, products, (zero,) * 5)
    total = jnp.concatenate([jnp.sum(v, axis=0, keepdims=True) for v in sums] + [jnp.zeros((3, LANES), F32)], axis=0)
    at = 0
    for level, (group, place, count) in enumerate(((peers, j, nbd), (peers_r, i_row, nrow))):
        red_src[level] = total
        red_in[level, place] = total
        copies = []
        for d in group:
            c = remote(red_src.at[level], red_in.at[level, place], red_sem.at[0, at], red_sem.at[1, at], d)
            c.start()
            copies.append(c)
            at += 1
        for c in copies:
            c.wait()
        total = red_in[level, 0]
        for k in range(1, count):
            total = total + red_in[level, k]
    tot = jnp.sum(total, axis=1, keepdims=True)
    r00, r01, r11, r02, r12 = [tot[k : k + 1] for k in range(5)]
    alpha = r00 / r01
    new = r00 - 2.0 * alpha * r01 + alpha * alpha * r11
    gain = 1.0 + new / r00
    curve = gain * gain * r01 - alpha * gain * (r11 + r02) + alpha * alpha * r12
    alpha2 = new / curve

    def finish(i, carry):
        a, b, c = vec[0, i], vec[1, i], vec[2, i]
        xs = alpha * a + alpha2 * (gain * a - alpha * b)
        rs = (a - alpha * b) - alpha2 * (gain * b - alpha * c)
        sl = pl.ds(pl.multiple_of(8 * i, 8), 8)
        out[0, :, sl, :] = xs.reshape(comps, 8, LANES)
        out[1, :, sl, :] = rs.reshape(comps, 8, LANES)
        return carry

    lax.fori_loop(0, nblk, finish, 0)


def local(height, width, sizes, observed, row_taps, col_taps, spectral_basis, ridge_weights):
    own, rows, _ = observed.shape
    bands, comps = spectral_basis.shape
    ny, nc, nx, nz = sizes
    nbd = ny * nc
    cols = width // nbd
    full = -(-width // LANES) * LANES
    ext_r = rows + 2 * HALO
    ck, nblk = comps * 8, rows // 8
    third = -(-bands // 24) * 8
    ku = -(-(cols + 2 * HALO) // 16) * 16
    kw = -(-(nc * cols + 2 * RAD) // 16) * 16

    pad_own = -(-own // 16) * 16

    def vm(*shape, dtype=BF):
        return pltpu.VMEM(shape, dtype)

    dma = pltpu.SemaphoreType.DMA
    scratch = [
        vm(2, own * RAD, width),
        vm(4, pad_own, 256),
        vm(own, 8, LANES, dtype=F32),
        vm(ck, LANES, dtype=F32),
        vm(2 * pad_own, LANES, dtype=F32),
        vm(4 * rows, full, dtype=F32),
        vm(2, own * RAD, width),
        vm(nbd, 2, pad_own, 256),
        vm(2, bands, 256, dtype=F32),
        vm(own // 4, 4 * rows, 256),
        vm(own, kw, 256),
        vm(ny, own, rows, 256, dtype=F32),
        vm(ny, nblk, ck, LANES, dtype=F32),
        vm(ny, nblk, ck, LANES),
        vm(ny, nblk, ck, LANES),
        vm(ny - 1, nblk, ck, LANES),
        vm(ny - 1, nblk, ck, LANES),
        vm(bands, ku, LANES),
        vm(third, 3 * rows, 256),
        vm(bands * 8, ck),
        vm(ck, bands * 8),
        vm(ck, 256),
        vm(bands, ext_r, 256),
        vm(3 * third, ext_r, LANES),
        vm(3 * third, rows, LANES, dtype=F32),
        vm(bands // 8, LANES, LANES, dtype=F32),
        vm(2, ext_r // 8, ck, LANES),
        vm(2, 2, 3, ck, LANES),
        vm(2, 2, 3, ck, LANES),
        vm(3, nblk, ck, LANES, dtype=F32),
        vm(2, 8, LANES, dtype=F32),
        vm(2, max(nbd, nx * nz), 8, LANES, dtype=F32),
        vm(2, 2, 2, ck, LANES),
        vm(2, 2, 2, ck, LANES),
        dma((4,)),
        dma((2, nbd - 1, 2)),
        dma((2, ny)),
        dma((2, ny - 1)),
        dma((2, 4)),
        dma((2, 2, 6)),
        dma((2, nbd + nx * nz - 2)),
    ]
    vmem = pl.BlockSpec(memory_space=pltpu.VMEM)
    both = pl.pallas_call(
        functools.partial(kernel, (cols, sizes)),
        out_shape=jax.ShapeDtypeStruct((2, comps, rows, LANES), F32),
        in_specs=[vmem] * 5,
        out_specs=vmem,
        scratch_shapes=scratch,
        compiler_params=pltpu.CompilerParams(
            collective_id=0, has_side_effects=True, vmem_limit_bytes=67043328
        ),
    )(observed, row_taps, col_taps, spectral_basis.T, ridge_weights[None, :])
    return both[0, :, :, :cols], both[1, :, :, :cols]


def solution(mesh):
    sizes = (4, 2, 4, 4)
    split = Mesh(mesh.devices.reshape(sizes), AXES)
    placed = (P(BAND, ROW, None), P(BAND, None), P(BAND, None), P(), P())

    def whole(observed, row_taps, col_taps, spectral_basis, ridge_weights):
        _, height, width = observed.shape
        return jax.shard_map(
            functools.partial(local, height, width, sizes),
            mesh=split,
            in_specs=placed,
            out_specs=(P(None, ROW, BAND), P(None, ROW, BAND)),
            check_vma=False,
        )(observed, row_taps, col_taps, spectral_basis, ridge_weights)

    return whole
```

```python
import functools

import jax
import jax.numpy as jnp
from jax import lax
from jax.experimental import pallas as pl
from jax.experimental.pallas import tpu as pltpu
from jax.sharding import Mesh
from jax.sharding import PartitionSpec as P

AXES = ("band_0", "band_1", "row_0", "row_1")
BAND = ("band_0", "band_1")
ROW = ("row_0", "row_1")
TAPS = 25
RAD = 12
HALO = 24
LANES = 128
SLOT = 64
BF = jnp.bfloat16
F32 = jnp.float32


def iota(shape, dim):
    return lax.broadcasted_iota(jnp.int32, shape, dim)


def mm(a, b):
    return lax.dot_general(a, b, (((1,), (0,)), ((), ())), preferred_element_type=F32)


def halves(v):
    hi = v.astype(BF)
    return hi, (v - hi.astype(F32)).astype(BF)


def onehot(mask):
    return jnp.where(mask, 1.0, 0.0)


def staircase(line, rows, shift):
    step = pltpu.roll(jnp.broadcast_to(line, (8, LANES)), 0, 1, stride=1, stride_axis=0)
    tiles = []
    for g in range(rows // 8):
        turn = (shift + 8 * g) % LANES
        tiles.append(pltpu.roll(step, turn, 1) if turn else step)
    return jnp.concatenate(tiles, axis=0)


def kernel(
    dims, obs, row_taps, col_taps, basis_t, ridge_in,
    out,
    edges, feats, taps, ridge, raw, vpad, edge_in, line_in, lines, rows_adj, cols_adj, zed, keep, out_a, in_a, out_b, in_b,
    tt, rr, e8, p8, p8_own, spec, mid, fin, work, ext, pack, pack_in, vec, red_src, red_in, tight, tight_in,
    edge_sem, line_sem, a_sem, b_sem, row_sem, col_sem, red_sem,
):
    cols, sizes = dims
    ny, nc, nx, nz = sizes
    nbd, nrow = ny * nc, nx * nz
    y, core = lax.axis_index("band_0"), lax.axis_index("band_1")
    x, z = lax.axis_index("row_0"), lax.axis_index("row_1")
    j, i_row = y * nc + core, x * nz + z
    own, rows, full = obs.shape
    comps, bands = basis_t.shape
    ext_r = rows + 2 * HALO
    nblk = rows // 8
    ck = comps * 8
    ku = tt.shape[1]
    first, last = j == 0, j == nbd - 1
    top_dev, low_dev = i_row == 0, i_row == nrow - 1

    def at_band(jj):
        return (jj // nc, lax.rem(jj, nc), x, z)

    def at_row(ii):
        return (y, core, ii // nz, lax.rem(ii, nz))

    up = at_row(lax.rem(i_row + nrow - 1, nrow))
    down = at_row(lax.rem(i_row + 1, nrow))
    left = at_band(lax.rem(j + nbd - 1, nbd))
    right = at_band(lax.rem(j + 1, nbd))
    partner = (y, 1 - core, x, z)
    peers = [at_band(lax.rem(j + s, nbd)) for s in range(1, nbd)]
    peers_r = [at_row(lax.rem(i_row + s, nrow)) for s in range(1, nrow)]


    def corner(di, dj):
        ii, jj = lax.rem(i_row + nrow + di, nrow), lax.rem(j + nbd + dj, nbd)
        return (jj // nc, lax.rem(jj, nc), ii // nz, lax.rem(ii, nz))

    corners = {(di, dj): corner(di, dj) for di in (-1, 1) for dj in (-1, 1)}

    barrier = pltpu.get_barrier_semaphore()
    everyone = peers + peers_r + list(corners.values())
    for d in everyone:
        pl.semaphore_signal(barrier, inc=1, device_id=d, device_id_type=pl.DeviceIdType.MESH)

    def pack_edges(g, carry):
        sl = pl.ds(pl.multiple_of(4 * RAD * g, 16), 4 * RAD)
        v = obs[pl.ds(4 * g, 4)].astype(F32)
        for k, lo in enumerate((0, rows - RAD)):
            slab = jnp.concatenate([v[q, lo : lo + RAD] for q in range(4)], axis=0)
            edges[k, sl, :] = slab.astype(BF)
        return carry

    lax.fori_loop(0, own // 4, pack_edges, 0)
    pl.semaphore_wait(barrier, len(everyone))

    def remote(src, dst, send, recv, device):
        return pltpu.make_async_remote_copy(
            src_ref=src, dst_ref=dst, send_sem=send, recv_sem=recv,
            device_id=device, device_id_type=pl.DeviceIdType.MESH,
        )

    early = (own // 4 + 1) // 2
    edge_copies = []
    for part, sl in enumerate((pl.ds(0, 4 * RAD * early), pl.ds(4 * RAD * early, RAD * own - 4 * RAD * early))):
        a = remote(edges.at[0, sl], edge_in.at[1, sl], edge_sem.at[0, part, 0], edge_sem.at[1, part, 0], up)
        b = remote(edges.at[1, sl], edge_in.at[0, sl], edge_sem.at[0, part, 1], edge_sem.at[1, part, 1], down)
        a.start()
        b.start()
        edge_copies.append((a, b))

    pad_own = feats.shape[1]
    raw[...] = jnp.zeros_like(raw)
    raw[:own, :TAPS] = col_taps[...]
    raw[pad_own : pad_own + own, :TAPS] = row_taps[...]
    t = raw[...]
    t_hi, t_lo = halves(t)
    gr, gp = iota((LANES, 640), 0), iota((LANES, 640), 1)
    g1 = (gp * 5243) >> 17
    g1, g2 = onehot(gr == g1).astype(BF), onehot(gr == gp - TAPS * g1).astype(BF)
    prod = (mm(t_hi, g1) + mm(t_lo, g1)) * (mm(t_hi, g2) + mm(t_lo, g2))
    p_hi, p_lo = halves(prod)
    pp, f = iota((640, 256), 0), iota((640, 256), 1)
    m1 = (pp * 5243) >> 17
    m2 = pp - TAPS * m1
    fe = f - SLOT
    fx = (fe * 5462) >> 16
    fy = fe - RAD * fx
    lag = (f < 2 * TAPS - 1) & (m2 - m1 + TAPS - 1 == f)
    edge = (fe >= 0) & (fe < RAD * RAD)
    for k, cut in enumerate((
        (m1 - fx == m2 - fy) & (m1 - fx > RAD) & (m1 < TAPS),
        (m1 + fx == m2 + fy) & (m1 + fx < RAD),
    )):
        sel = onehot(lag | (edge & cut)).astype(BF)
        v = (mm(p_hi, sel) + mm(p_lo, sel)).astype(BF)
        feats[k] = v[:pad_own]
        feats[2 + k] = v[pad_own:]
    flip = onehot(iota((LANES, LANES), 0) + iota((LANES, LANES), 1) == TAPS - 1).astype(BF)
    taps[:, 0:1, :] = t[:own].reshape(own, 1, LANES)
    taps[:, 1:2, :] = mm(t_hi, flip)[pad_own : pad_own + own].reshape(own, 1, LANES)

    line_copies = []
    row_kind = jnp.where(low_dev, 3, 2)
    for s in range(1, nbd):
        dest = lax.rem(j + s, nbd)
        for k, kind in enumerate((jnp.where(dest == nbd - 1, 1, 0), row_kind)):
            c = remote(
                feats.at[kind], line_in.at[j, k], line_sem.at[0, s - 1, k], line_sem.at[1, s - 1, k], at_band(dest)
            )
            c.start()
            line_copies.append(c)
    line_in[j, 0] = feats[jnp.where(last, 1, 0)]
    line_in[j, 1] = feats[row_kind]

    r, l = iota((rows, LANES), 0), iota((rows, LANES), 1)

    def own_rows(g, carry):
        for q in range(4):
            line = taps[4 * g + q][1:2]
            d = l - rows * q + RAD - r
            m = (d >= 0) & (d < TAPS) & (l >= rows * q) & (l < rows * (q + 1))
            mine = jnp.where(m, staircase(line, rows, rows * q - RAD), 0.0)
            k = l - RAD * q
            d = k - r
            m = (d >= 0) & (d < TAPS) & (k >= 0) & (k < RAD)
            above = jnp.where(m, staircase(line, rows, RAD * q), 0.0)
            k = l - 4 * RAD - RAD * q
            d = k + rows + RAD - r
            m = (d >= 0) & (d < TAPS) & (k >= 0) & (k < RAD)
            below = jnp.where(m, staircase(line, rows, 4 * RAD + RAD * q - RAD - rows), 0.0)
            rows_adj[g, rows * q : rows * (q + 1), :LANES] = mine.astype(BF)
            rows_adj[g, rows * q : rows * (q + 1), LANES:] = (above + below).astype(BF)
        return carry

    lax.fori_loop(0, own // 4, own_rows, 0)

    kw = cols_adj.shape[1]
    w, o = iota((kw, LANES), 0), iota((kw, LANES), 1)

    def own_cols(b, carry):
        line = taps[b][0:1]
        for k in range(2):
            d = w - o - cols * k
            m = (d >= 0) & (d < TAPS) & (o < cols)
            t = jnp.where(m, staircase(line, kw, -HALO - cols * k), 0.0)
            cols_adj[b, :, LANES * k : LANES * (k + 1)] = t.astype(BF)
        return carry

    lax.fori_loop(0, own, own_cols, 0)

    spread = onehot(iota((comps, ck), 0) == (iota((comps, ck), 1) >> 3)).astype(BF)
    wide = lax.dot_general(basis_t[...], spread, (((0,), (0,)), ((), ())), preferred_element_type=F32)
    step = bands // 4
    er, el = iota((8 * step, ck), 0), iota((8 * step, ck), 1)
    for c in range(4):
        v = jnp.broadcast_to(wide[step * c : step * (c + 1)][:, None, :], (step, 8, ck)).reshape(8 * step, ck)
        e8[8 * step * c : 8 * step * (c + 1)] = jnp.where((er & 7) == (el & 7), v, 0.0).astype(BF)
    tall = onehot(iota((ck, comps), 1) == (iota((ck, comps), 0) >> 3)).astype(BF)
    tall = mm(tall, basis_t[...]).astype(BF)
    br, bl = iota((bands, 256), 0), iota((bands, 256), 1)
    same = (iota((ck, 256), 0) & 7) == (iota((ck, 256), 1) & 7)
    kr, kl = iota((ck, comps), 0), iota((ck, comps), 1)
    ridge_col = jnp.sum(jnp.where(kl == (kr >> 3), ridge_in[...], 0.0), axis=1, keepdims=True)
    ridge[...] = jnp.broadcast_to(ridge_col, (ck, LANES))
    vpad[...] = jnp.zeros_like(vpad)

    def widen(start):
        return jnp.where(same, mm(tall, onehot(br == start + (bl >> 3)).astype(BF)), 0.0).astype(BF)

    for c in range(bands // 32):
        p8[:, 256 * c : 256 * (c + 1)] = widen(32 * c)
    p8_own[...] = widen(own * j)

    for c in line_copies:
        c.wait()
    for k in range(2):
        for jj in range(nbd):
            lines[k, own * jj : own * (jj + 1)] = line_in[jj, k][:own].astype(F32)
    groups = bands // 8
    wide_n = 16 * LANES

    def shifted(depth, hit, edge_hit):
        f, n = iota((depth, wide_n), 0), iota((1, wide_n), 1)
        s = onehot(f == hit(n))
        if edge_hit is not None:
            s = s - onehot(f == edge_hit(n))
        return s.astype(BF)

    def unfold(k, depth, sel):
        res = mm(lines[k, :, :depth].astype(BF), sel)
        for t in range(16):
            work[:, 8 * t : 8 * (t + 1), :] = res[:, LANES * t : LANES * (t + 1)].reshape(groups, 8, LANES)

    def tt_pair(p, carry, depth):
        def hit(n):
            a, b = 16 * p + (n >> 7), n & 127
            return jnp.where((b < cols) & (a < cols + 2 * HALO) & (a - b <= 2 * HALO), a - b, -1)

        def edge_hit(n):
            a, b = 16 * p + (n >> 7) - HALO, n & 127
            a, b = jnp.where(last, cols - 1 - a, a), jnp.where(last, cols - 1 - b, b)
            ok = (first | last) & (a >= 0) & (a < RAD) & (b >= 0) & (b < RAD)
            return jnp.where(ok, SLOT + RAD * a + b, -1)

        unfold(0, depth, shifted(depth, hit, edge_hit if depth > SLOT else None))

        def place(g, c):
            for s in range(8):
                v = work[g, pl.ds(s, 16, stride=8), :]
                tt[8 * g + s, pl.ds(pl.multiple_of(16 * p, 16), 16), :] = v.astype(BF)
            return c

        lax.fori_loop(0, groups, place, 0)
        return carry

    third = rr.shape[0]
    lane16 = iota((16, LANES), 1)

    def rr_pair(p, carry):
        def row_of(n):
            b = n & 127
            return jnp.where(b < rows, b + HALO, jnp.where(b < rows + HALO, b - rows, b))

        def hit(n):
            a, b = 16 * p + (n >> 7), row_of(n)
            return jnp.where((b < ext_r) & (b >= a) & (b - a <= 2 * HALO), b - a, -1)

        def edge_hit(n):
            a, b = 16 * p + (n >> 7), row_of(n) - HALO
            a, b = jnp.where(low_dev, rows - 1 - a, a), jnp.where(low_dev, rows - 1 - b, b)
            ok = (top_dev | low_dev) & (a >= 0) & (a < RAD) & (b >= 0) & (b < RAD)
            return jnp.where(ok, SLOT + RAD * a + b, -1)

        unfold(1, 256, shifted(256, hit, edge_hit))
        for q in range(3):
            lo = ext_r * q

            def place(g, c):
                for s in range(8):
                    v = work[g, pl.ds(s, 16, stride=8), :]
                    if lo % LANES:
                        v = pltpu.roll(v, lo % LANES, 1)
                    t0 = v if lo + ext_r <= LANES else jnp.where(lane16 >= lo, v, 0.0)
                    t1 = v if lo >= LANES else jnp.where(lane16 < lo + ext_r - LANES, v, 0.0)
                    at = (8 * g + s - third * q, pl.ds(pl.multiple_of(rows * q + 16 * p, 16), 16))
                    rr[at + (slice(0, LANES),)] = t0.astype(BF)
                    rr[at + (slice(LANES, 2 * LANES),)] = t1.astype(BF)
                return c

            lax.fori_loop(third * q // 8, min(third * (q + 1), bands) // 8, place, 0)
        return carry

    lax.fori_loop(0, rows // 16, rr_pair, 0)

    above_ok, below_ok = i_row > 0, i_row < nrow - 1

    def adjoint(g):
        e = slice(4 * RAD * g, 4 * RAD * (g + 1))
        above = edge_in[0, e]
        below = edge_in[1, e]
        mine = obs[4 * g : 4 * g + 4].reshape(4 * rows, full)
        above = jnp.where(above_ok, above, jnp.zeros_like(above))
        below = jnp.where(below_ok, below, jnp.zeros_like(below))
        v = mm(rows_adj[g][:, : 4 * rows + 8 * RAD], jnp.concatenate([mine, above, below], axis=0))
        vpad[g % 2, :, :full] = v
        v = vpad[g % 2]
        wins = []
        for k in range(ny):
            start = nc * cols * k - RAD
            wins.append(pltpu.roll(v, (v.shape[1] - start) % v.shape[1], 1)[:, :256].astype(BF))
        for q in range(4):
            u = jnp.concatenate([t[rows * q : rows * (q + 1)] for t in wins], axis=0)
            u = mm(u[:, :kw], cols_adj[4 * g + q])
            for k in range(ny):
                zed[k, 4 * g + q] = u[rows * k : rows * (k + 1)]

    for g in range(own // 4):
        if g in (0, early):
            for c in edge_copies[g // max(early, 1)]:
                c.wait()
        adjoint(g)

    lane_k = iota((ck, LANES), 1)
    cut = LANES - cols
    offsets = [s for s in (2, 1, 3, 0) if s < ny]
    a_copies, b_copies = [], []

    def merge(idx):
        a_copies[idx].wait()
        done = idx == len(offsets) - 1

        def add(i):
            return keep[idx, i] + in_a[idx, i].astype(F32)

        if done:
            for i in range(nblk):
                vec[0, i] = add(i)
        else:
            b = pltpu.roll(add(1), cols, 1)
            out_b[idx, 0] = jnp.where(lane_k < cols, add(0), b).astype(BF)
            out_b[idx, 1] = jnp.where(lane_k < cols - cut, b, pltpu.roll(add(2), cols - cut, 1)).astype(BF)
            out_b[idx, 2] = add(3).astype(BF)
        if not done:
            dest = (lax.rem(y + offsets[idx], ny), core, x, z)
            c = remote(out_b.at[idx], in_b.at[idx], b_sem.at[0, idx], b_sem.at[1, idx], dest)
            c.start()
            b_copies.append(c)

    for idx, off in enumerate(offsets):
        k = lax.rem(y + off, ny)

        for i in range(nblk):
            v = zed[k, :, 8 * i : 8 * (i + 1), :].reshape(own * 8, 256).astype(BF)
            v = mm(p8_own[:, : own * 8], v)
            lo, hi = v[:, :LANES], v[:, LANES:]
            keep[idx, i] = jnp.where(core == 0, lo, hi)
            out_a[idx, i] = jnp.where(core == 0, hi, lo).astype(BF)
        c = remote(out_a.at[idx], in_a.at[idx], a_sem.at[0, idx], a_sem.at[1, idx], partner)
        c.start()
        a_copies.append(c)
        if idx:
            merge(idx - 1)
    merge(len(offsets) - 1)
    lax.fori_loop(0, ku // 16, functools.partial(tt_pair, depth=SLOT), 0)

    @pl.when(first | last)
    def _():
        p0 = jnp.where(first, HALO // 16, (cols + RAD - 1) // 16)
        lax.fori_loop(p0, p0 + 2, functools.partial(tt_pair, depth=256), 0)

    mid[pl.ds(bands, mid.shape[0] - bands)] = jnp.zeros((mid.shape[0] - bands, ext_r, LANES), BF)
    for c in b_copies:
        c.wait()
    a, b, c = (sum(in_b[idx, t].astype(F32) for idx in range(ny - 1)) for t in range(3))
    b1 = jnp.where(lane_k < cut, pltpu.roll(a, cut, 1), pltpu.roll(b, cut, 1))
    for i, v in enumerate((a, b1, pltpu.roll(b, 2 * cut, 1), c)):
        vec[0, i] = vec[0, i] + jnp.where(lane_k < cols, v, 0.0)

    chunk = ck // 4
    lane_c = iota((chunk, LANES), 1)

    def normal(n, carry):
        def stage(i, c):
            ext[n, i] = vec[n, i].astype(BF)
            return c

        lax.fori_loop(0, nblk, stage, 0)
        for k, lo in enumerate((0, nblk - 3)):
            a, b, c = (vec[n, lo + q] for q in range(3))
            b = pltpu.roll(b, cols, 1)
            c = pltpu.roll(c, cols - cut, 1)
            tight[n, k, 0] = jnp.where(lane_k < cols, a, b).astype(BF)
            tight[n, k, 1] = jnp.where(lane_k < cols - cut, b, c).astype(BF)
        r_up = remote(tight.at[n, 0], tight_in.at[n, 1], row_sem.at[n, 0], row_sem.at[n, 2], up)
        r_down = remote(tight.at[n, 1], tight_in.at[n, 0], row_sem.at[n, 1], row_sem.at[n, 3], down)

        def packing(t, blocks):
            def part(c, cc):
                sl = pl.ds(pl.multiple_of(chunk * c, chunk), chunk)
                a = jnp.zeros((chunk, LANES), F32)
                b = a
                for g, blk in enumerate(blocks):
                    v = ext[n, blk, sl, :].astype(F32)
                    m = (lane_c >= HALO * g) & (lane_c < HALO * (g + 1))
                    a = jnp.where(m, pltpu.roll(v, HALO * g, 1) if g else v, a)
                    b = jnp.where(m, pltpu.roll(v, (HALO * g - cols + HALO) % LANES, 1), b)
                pack[n, 0, t, sl, :] = a.astype(BF)
                pack[n, 1, t, sl, :] = b.astype(BF)
                return cc

            lax.fori_loop(0, ck // chunk, part, 0)

        def to(src, dst, k, device):
            c = remote(pack.at[(n,) + src], pack_in.at[(n,) + dst], col_sem.at[n, 0, k], col_sem.at[n, 1, k], device)
            c.start()
            return c

        def block(blk, t, g):
            mine = pltpu.roll(ext[n, blk].astype(F32), HALO, 1)
            a = pltpu.roll(pack_in[n, 0, t].astype(F32), (LANES - HALO * g) % LANES, 1)
            b = pltpu.roll(pack_in[n, 1, t].astype(F32), (cols + HALO - HALO * g) % LANES, 1)
            a_ok, b_ok = jnp.logical_not(first), jnp.logical_not(last)
            if blk >= nblk:
                inside = jnp.logical_not(top_dev if blk < nblk + 3 else low_dev)
                a_ok, b_ok = a_ok & inside, b_ok & inside
                mine = jnp.where(inside, mine, 0.0)
            a = jnp.where(a_ok, a, 0.0)
            b = jnp.where(b_ok, b, 0.0)
            t0 = jnp.where(lane_k < HALO, a, jnp.where(lane_k < HALO + cols, mine, b))
            t1 = jnp.where(lane_k < cols + 2 * HALO - LANES, b, 0.0)
            return jnp.concatenate([t0, t1], axis=1).astype(BF)

        def expand(row, x0, x1):
            for m in range(4):
                e = e8[8 * step * m : 8 * step * (m + 1)]
                y0 = mm(e, x0).reshape(step, 8, 256)
                y1 = mm(e, x1).reshape(step, 8, 256)
                v = jnp.concatenate([y0, y1], axis=1).astype(BF)
                spec[step * m : step * (m + 1), row : row + 16, :] = v

        def columns(lo, count):
            def body(g, c):
                for q in range(56):
                    b = 56 * g + q
                    mid[b, lo : lo + count] = mm(spec[b, lo : lo + count][:, :ku], tt[b]).astype(BF)
                return c

            lax.fori_loop(0, bands // 56, body, 0)

        packing(0, range(nblk))
        own_edges = [to((0, 0), (1, 0), 0, left), to((1, 0), (0, 0), 1, right)]
        r_up.start()
        r_down.start()
        packing(1, range(nblk - 3, nblk))
        packing(2, range(3))
        halo_edges = [
            to((1, 1), (0, 1), 2, corners[1, 1]),
            to((0, 1), (1, 1), 3, corners[1, -1]),
            to((1, 2), (0, 2), 4, corners[-1, 1]),
            to((0, 2), (1, 2), 5, corners[-1, -1]),
        ]
        for c in own_edges:
            c.wait()
        for i in range(nblk // 2):
            expand(16 * i, block(2 * i, 0, 2 * i), block(2 * i + 1, 0, 2 * i + 1))
        columns(0, rows)
        r_up.wait()
        r_down.wait()
        for k in range(2):
            a, b = tight_in[n, k, 0].astype(F32), tight_in[n, k, 1].astype(F32)
            ext[n, nblk + 3 * k] = tight_in[n, k, 0]
            b1 = jnp.where(lane_k < cut, pltpu.roll(a, cut, 1), pltpu.roll(b, cut, 1))
            ext[n, nblk + 3 * k + 1] = b1.astype(BF)
            ext[n, nblk + 3 * k + 2] = pltpu.roll(b, 2 * cut, 1).astype(BF)
        for c in halo_edges:
            c.wait()
        for i in range(3):
            k0, k1 = 2 * i, 2 * i + 1
            expand(
                rows + 16 * i,
                block(nblk + k0, 1 + k0 // 3, k0 % 3),
                block(nblk + k1, 1 + k1 // 3, k1 % 3),
            )
        columns(rows, ext_r - rows)

        def along(g, c):
            for q in range(40):
                t = 40 * g + q
                v = jnp.concatenate([mid[t], mid[third + t], mid[2 * third + t]], axis=0)
                v = mm(rr[t][:, : 3 * ext_r], v)
                for k in range(3):
                    fin[third * k + t] = v[rows * k : rows * (k + 1)]
            return c

        lax.fori_loop(0, third // 40, along, 0)

        for i in range(nblk):
            v = fin[:bands, 8 * i : 8 * (i + 1), :].reshape(bands * 8, LANES).astype(BF)
            vec[n + 1, i] = mm(p8[...], v) + ridge[...] * vec[n, i]
        return carry

    lax.fori_loop(0, 2, normal, 0)

    def products(i, sums):
        a, b, c = vec[0, i], vec[1, i], vec[2, i]
        parts = [a * a, a * b, b * b, a * c, b * c]
        return tuple(s + jnp.sum(v.reshape(comps, 8, LANES), axis=0) for s, v in zip(sums, parts))

    zero = jnp.zeros((8, LANES), F32)
    sums = lax.fori_loop(0, nblk, products, (zero,) * 5)
    total = jnp.concatenate([jnp.sum(v, axis=0, keepdims=True) for v in sums] + [jnp.zeros((3, LANES), F32)], axis=0)
    at = 0
    for level, (group, place, count) in enumerate(((peers, j, nbd), (peers_r, i_row, nrow))):
        red_src[level] = total
        red_in[level, place] = total
        copies = []
        for d in group:
            c = remote(red_src.at[level], red_in.at[level, place], red_sem.at[0, at], red_sem.at[1, at], d)
            c.start()
            copies.append(c)
            at += 1
        for c in copies:
            c.wait()
        total = red_in[level, 0]
        for k in range(1, count):
            total = total + red_in[level, k]
    tot = jnp.sum(total, axis=1, keepdims=True)
    r00, r01, r11, r02, r12 = [tot[k : k + 1] for k in range(5)]
    alpha = r00 / r01
    new = r00 - 2.0 * alpha * r01 + alpha * alpha * r11
    gain = 1.0 + new / r00
    curve = gain * gain * r01 - alpha * gain * (r11 + r02) + alpha * alpha * r12
    alpha2 = new / curve

    def finish(i, carry):
        a, b, c = vec[0, i], vec[1, i], vec[2, i]
        xs = alpha * a + alpha2 * (gain * a - alpha * b)
        rs = (a - alpha * b) - alpha2 * (gain * b - alpha * c)
        sl = pl.ds(pl.multiple_of(8 * i, 8), 8)
        out[0, :, sl, :] = xs.reshape(comps, 8, LANES)
        out[1, :, sl, :] = rs.reshape(comps, 8, LANES)
        return carry

    lax.fori_loop(0, nblk, finish, 0)


def local(height, width, sizes, observed, row_taps, col_taps, spectral_basis, ridge_weights):
    own, rows, _ = observed.shape
    bands, comps = spectral_basis.shape
    ny, nc, nx, nz = sizes
    nbd = ny * nc
    cols = width // nbd
    full = -(-width // LANES) * LANES
    ext_r = rows + 2 * HALO
    ck, nblk = comps * 8, rows // 8
    third = -(-bands // 24) * 8
    ku = -(-(cols + 2 * HALO) // 16) * 16
    kw = -(-(nc * cols + 2 * RAD) // 16) * 16

    pad_own = -(-own // 16) * 16

    def vm(*shape, dtype=BF):
        return pltpu.VMEM(shape, dtype)

    dma = pltpu.SemaphoreType.DMA
    scratch = [
        vm(2, own * RAD, width),
        vm(4, pad_own, 256),
        vm(own, 8, LANES, dtype=F32),
        vm(ck, LANES, dtype=F32),
        vm(2 * pad_own, LANES, dtype=F32),
        vm(2, 4 * rows, full, dtype=F32),
        vm(2, own * RAD, width),
        vm(nbd, 2, pad_own, 256),
        vm(2, bands, 256, dtype=F32),
        vm(own // 4, 4 * rows, 256),
        vm(own, kw, 256),
        vm(ny, own, rows, 256, dtype=F32),
        vm(ny, nblk, ck, LANES, dtype=F32),
        vm(ny, nblk, ck, LANES),
        vm(ny, nblk, ck, LANES),
        vm(ny - 1, 3, ck, LANES),
        vm(ny - 1, 3, ck, LANES),
        vm(bands, ku, LANES),
        vm(third, 3 * rows, 256),
        vm(bands * 8, ck),
        vm(ck, bands * 8),
        vm(ck, 256),
        vm(bands, ext_r, 256),
        vm(3 * third, ext_r, LANES),
        vm(3 * third, rows, LANES, dtype=F32),
        vm(bands // 8, LANES, LANES, dtype=F32),
        vm(2, ext_r // 8, ck, LANES),
        vm(2, 2, 3, ck, LANES),
        vm(2, 2, 3, ck, LANES),
        vm(3, nblk, ck, LANES, dtype=F32),
        vm(2, 8, LANES, dtype=F32),
        vm(2, max(nbd, nx * nz), 8, LANES, dtype=F32),
        vm(2, 2, 2, ck, LANES),
        vm(2, 2, 2, ck, LANES),
        dma((2, 2, 2)),
        dma((2, nbd - 1, 2)),
        dma((2, ny)),
        dma((2, ny - 1)),
        dma((2, 4)),
        dma((2, 2, 6)),
        dma((2, nbd + nx * nz - 2)),
    ]
    vmem = pl.BlockSpec(memory_space=pltpu.VMEM)
    both = pl.pallas_call(
        functools.partial(kernel, (cols, sizes)),
        out_shape=jax.ShapeDtypeStruct((2, comps, rows, LANES), F32),
        in_specs=[vmem] * 5,
        out_specs=vmem,
        scratch_shapes=scratch,
        compiler_params=pltpu.CompilerParams(
            collective_id=0, has_side_effects=True, vmem_limit_bytes=67043328
        ),
    )(observed, row_taps, col_taps, spectral_basis.T, ridge_weights[None, :])
    return both[0, :, :, :cols], both[1, :, :, :cols]


def solution(mesh):
    sizes = (4, 2, 4, 4)
    split = Mesh(mesh.devices.reshape(sizes), AXES)
    placed = (P(BAND, ROW, None), P(BAND, None), P(BAND, None), P(), P())

    def whole(observed, row_taps, col_taps, spectral_basis, ridge_weights):
        _, height, width = observed.shape
        return jax.shard_map(
            functools.partial(local, height, width, sizes),
            mesh=split,
            in_specs=placed,
            out_specs=(P(None, ROW, BAND), P(None, ROW, BAND)),
            check_vma=False,
        )(observed, row_taps, col_taps, spectral_basis, ridge_weights)

    return whole
```

```python
import functools

import jax
import jax.numpy as jnp
from jax import lax
from jax.experimental import pallas as pl
from jax.experimental.pallas import tpu as pltpu
from jax.sharding import Mesh
from jax.sharding import PartitionSpec as P

AXES = ("band_0", "band_1", "row_0", "row_1")
BAND = ("band_0", "band_1")
ROW = ("row_0", "row_1")
TAPS = 25
RAD = 12
HALO = 24
LANES = 128
SLOT = 64
BF = jnp.bfloat16
F32 = jnp.float32


def iota(shape, dim):
    return lax.broadcasted_iota(jnp.int32, shape, dim)


def mm(a, b):
    return lax.dot_general(a, b, (((1,), (0,)), ((), ())), preferred_element_type=F32)


def halves(v):
    hi = v.astype(BF)
    return hi, (v - hi.astype(F32)).astype(BF)


def onehot(mask):
    return jnp.where(mask, 1.0, 0.0)


def staircase(line, rows, shift):
    step = pltpu.roll(jnp.broadcast_to(line, (8, LANES)), 0, 1, stride=1, stride_axis=0)
    tiles = []
    for g in range(rows // 8):
        turn = (shift + 8 * g) % LANES
        tiles.append(pltpu.roll(step, turn, 1) if turn else step)
    return jnp.concatenate(tiles, axis=0)


def kernel(
    dims, obs, row_taps, col_taps, basis_t, ridge_in,
    out,
    edges, feats, taps, ridge, raw, vpad, edge_in, line_in, lines, rows_adj, cols_adj, zed, keep, out_a, in_a, out_b, in_b,
    tt, rr, e8, p8, p8_own, spec, mid, fin, work, ext, pack, pack_in, vec, red_src, red_in, tight, tight_in,
    edge_sem, line_sem, a_sem, b_sem, row_sem, col_sem, red_sem,
):
    cols, sizes = dims
    ny, nc, nx, nz = sizes
    nbd, nrow = ny * nc, nx * nz
    y, core = lax.axis_index("band_0"), lax.axis_index("band_1")
    x, z = lax.axis_index("row_0"), lax.axis_index("row_1")
    j, i_row = y * nc + core, x * nz + z
    own, rows, full = obs.shape
    comps, bands = basis_t.shape
    ext_r = rows + 2 * HALO
    nblk = rows // 8
    ck = comps * 8
    ku = tt.shape[1]
    first, last = j == 0, j == nbd - 1
    top_dev, low_dev = i_row == 0, i_row == nrow - 1

    def at_band(jj):
        return (jj // nc, lax.rem(jj, nc), x, z)

    def at_row(ii):
        return (y, core, ii // nz, lax.rem(ii, nz))

    up = at_row(lax.rem(i_row + nrow - 1, nrow))
    down = at_row(lax.rem(i_row + 1, nrow))
    left = at_band(lax.rem(j + nbd - 1, nbd))
    right = at_band(lax.rem(j + 1, nbd))
    partner = (y, 1 - core, x, z)
    peers = [at_band(lax.rem(j + s, nbd)) for s in range(1, nbd)]
    peers_r = [at_row(lax.rem(i_row + s, nrow)) for s in range(1, nrow)]


    def corner(di, dj):
        ii, jj = lax.rem(i_row + nrow + di, nrow), lax.rem(j + nbd + dj, nbd)
        return (jj // nc, lax.rem(jj, nc), ii // nz, lax.rem(ii, nz))

    corners = {(di, dj): corner(di, dj) for di in (-1, 1) for dj in (-1, 1)}

    barrier = pltpu.get_barrier_semaphore()
    everyone = peers + peers_r + list(corners.values())
    for d in everyone:
        pl.semaphore_signal(barrier, inc=1, device_id=d, device_id_type=pl.DeviceIdType.MESH)

    def pack_edges(g, carry):
        sl = pl.ds(pl.multiple_of(4 * RAD * g, 16), 4 * RAD)
        v = obs[pl.ds(4 * g, 4)].astype(F32)
        for k, lo in enumerate((0, rows - RAD)):
            slab = jnp.concatenate([v[q, lo : lo + RAD] for q in range(4)], axis=0)
            edges[k, sl, :] = slab.astype(BF)
        return carry

    lax.fori_loop(0, own // 4, pack_edges, 0)
    pl.semaphore_wait(barrier, len(everyone))

    def remote(src, dst, send, recv, device):
        return pltpu.make_async_remote_copy(
            src_ref=src, dst_ref=dst, send_sem=send, recv_sem=recv,
            device_id=device, device_id_type=pl.DeviceIdType.MESH,
        )

    early = (own // 4 + 1) // 2
    edge_copies = []
    for part, sl in enumerate((pl.ds(0, 4 * RAD * early), pl.ds(4 * RAD * early, RAD * own - 4 * RAD * early))):
        a = remote(edges.at[0, sl], edge_in.at[1, sl], edge_sem.at[0, part, 0], edge_sem.at[1, part, 0], up)
        b = remote(edges.at[1, sl], edge_in.at[0, sl], edge_sem.at[0, part, 1], edge_sem.at[1, part, 1], down)
        a.start()
        b.start()
        edge_copies.append((a, b))

    pad_own = feats.shape[1]
    raw[...] = jnp.zeros_like(raw)
    raw[:own, :TAPS] = col_taps[...]
    raw[pad_own : pad_own + own, :TAPS] = row_taps[...]
    t = raw[...]
    t_hi, t_lo = halves(t)
    gr, gp = iota((LANES, 640), 0), iota((LANES, 640), 1)
    g1 = (gp * 5243) >> 17
    g1, g2 = onehot(gr == g1).astype(BF), onehot(gr == gp - TAPS * g1).astype(BF)
    prod = (mm(t_hi, g1) + mm(t_lo, g1)) * (mm(t_hi, g2) + mm(t_lo, g2))
    p_hi, p_lo = halves(prod)
    pp, f = iota((640, 256), 0), iota((640, 256), 1)
    m1 = (pp * 5243) >> 17
    m2 = pp - TAPS * m1
    fe = f - SLOT
    fx = (fe * 5462) >> 16
    fy = fe - RAD * fx
    lag = (f < 2 * TAPS - 1) & (m2 - m1 + TAPS - 1 == f)
    edge = (fe >= 0) & (fe < RAD * RAD)
    for k, cut in enumerate((
        (m1 - fx == m2 - fy) & (m1 - fx > RAD) & (m1 < TAPS),
        (m1 + fx == m2 + fy) & (m1 + fx < RAD),
    )):
        sel = onehot(lag | (edge & cut)).astype(BF)
        v = (mm(p_hi, sel) + mm(p_lo, sel)).astype(BF)
        feats[k] = v[:pad_own]
        feats[2 + k] = v[pad_own:]
    flip = onehot(iota((LANES, LANES), 0) + iota((LANES, LANES), 1) == TAPS - 1).astype(BF)
    taps[:, 0:1, :] = t[:own].reshape(own, 1, LANES)
    taps[:, 1:2, :] = mm(t_hi, flip)[pad_own : pad_own + own].reshape(own, 1, LANES)

    line_copies = []
    row_kind = jnp.where(low_dev, 3, 2)
    for s in range(1, nbd):
        dest = lax.rem(j + s, nbd)
        for k, kind in enumerate((jnp.where(dest == nbd - 1, 1, 0), row_kind)):
            c = remote(
                feats.at[kind], line_in.at[j, k], line_sem.at[0, s - 1, k], line_sem.at[1, s - 1, k], at_band(dest)
            )
            c.start()
            line_copies.append(c)
    line_in[j, 0] = feats[jnp.where(last, 1, 0)]
    line_in[j, 1] = feats[row_kind]

    r, l = iota((rows, LANES), 0), iota((rows, LANES), 1)

    def own_rows(g, carry):
        for q in range(4):
            line = taps[4 * g + q][1:2]
            d = l - rows * q + RAD - r
            m = (d >= 0) & (d < TAPS) & (l >= rows * q) & (l < rows * (q + 1))
            mine = jnp.where(m, staircase(line, rows, rows * q - RAD), 0.0)
            k = l - RAD * q
            d = k - r
            m = (d >= 0) & (d < TAPS) & (k >= 0) & (k < RAD)
            above = jnp.where(m, staircase(line, rows, RAD * q), 0.0)
            k = l - 4 * RAD - RAD * q
            d = k + rows + RAD - r
            m = (d >= 0) & (d < TAPS) & (k >= 0) & (k < RAD)
            below = jnp.where(m, staircase(line, rows, 4 * RAD + RAD * q - RAD - rows), 0.0)
            rows_adj[g, rows * q : rows * (q + 1), :LANES] = mine.astype(BF)
            rows_adj[g, rows * q : rows * (q + 1), LANES:] = (above + below).astype(BF)
        return carry

    lax.fori_loop(0, own // 4, own_rows, 0)

    kw = cols_adj.shape[1]
    w, o = iota((kw, LANES), 0), iota((kw, LANES), 1)

    def own_cols(b, carry):
        line = taps[b][0:1]
        for k in range(2):
            d = w - o - cols * k
            m = (d >= 0) & (d < TAPS) & (o < cols)
            t = jnp.where(m, staircase(line, kw, -HALO - cols * k), 0.0)
            cols_adj[b, :, LANES * k : LANES * (k + 1)] = t.astype(BF)
        return carry

    lax.fori_loop(0, own, own_cols, 0)

    spread = onehot(iota((comps, ck), 0) == (iota((comps, ck), 1) >> 3)).astype(BF)
    wide = lax.dot_general(basis_t[...], spread, (((0,), (0,)), ((), ())), preferred_element_type=F32)
    step = bands // 4
    er, el = iota((8 * step, ck), 0), iota((8 * step, ck), 1)
    for c in range(4):
        v = jnp.broadcast_to(wide[step * c : step * (c + 1)][:, None, :], (step, 8, ck)).reshape(8 * step, ck)
        e8[8 * step * c : 8 * step * (c + 1)] = jnp.where((er & 7) == (el & 7), v, 0.0).astype(BF)
    tall = onehot(iota((ck, comps), 1) == (iota((ck, comps), 0) >> 3)).astype(BF)
    tall = mm(tall, basis_t[...]).astype(BF)
    br, bl = iota((bands, 256), 0), iota((bands, 256), 1)
    same = (iota((ck, 256), 0) & 7) == (iota((ck, 256), 1) & 7)
    kr, kl = iota((ck, comps), 0), iota((ck, comps), 1)
    ridge_col = jnp.sum(jnp.where(kl == (kr >> 3), ridge_in[...], 0.0), axis=1, keepdims=True)
    ridge[...] = jnp.broadcast_to(ridge_col, (ck, LANES))
    vpad[...] = jnp.zeros_like(vpad)

    def widen(start):
        return jnp.where(same, mm(tall, onehot(br == start + (bl >> 3)).astype(BF)), 0.0).astype(BF)

    for c in range(bands // 32):
        p8[:, 256 * c : 256 * (c + 1)] = widen(32 * c)
    p8_own[...] = widen(own * j)

    for c in line_copies:
        c.wait()
    for k in range(2):
        for jj in range(nbd):
            lines[k, own * jj : own * (jj + 1)] = line_in[jj, k][:own].astype(F32)
    groups = bands // 8
    wide_n = 16 * LANES

    def shifted(depth, hit, edge_hit):
        f, n = iota((depth, wide_n), 0), iota((1, wide_n), 1)
        s = onehot(f == hit(n))
        if edge_hit is not None:
            s = s - onehot(f == edge_hit(n))
        return s.astype(BF)

    def unfold(k, depth, sel):
        res = mm(lines[k, :, :depth].astype(BF), sel)
        for t in range(16):
            work[:, 8 * t : 8 * (t + 1), :] = res[:, LANES * t : LANES * (t + 1)].reshape(groups, 8, LANES)

    def tt_pair(p, carry, depth):
        def hit(n):
            a, b = 16 * p + (n >> 7), n & 127
            return jnp.where((b < cols) & (a < cols + 2 * HALO) & (a - b <= 2 * HALO), a - b, -1)

        def edge_hit(n):
            a, b = 16 * p + (n >> 7) - HALO, n & 127
            a, b = jnp.where(last, cols - 1 - a, a), jnp.where(last, cols - 1 - b, b)
            ok = (first | last) & (a >= 0) & (a < RAD) & (b >= 0) & (b < RAD)
            return jnp.where(ok, SLOT + RAD * a + b, -1)

        unfold(0, depth, shifted(depth, hit, edge_hit if depth > SLOT else None))

        def place(g, c):
            for s in range(8):
                v = work[g, pl.ds(s, 16, stride=8), :]
                tt[8 * g + s, pl.ds(pl.multiple_of(16 * p, 16), 16), :] = v.astype(BF)
            return c

        lax.fori_loop(0, groups, place, 0)
        return carry

    third = rr.shape[0]
    lane16 = iota((16, LANES), 1)

    def rr_pair(p, carry):
        def row_of(n):
            b = n & 127
            return jnp.where(b < rows, b + HALO, jnp.where(b < rows + HALO, b - rows, b))

        def hit(n):
            a, b = 16 * p + (n >> 7), row_of(n)
            return jnp.where((b < ext_r) & (b >= a) & (b - a <= 2 * HALO), b - a, -1)

        def edge_hit(n):
            a, b = 16 * p + (n >> 7), row_of(n) - HALO
            a, b = jnp.where(low_dev, rows - 1 - a, a), jnp.where(low_dev, rows - 1 - b, b)
            ok = (top_dev | low_dev) & (a >= 0) & (a < RAD) & (b >= 0) & (b < RAD)
            return jnp.where(ok, SLOT + RAD * a + b, -1)

        unfold(1, 256, shifted(256, hit, edge_hit))
        for q in range(3):
            lo = ext_r * q

            def place(g, c):
                for s in range(8):
                    v = work[g, pl.ds(s, 16, stride=8), :]
                    if lo % LANES:
                        v = pltpu.roll(v, lo % LANES, 1)
                    t0 = v if lo + ext_r <= LANES else jnp.where(lane16 >= lo, v, 0.0)
                    t1 = v if lo >= LANES else jnp.where(lane16 < lo + ext_r - LANES, v, 0.0)
                    at = (8 * g + s - third * q, pl.ds(pl.multiple_of(rows * q + 16 * p, 16), 16))
                    rr[at + (slice(0, LANES),)] = t0.astype(BF)
                    rr[at + (slice(LANES, 2 * LANES),)] = t1.astype(BF)
                return c

            lax.fori_loop(third * q // 8, min(third * (q + 1), bands) // 8, place, 0)
        return carry

    lax.fori_loop(0, ku // 48, functools.partial(tt_pair, depth=SLOT), 0)

    above_ok, below_ok = i_row > 0, i_row < nrow - 1

    def adjoint(g):
        e = slice(4 * RAD * g, 4 * RAD * (g + 1))
        above = edge_in[0, e]
        below = edge_in[1, e]
        mine = obs[4 * g : 4 * g + 4].reshape(4 * rows, full)
        above = jnp.where(above_ok, above, jnp.zeros_like(above))
        below = jnp.where(below_ok, below, jnp.zeros_like(below))
        v = mm(rows_adj[g][:, : 4 * rows + 8 * RAD], jnp.concatenate([mine, above, below], axis=0))
        vpad[g % 2, :, :full] = v
        v = vpad[g % 2]
        wins = []
        for k in range(ny):
            start = nc * cols * k - RAD
            wins.append(pltpu.roll(v, (v.shape[1] - start) % v.shape[1], 1)[:, :256].astype(BF))
        for q in range(4):
            u = jnp.concatenate([t[rows * q : rows * (q + 1)] for t in wins], axis=0)
            u = mm(u[:, :kw], cols_adj[4 * g + q])
            for k in range(ny):
                zed[k, 4 * g + q] = u[rows * k : rows * (k + 1)]

    for g in range(own // 4):
        if g in (0, early):
            for c in edge_copies[g // max(early, 1)]:
                c.wait()
        adjoint(g)

    lane_k = iota((ck, LANES), 1)
    cut = LANES - cols
    offsets = [s for s in (2, 1, 3, 0) if s < ny]
    a_copies, b_copies = [], []

    def merge(idx):
        a_copies[idx].wait()
        done = idx == len(offsets) - 1

        def add(i):
            return keep[idx, i] + in_a[idx, i].astype(F32)

        if done:
            for i in range(nblk):
                vec[0, i] = add(i)
        else:
            b = pltpu.roll(add(1), cols, 1)
            out_b[idx, 0] = jnp.where(lane_k < cols, add(0), b).astype(BF)
            out_b[idx, 1] = jnp.where(lane_k < cols - cut, b, pltpu.roll(add(2), cols - cut, 1)).astype(BF)
            out_b[idx, 2] = add(3).astype(BF)
        if not done:
            dest = (lax.rem(y + offsets[idx], ny), core, x, z)
            c = remote(out_b.at[idx], in_b.at[idx], b_sem.at[0, idx], b_sem.at[1, idx], dest)
            c.start()
            b_copies.append(c)

    for idx, off in enumerate(offsets):
        k = lax.rem(y + off, ny)

        for i in range(nblk):
            v = zed[k, :, 8 * i : 8 * (i + 1), :].reshape(own * 8, 256).astype(BF)
            v = mm(p8_own[:, : own * 8], v)
            lo, hi = v[:, :LANES], v[:, LANES:]
            keep[idx, i] = jnp.where(core == 0, lo, hi)
            out_a[idx, i] = jnp.where(core == 0, hi, lo).astype(BF)
        c = remote(out_a.at[idx], in_a.at[idx], a_sem.at[0, idx], a_sem.at[1, idx], partner)
        c.start()
        a_copies.append(c)
        if idx:
            merge(idx - 1)
    merge(len(offsets) - 1)
    lax.fori_loop(ku // 48, ku // 16, functools.partial(tt_pair, depth=SLOT), 0)

    @pl.when(first | last)
    def _():
        p0 = jnp.where(first, HALO // 16, (cols + RAD - 1) // 16)
        lax.fori_loop(p0, p0 + 2, functools.partial(tt_pair, depth=256), 0)

    mid[pl.ds(bands, mid.shape[0] - bands)] = jnp.zeros((mid.shape[0] - bands, ext_r, LANES), BF)
    for c in b_copies:
        c.wait()
    a, b, c = (sum(in_b[idx, t].astype(F32) for idx in range(ny - 1)) for t in range(3))
    b1 = jnp.where(lane_k < cut, pltpu.roll(a, cut, 1), pltpu.roll(b, cut, 1))
    for i, v in enumerate((a, b1, pltpu.roll(b, 2 * cut, 1), c)):
        vec[0, i] = vec[0, i] + jnp.where(lane_k < cols, v, 0.0)

    chunk = ck // 4
    lane_c = iota((chunk, LANES), 1)

    def normal(n, carry):
        def stage(i, c):
            ext[n, i] = vec[n, i].astype(BF)
            return c

        lax.fori_loop(0, nblk, stage, 0)
        for k, lo in enumerate((0, nblk - 3)):
            a, b, c = (vec[n, lo + q] for q in range(3))
            b = pltpu.roll(b, cols, 1)
            c = pltpu.roll(c, cols - cut, 1)
            tight[n, k, 0] = jnp.where(lane_k < cols, a, b).astype(BF)
            tight[n, k, 1] = jnp.where(lane_k < cols - cut, b, c).astype(BF)
        r_up = remote(tight.at[n, 0], tight_in.at[n, 1], row_sem.at[n, 0], row_sem.at[n, 2], up)
        r_down = remote(tight.at[n, 1], tight_in.at[n, 0], row_sem.at[n, 1], row_sem.at[n, 3], down)

        def packing(t, blocks):
            def part(c, cc):
                sl = pl.ds(pl.multiple_of(chunk * c, chunk), chunk)
                a = jnp.zeros((chunk, LANES), F32)
                b = a
                for g, blk in enumerate(blocks):
                    v = ext[n, blk, sl, :].astype(F32)
                    m = (lane_c >= HALO * g) & (lane_c < HALO * (g + 1))
                    a = jnp.where(m, pltpu.roll(v, HALO * g, 1) if g else v, a)
                    b = jnp.where(m, pltpu.roll(v, (HALO * g - cols + HALO) % LANES, 1), b)
                pack[n, 0, t, sl, :] = a.astype(BF)
                pack[n, 1, t, sl, :] = b.astype(BF)
                return cc

            lax.fori_loop(0, ck // chunk, part, 0)

        def to(src, dst, k, device):
            c = remote(pack.at[(n,) + src], pack_in.at[(n,) + dst], col_sem.at[n, 0, k], col_sem.at[n, 1, k], device)
            c.start()
            return c

        def block(blk, t, g):
            mine = pltpu.roll(ext[n, blk].astype(F32), HALO, 1)
            a = pltpu.roll(pack_in[n, 0, t].astype(F32), (LANES - HALO * g) % LANES, 1)
            b = pltpu.roll(pack_in[n, 1, t].astype(F32), (cols + HALO - HALO * g) % LANES, 1)
            a_ok, b_ok = jnp.logical_not(first), jnp.logical_not(last)
            if blk >= nblk:
                inside = jnp.logical_not(top_dev if blk < nblk + 3 else low_dev)
                a_ok, b_ok = a_ok & inside, b_ok & inside
                mine = jnp.where(inside, mine, 0.0)
            a = jnp.where(a_ok, a, 0.0)
            b = jnp.where(b_ok, b, 0.0)
            t0 = jnp.where(lane_k < HALO, a, jnp.where(lane_k < HALO + cols, mine, b))
            t1 = jnp.where(lane_k < cols + 2 * HALO - LANES, b, 0.0)
            return jnp.concatenate([t0, t1], axis=1).astype(BF)

        def expand(row, x0, x1):
            for m in range(4):
                e = e8[8 * step * m : 8 * step * (m + 1)]
                y0 = mm(e, x0).reshape(step, 8, 256)
                y1 = mm(e, x1).reshape(step, 8, 256)
                v = jnp.concatenate([y0, y1], axis=1).astype(BF)
                spec[step * m : step * (m + 1), row : row + 16, :] = v

        def columns(lo, count):
            for b in range(bands):
                mid[b, lo : lo + count] = mm(spec[b, lo : lo + count][:, :ku], tt[b]).astype(BF)

        packing(0, range(nblk))
        own_edges = [to((0, 0), (1, 0), 0, left), to((1, 0), (0, 0), 1, right)]
        r_up.start()
        r_down.start()
        packing(1, range(nblk - 3, nblk))
        packing(2, range(3))
        halo_edges = [
            to((1, 1), (0, 1), 2, corners[1, 1]),
            to((0, 1), (1, 1), 3, corners[1, -1]),
            to((1, 2), (0, 2), 4, corners[-1, 1]),
            to((0, 2), (1, 2), 5, corners[-1, -1]),
        ]
        for c in own_edges:
            c.wait()
        for i in range(nblk // 2):
            expand(16 * i, block(2 * i, 0, 2 * i), block(2 * i + 1, 0, 2 * i + 1))
        columns(0, rows)

        @pl.when(n == 0)
        def _():
            lax.fori_loop(0, rows // 16, rr_pair, 0)

        r_up.wait()
        r_down.wait()
        for k in range(2):
            a, b = tight_in[n, k, 0].astype(F32), tight_in[n, k, 1].astype(F32)
            ext[n, nblk + 3 * k] = tight_in[n, k, 0]
            b1 = jnp.where(lane_k < cut, pltpu.roll(a, cut, 1), pltpu.roll(b, cut, 1))
            ext[n, nblk + 3 * k + 1] = b1.astype(BF)
            ext[n, nblk + 3 * k + 2] = pltpu.roll(b, 2 * cut, 1).astype(BF)
        for c in halo_edges:
            c.wait()
        for i in range(3):
            k0, k1 = 2 * i, 2 * i + 1
            expand(
                rows + 16 * i,
                block(nblk + k0, 1 + k0 // 3, k0 % 3),
                block(nblk + k1, 1 + k1 // 3, k1 % 3),
            )
        columns(rows, ext_r - rows)

        for t in range(third):
            v = jnp.concatenate([mid[t], mid[third + t], mid[2 * third + t]], axis=0)
            v = mm(rr[t][:, : 3 * ext_r], v)
            for k in range(3):
                fin[third * k + t] = v[rows * k : rows * (k + 1)]

        for i in range(nblk):
            v = fin[:bands, 8 * i : 8 * (i + 1), :].reshape(bands * 8, LANES).astype(BF)
            vec[n + 1, i] = mm(p8[...], v) + ridge[...] * vec[n, i]
        return carry

    lax.fori_loop(0, 2, normal, 0)

    def products(i, sums):
        a, b, c = vec[0, i], vec[1, i], vec[2, i]
        parts = [a * a, a * b, b * b, a * c, b * c]
        return tuple(s + jnp.sum(v.reshape(comps, 8, LANES), axis=0) for s, v in zip(sums, parts))

    zero = jnp.zeros((8, LANES), F32)
    sums = lax.fori_loop(0, nblk, products, (zero,) * 5)
    total = jnp.concatenate([jnp.sum(v, axis=0, keepdims=True) for v in sums] + [jnp.zeros((3, LANES), F32)], axis=0)
    at = 0
    for level, (group, place, count) in enumerate(((peers, j, nbd), (peers_r, i_row, nrow))):
        red_src[level] = total
        red_in[level, place] = total
        copies = []
        for d in group:
            c = remote(red_src.at[level], red_in.at[level, place], red_sem.at[0, at], red_sem.at[1, at], d)
            c.start()
            copies.append(c)
            at += 1
        for c in copies:
            c.wait()
        total = red_in[level, 0]
        for k in range(1, count):
            total = total + red_in[level, k]
    tot = jnp.sum(total, axis=1, keepdims=True)
    r00, r01, r11, r02, r12 = [tot[k : k + 1] for k in range(5)]
    alpha = r00 / r01
    new = r00 - 2.0 * alpha * r01 + alpha * alpha * r11
    gain = 1.0 + new / r00
    curve = gain * gain * r01 - alpha * gain * (r11 + r02) + alpha * alpha * r12
    alpha2 = new / curve

    def finish(i, carry):
        a, b, c = vec[0, i], vec[1, i], vec[2, i]
        xs = alpha * a + alpha2 * (gain * a - alpha * b)
        rs = (a - alpha * b) - alpha2 * (gain * b - alpha * c)
        sl = pl.ds(pl.multiple_of(8 * i, 8), 8)
        out[0, :, sl, :] = xs.reshape(comps, 8, LANES)
        out[1, :, sl, :] = rs.reshape(comps, 8, LANES)
        return carry

    lax.fori_loop(0, nblk, finish, 0)


def local(height, width, sizes, observed, row_taps, col_taps, spectral_basis, ridge_weights):
    own, rows, _ = observed.shape
    bands, comps = spectral_basis.shape
    ny, nc, nx, nz = sizes
    nbd = ny * nc
    cols = width // nbd
    full = -(-width // LANES) * LANES
    ext_r = rows + 2 * HALO
    ck, nblk = comps * 8, rows // 8
    third = -(-bands // 24) * 8
    ku = -(-(cols + 2 * HALO) // 16) * 16
    kw = -(-(nc * cols + 2 * RAD) // 16) * 16

    pad_own = -(-own // 16) * 16

    def vm(*shape, dtype=BF):
        return pltpu.VMEM(shape, dtype)

    dma = pltpu.SemaphoreType.DMA
    scratch = [
        vm(2, own * RAD, width),
        vm(4, pad_own, 256),
        vm(own, 8, LANES, dtype=F32),
        vm(ck, LANES, dtype=F32),
        vm(2 * pad_own, LANES, dtype=F32),
        vm(2, 4 * rows, full, dtype=F32),
        vm(2, own * RAD, width),
        vm(nbd, 2, pad_own, 256),
        vm(2, bands, 256, dtype=F32),
        vm(own // 4, 4 * rows, 256),
        vm(own, kw, 256),
        vm(ny, own, rows, 256, dtype=F32),
        vm(ny, nblk, ck, LANES, dtype=F32),
        vm(ny, nblk, ck, LANES),
        vm(ny, nblk, ck, LANES),
        vm(ny - 1, 3, ck, LANES),
        vm(ny - 1, 3, ck, LANES),
        vm(bands, ku, LANES),
        vm(third, 3 * rows, 256),
        vm(bands * 8, ck),
        vm(ck, bands * 8),
        vm(ck, 256),
        vm(bands, ext_r, 256),
        vm(3 * third, ext_r, LANES),
        vm(3 * third, rows, LANES, dtype=F32),
        vm(bands // 8, LANES, LANES, dtype=F32),
        vm(2, ext_r // 8, ck, LANES),
        vm(2, 2, 3, ck, LANES),
        vm(2, 2, 3, ck, LANES),
        vm(3, nblk, ck, LANES, dtype=F32),
        vm(2, 8, LANES, dtype=F32),
        vm(2, max(nbd, nx * nz), 8, LANES, dtype=F32),
        vm(2, 2, 2, ck, LANES),
        vm(2, 2, 2, ck, LANES),
        dma((2, 2, 2)),
        dma((2, nbd - 1, 2)),
        dma((2, ny)),
        dma((2, ny - 1)),
        dma((2, 4)),
        dma((2, 2, 6)),
        dma((2, nbd + nx * nz - 2)),
    ]
    vmem = pl.BlockSpec(memory_space=pltpu.VMEM)
    both = pl.pallas_call(
        functools.partial(kernel, (cols, sizes)),
        out_shape=jax.ShapeDtypeStruct((2, comps, rows, LANES), F32),
        in_specs=[vmem] * 5,
        out_specs=vmem,
        scratch_shapes=scratch,
        compiler_params=pltpu.CompilerParams(
            collective_id=0, has_side_effects=True, vmem_limit_bytes=67043328
        ),
    )(observed, row_taps, col_taps, spectral_basis.T, ridge_weights[None, :])
    return both[0, :, :, :cols], both[1, :, :, :cols]


def solution(mesh):
    sizes = (4, 2, 4, 4)
    split = Mesh(mesh.devices.reshape(sizes), AXES)
    placed = (P(BAND, ROW, None), P(BAND, None), P(BAND, None), P(), P())

    def whole(observed, row_taps, col_taps, spectral_basis, ridge_weights):
        _, height, width = observed.shape
        return jax.shard_map(
            functools.partial(local, height, width, sizes),
            mesh=split,
            in_specs=placed,
            out_specs=(P(None, ROW, BAND), P(None, ROW, BAND)),
            check_vma=False,
        )(observed, row_taps, col_taps, spectral_basis, ridge_weights)

    return whole
```

```python
import functools

import jax
import jax.numpy as jnp
from jax import lax
from jax.experimental import pallas as pl
from jax.experimental.pallas import tpu as pltpu
from jax.sharding import Mesh
from jax.sharding import PartitionSpec as P

AXES = ("band_0", "band_1", "row_0", "row_1")
BAND = ("band_0", "band_1")
ROW = ("row_0", "row_1")
TAPS = 25
RAD = 12
HALO = 24
LANES = 128
SLOT = 64
BF = jnp.bfloat16
F32 = jnp.float32


def iota(shape, dim):
    return lax.broadcasted_iota(jnp.int32, shape, dim)


def mm(a, b):
    return lax.dot_general(a, b, (((1,), (0,)), ((), ())), preferred_element_type=F32)


def halves(v):
    hi = v.astype(BF)
    return hi, (v - hi.astype(F32)).astype(BF)


def onehot(mask):
    return jnp.where(mask, 1.0, 0.0)


def staircase(line, rows, shift):
    step = pltpu.roll(jnp.broadcast_to(line, (8, LANES)), 0, 1, stride=1, stride_axis=0)
    tiles = []
    for g in range(rows // 8):
        turn = (shift + 8 * g) % LANES
        tiles.append(pltpu.roll(step, turn, 1) if turn else step)
    return jnp.concatenate(tiles, axis=0)


def kernel(
    dims, obs_in, row_taps, col_taps, basis_t, ridge_in,
    out,
    obs, obs_sem, edges, feats, taps, ridge, raw, vpad, edge_in, line_in, lines, rows_adj, cols_adj, zed, keep, out_a, in_a, out_b, in_b,
    tt, rr, e8, p8, p8_own, spec, mid, fin, work, ext, pack, pack_in, vec, red_src, red_in, tight, tight_in,
    edge_sem, line_sem, a_sem, b_sem, row_sem, col_sem, red_sem,
):
    cols, sizes = dims
    ny, nc, nx, nz = sizes
    nbd, nrow = ny * nc, nx * nz
    y, core = lax.axis_index("band_0"), lax.axis_index("band_1")
    x, z = lax.axis_index("row_0"), lax.axis_index("row_1")
    j, i_row = y * nc + core, x * nz + z
    own, rows, full = obs.shape
    comps, bands = basis_t.shape
    ext_r = rows + 2 * HALO
    nblk = rows // 8
    ck = comps * 8
    ku = tt.shape[1]
    first, last = j == 0, j == nbd - 1
    top_dev, low_dev = i_row == 0, i_row == nrow - 1

    def at_band(jj):
        return (jj // nc, lax.rem(jj, nc), x, z)

    def at_row(ii):
        return (y, core, ii // nz, lax.rem(ii, nz))

    up = at_row(lax.rem(i_row + nrow - 1, nrow))
    down = at_row(lax.rem(i_row + 1, nrow))
    left = at_band(lax.rem(j + nbd - 1, nbd))
    right = at_band(lax.rem(j + 1, nbd))
    partner = (y, 1 - core, x, z)
    peers = [at_band(lax.rem(j + s, nbd)) for s in range(1, nbd)]
    peers_r = [at_row(lax.rem(i_row + s, nrow)) for s in range(1, nrow)]


    def corner(di, dj):
        ii, jj = lax.rem(i_row + nrow + di, nrow), lax.rem(j + nbd + dj, nbd)
        return (jj // nc, lax.rem(jj, nc), ii // nz, lax.rem(ii, nz))

    corners = {(di, dj): corner(di, dj) for di in (-1, 1) for dj in (-1, 1)}

    barrier = pltpu.get_barrier_semaphore()
    everyone = peers + peers_r + list(corners.values())
    for d in everyone:
        pl.semaphore_signal(barrier, inc=1, device_id=d, device_id_type=pl.DeviceIdType.MESH)

    fetch = pltpu.make_async_copy(obs_in, obs, obs_sem)
    fetch.start()
    fetch.wait()

    def pack_edges(g, carry):
        sl = pl.ds(pl.multiple_of(4 * RAD * g, 16), 4 * RAD)
        v = obs[pl.ds(4 * g, 4)].astype(F32)
        for k, lo in enumerate((0, rows - RAD)):
            slab = jnp.concatenate([v[q, lo : lo + RAD] for q in range(4)], axis=0)
            edges[k, sl, :] = slab.astype(BF)
        return carry

    lax.fori_loop(0, own // 4, pack_edges, 0)
    pl.semaphore_wait(barrier, len(everyone))

    def remote(src, dst, send, recv, device):
        return pltpu.make_async_remote_copy(
            src_ref=src, dst_ref=dst, send_sem=send, recv_sem=recv,
            device_id=device, device_id_type=pl.DeviceIdType.MESH,
        )

    early = (own // 4 + 1) // 2
    edge_copies = []
    for part, sl in enumerate((pl.ds(0, 4 * RAD * early), pl.ds(4 * RAD * early, RAD * own - 4 * RAD * early))):
        a = remote(edges.at[0, sl], edge_in.at[1, sl], edge_sem.at[0, part, 0], edge_sem.at[1, part, 0], up)
        b = remote(edges.at[1, sl], edge_in.at[0, sl], edge_sem.at[0, part, 1], edge_sem.at[1, part, 1], down)
        a.start()
        b.start()
        edge_copies.append((a, b))

    pad_own = feats.shape[1]
    raw[...] = jnp.zeros_like(raw)
    raw[:own, :TAPS] = col_taps[...]
    raw[pad_own : pad_own + own, :TAPS] = row_taps[...]
    t = raw[...]
    t_hi, t_lo = halves(t)
    gr, gp = iota((LANES, 640), 0), iota((LANES, 640), 1)
    g1 = (gp * 5243) >> 17
    g1, g2 = onehot(gr == g1).astype(BF), onehot(gr == gp - TAPS * g1).astype(BF)
    prod = (mm(t_hi, g1) + mm(t_lo, g1)) * (mm(t_hi, g2) + mm(t_lo, g2))
    p_hi, p_lo = halves(prod)
    pp, f = iota((640, 256), 0), iota((640, 256), 1)
    m1 = (pp * 5243) >> 17
    m2 = pp - TAPS * m1
    fe = f - SLOT
    fx = (fe * 5462) >> 16
    fy = fe - RAD * fx
    lag = (f < 2 * TAPS - 1) & (m2 - m1 + TAPS - 1 == f)
    edge = (fe >= 0) & (fe < RAD * RAD)
    for k, cut in enumerate((
        (m1 - fx == m2 - fy) & (m1 - fx > RAD) & (m1 < TAPS),
        (m1 + fx == m2 + fy) & (m1 + fx < RAD),
    )):
        sel = onehot(lag | (edge & cut)).astype(BF)
        v = (mm(p_hi, sel) + mm(p_lo, sel)).astype(BF)
        feats[k] = v[:pad_own]
        feats[2 + k] = v[pad_own:]
    flip = onehot(iota((LANES, LANES), 0) + iota((LANES, LANES), 1) == TAPS - 1).astype(BF)
    taps[:, 0:1, :] = t[:own].reshape(own, 1, LANES)
    taps[:, 1:2, :] = mm(t_hi, flip)[pad_own : pad_own + own].reshape(own, 1, LANES)

    line_copies = []
    row_kind = jnp.where(low_dev, 3, 2)
    for s in range(1, nbd):
        dest = lax.rem(j + s, nbd)
        for k, kind in enumerate((jnp.where(dest == nbd - 1, 1, 0), row_kind)):
            c = remote(
                feats.at[kind], line_in.at[j, k], line_sem.at[0, s - 1, k], line_sem.at[1, s - 1, k], at_band(dest)
            )
            c.start()
            line_copies.append(c)
    line_in[j, 0] = feats[jnp.where(last, 1, 0)]
    line_in[j, 1] = feats[row_kind]

    r, l = iota((rows, LANES), 0), iota((rows, LANES), 1)

    def own_rows(g, carry):
        for q in range(4):
            line = taps[4 * g + q][1:2]
            d = l - rows * q + RAD - r
            m = (d >= 0) & (d < TAPS) & (l >= rows * q) & (l < rows * (q + 1))
            mine = jnp.where(m, staircase(line, rows, rows * q - RAD), 0.0)
            k = l - RAD * q
            d = k - r
            m = (d >= 0) & (d < TAPS) & (k >= 0) & (k < RAD)
            above = jnp.where(m, staircase(line, rows, RAD * q), 0.0)
            k = l - 4 * RAD - RAD * q
            d = k + rows + RAD - r
            m = (d >= 0) & (d < TAPS) & (k >= 0) & (k < RAD)
            below = jnp.where(m, staircase(line, rows, 4 * RAD + RAD * q - RAD - rows), 0.0)
            rows_adj[g, rows * q : rows * (q + 1), :LANES] = mine.astype(BF)
            rows_adj[g, rows * q : rows * (q + 1), LANES:] = (above + below).astype(BF)
        return carry

    lax.fori_loop(0, own // 4, own_rows, 0)

    kw = cols_adj.shape[1]
    w, o = iota((kw, LANES), 0), iota((kw, LANES), 1)

    def own_cols(b, carry):
        line = taps[b][0:1]
        for k in range(2):
            d = w - o - cols * k
            m = (d >= 0) & (d < TAPS) & (o < cols)
            t = jnp.where(m, staircase(line, kw, -HALO - cols * k), 0.0)
            cols_adj[b, :, LANES * k : LANES * (k + 1)] = t.astype(BF)
        return carry

    lax.fori_loop(0, own, own_cols, 0)

    spread = onehot(iota((comps, ck), 0) == (iota((comps, ck), 1) >> 3)).astype(BF)
    wide = lax.dot_general(basis_t[...], spread, (((0,), (0,)), ((), ())), preferred_element_type=F32)
    step = bands // 4
    er, el = iota((8 * step, ck), 0), iota((8 * step, ck), 1)
    for c in range(4):
        v = jnp.broadcast_to(wide[step * c : step * (c + 1)][:, None, :], (step, 8, ck)).reshape(8 * step, ck)
        e8[8 * step * c : 8 * step * (c + 1)] = jnp.where((er & 7) == (el & 7), v, 0.0).astype(BF)
    tall = onehot(iota((ck, comps), 1) == (iota((ck, comps), 0) >> 3)).astype(BF)
    tall = mm(tall, basis_t[...]).astype(BF)
    br, bl = iota((bands, 256), 0), iota((bands, 256), 1)
    same = (iota((ck, 256), 0) & 7) == (iota((ck, 256), 1) & 7)
    kr, kl = iota((ck, comps), 0), iota((ck, comps), 1)
    ridge_col = jnp.sum(jnp.where(kl == (kr >> 3), ridge_in[...], 0.0), axis=1, keepdims=True)
    ridge[...] = jnp.broadcast_to(ridge_col, (ck, LANES))
    vpad[...] = jnp.zeros_like(vpad)

    def widen(start):
        return jnp.where(same, mm(tall, onehot(br == start + (bl >> 3)).astype(BF)), 0.0).astype(BF)

    for c in range(bands // 32):
        p8[:, 256 * c : 256 * (c + 1)] = widen(32 * c)
    p8_own[...] = widen(own * j)

    for c in line_copies:
        c.wait()
    for k in range(2):
        for jj in range(nbd):
            lines[k, own * jj : own * (jj + 1)] = line_in[jj, k][:own].astype(F32)
    groups = bands // 8
    wide_n = 16 * LANES

    def shifted(depth, hit, edge_hit):
        f, n = iota((depth, wide_n), 0), iota((1, wide_n), 1)
        s = onehot(f == hit(n))
        if edge_hit is not None:
            s = s - onehot(f == edge_hit(n))
        return s.astype(BF)

    def unfold(k, depth, sel):
        res = mm(lines[k, :, :depth].astype(BF), sel)
        for t in range(16):
            work[:, 8 * t : 8 * (t + 1), :] = res[:, LANES * t : LANES * (t + 1)].reshape(groups, 8, LANES)

    def tt_pair(p, carry, depth):
        def hit(n):
            a, b = 16 * p + (n >> 7), n & 127
            return jnp.where((b < cols) & (a < cols + 2 * HALO) & (a - b <= 2 * HALO), a - b, -1)

        def edge_hit(n):
            a, b = 16 * p + (n >> 7) - HALO, n & 127
            a, b = jnp.where(last, cols - 1 - a, a), jnp.where(last, cols - 1 - b, b)
            ok = (first | last) & (a >= 0) & (a < RAD) & (b >= 0) & (b < RAD)
            return jnp.where(ok, SLOT + RAD * a + b, -1)

        unfold(0, depth, shifted(depth, hit, edge_hit if depth > SLOT else None))

        def place(g, c):
            for s in range(8):
                v = work[g, pl.ds(s, 16, stride=8), :]
                tt[8 * g + s, pl.ds(pl.multiple_of(16 * p, 16), 16), :] = v.astype(BF)
            return c

        lax.fori_loop(0, groups, place, 0)
        return carry

    third = rr.shape[0]
    lane16 = iota((16, LANES), 1)

    def rr_pair(p, carry):
        def row_of(n):
            b = n & 127
            return jnp.where(b < rows, b + HALO, jnp.where(b < rows + HALO, b - rows, b))

        def hit(n):
            a, b = 16 * p + (n >> 7), row_of(n)
            return jnp.where((b < ext_r) & (b >= a) & (b - a <= 2 * HALO), b - a, -1)

        def edge_hit(n):
            a, b = 16 * p + (n >> 7), row_of(n) - HALO
            a, b = jnp.where(low_dev, rows - 1 - a, a), jnp.where(low_dev, rows - 1 - b, b)
            ok = (top_dev | low_dev) & (a >= 0) & (a < RAD) & (b >= 0) & (b < RAD)
            return jnp.where(ok, SLOT + RAD * a + b, -1)

        unfold(1, 256, shifted(256, hit, edge_hit))
        for q in range(3):
            lo = ext_r * q

            def place(g, c):
                for s in range(8):
                    v = work[g, pl.ds(s, 16, stride=8), :]
                    if lo % LANES:
                        v = pltpu.roll(v, lo % LANES, 1)
                    t0 = v if lo + ext_r <= LANES else jnp.where(lane16 >= lo, v, 0.0)
                    t1 = v if lo >= LANES else jnp.where(lane16 < lo + ext_r - LANES, v, 0.0)
                    at = (8 * g + s - third * q, pl.ds(pl.multiple_of(rows * q + 16 * p, 16), 16))
                    rr[at + (slice(0, LANES),)] = t0.astype(BF)
                    rr[at + (slice(LANES, 2 * LANES),)] = t1.astype(BF)
                return c

            lax.fori_loop(third * q // 8, min(third * (q + 1), bands) // 8, place, 0)
        return carry

    slabs = ku // 16
    lax.fori_loop(1, 3, functools.partial(tt_pair, depth=SLOT), 0)

    above_ok, below_ok = i_row > 0, i_row < nrow - 1

    def adjoint(g):
        e = slice(4 * RAD * g, 4 * RAD * (g + 1))
        above = edge_in[0, e]
        below = edge_in[1, e]
        mine = obs[4 * g : 4 * g + 4].reshape(4 * rows, full)
        above = jnp.where(above_ok, above, jnp.zeros_like(above))
        below = jnp.where(below_ok, below, jnp.zeros_like(below))
        v = mm(rows_adj[g][:, : 4 * rows + 8 * RAD], jnp.concatenate([mine, above, below], axis=0))
        vpad[g % 2, :, :full] = v
        v = vpad[g % 2]
        wins = []
        for k in range(ny):
            start = nc * cols * k - RAD
            wins.append(pltpu.roll(v, (v.shape[1] - start) % v.shape[1], 1)[:, :256].astype(BF))
        for q in range(4):
            u = jnp.concatenate([t[rows * q : rows * (q + 1)] for t in wins], axis=0)
            u = mm(u[:, :kw], cols_adj[4 * g + q])
            for k in range(ny):
                zed[k, 4 * g + q] = u[rows * k : rows * (k + 1)]

    for g in range(own // 4):
        if g in (0, early):
            for c in edge_copies[g // max(early, 1)]:
                c.wait()
        adjoint(g)

    lane_k = iota((ck, LANES), 1)
    cut = LANES - cols
    offsets = [s for s in (2, 1, 3, 0) if s < ny]
    a_copies, b_copies = [], []

    def merge(idx):
        a_copies[idx].wait()
        done = idx == len(offsets) - 1

        def add(i):
            return keep[idx, i] + in_a[idx, i].astype(F32)

        if done:
            for i in range(nblk):
                vec[0, i] = add(i)
        else:
            b = pltpu.roll(add(1), cols, 1)
            out_b[idx, 0] = jnp.where(lane_k < cols, add(0), b).astype(BF)
            out_b[idx, 1] = jnp.where(lane_k < cols - cut, b, pltpu.roll(add(2), cols - cut, 1)).astype(BF)
            out_b[idx, 2] = add(3).astype(BF)
        if not done:
            dest = (lax.rem(y + offsets[idx], ny), core, x, z)
            c = remote(out_b.at[idx], in_b.at[idx], b_sem.at[0, idx], b_sem.at[1, idx], dest)
            c.start()
            b_copies.append(c)

    for idx, off in enumerate(offsets):
        k = lax.rem(y + off, ny)

        for i in range(nblk):
            v = zed[k, :, 8 * i : 8 * (i + 1), :].reshape(own * 8, 256).astype(BF)
            v = mm(p8_own[:, : own * 8], v)
            lo, hi = v[:, :LANES], v[:, LANES:]
            keep[idx, i] = jnp.where(core == 0, lo, hi)
            out_a[idx, i] = jnp.where(core == 0, hi, lo).astype(BF)
        c = remote(out_a.at[idx], in_a.at[idx], a_sem.at[0, idx], a_sem.at[1, idx], partner)
        c.start()
        a_copies.append(c)
        if idx:
            merge(idx - 1)
    merge(len(offsets) - 1)
    lax.fori_loop(3, slabs - 1, functools.partial(tt_pair, depth=SLOT), 0)

    @pl.when(first | last)
    def _():
        p0 = jnp.where(first, HALO // 16, (cols + RAD - 1) // 16)
        lax.fori_loop(p0, p0 + 2, functools.partial(tt_pair, depth=256), 0)

    mid[pl.ds(bands, mid.shape[0] - bands)] = jnp.zeros((mid.shape[0] - bands, ext_r, LANES), BF)
    for c in b_copies:
        c.wait()
    a, b, c = (sum(in_b[idx, t].astype(F32) for idx in range(ny - 1)) for t in range(3))
    b1 = jnp.where(lane_k < cut, pltpu.roll(a, cut, 1), pltpu.roll(b, cut, 1))
    for i, v in enumerate((a, b1, pltpu.roll(b, 2 * cut, 1), c)):
        vec[0, i] = vec[0, i] + jnp.where(lane_k < cols, v, 0.0)

    chunk = ck // 4
    lane_c = iota((chunk, LANES), 1)

    def normal(n, carry):
        def stage(i, c):
            ext[n, i] = vec[n, i].astype(BF)
            return c

        lax.fori_loop(0, nblk, stage, 0)
        for k, lo in enumerate((0, nblk - 3)):
            a, b, c = (vec[n, lo + q] for q in range(3))
            b = pltpu.roll(b, cols, 1)
            c = pltpu.roll(c, cols - cut, 1)
            tight[n, k, 0] = jnp.where(lane_k < cols, a, b).astype(BF)
            tight[n, k, 1] = jnp.where(lane_k < cols - cut, b, c).astype(BF)
        r_up = remote(tight.at[n, 0], tight_in.at[n, 1], row_sem.at[n, 0], row_sem.at[n, 2], up)
        r_down = remote(tight.at[n, 1], tight_in.at[n, 0], row_sem.at[n, 1], row_sem.at[n, 3], down)

        def packing(t, blocks):
            def part(c, cc):
                sl = pl.ds(pl.multiple_of(chunk * c, chunk), chunk)
                a = jnp.zeros((chunk, LANES), F32)
                b = a
                for g, blk in enumerate(blocks):
                    v = ext[n, blk, sl, :].astype(F32)
                    m = (lane_c >= HALO * g) & (lane_c < HALO * (g + 1))
                    a = jnp.where(m, pltpu.roll(v, HALO * g, 1) if g else v, a)
                    b = jnp.where(m, pltpu.roll(v, (HALO * g - cols + HALO) % LANES, 1), b)
                pack[n, 0, t, sl, :] = a.astype(BF)
                pack[n, 1, t, sl, :] = b.astype(BF)
                return cc

            lax.fori_loop(0, ck // chunk, part, 0)

        def to(src, dst, k, device):
            c = remote(pack.at[(n,) + src], pack_in.at[(n,) + dst], col_sem.at[n, 0, k], col_sem.at[n, 1, k], device)
            c.start()
            return c

        def block(blk, t, g):
            mine = pltpu.roll(ext[n, blk].astype(F32), HALO, 1)
            a = pltpu.roll(pack_in[n, 0, t].astype(F32), (LANES - HALO * g) % LANES, 1)
            b = pltpu.roll(pack_in[n, 1, t].astype(F32), (cols + HALO - HALO * g) % LANES, 1)
            a_ok, b_ok = jnp.logical_not(first), jnp.logical_not(last)
            if blk >= nblk:
                inside = jnp.logical_not(top_dev if blk < nblk + 3 else low_dev)
                a_ok, b_ok = a_ok & inside, b_ok & inside
                mine = jnp.where(inside, mine, 0.0)
            a = jnp.where(a_ok, a, 0.0)
            b = jnp.where(b_ok, b, 0.0)
            t0 = jnp.where(lane_k < HALO, a, jnp.where(lane_k < HALO + cols, mine, b))
            t1 = jnp.where(lane_k < cols + 2 * HALO - LANES, b, 0.0)
            return jnp.concatenate([t0, t1], axis=1).astype(BF)

        def expand(row, x0, x1):
            for m in range(4):
                e = e8[8 * step * m : 8 * step * (m + 1)]
                y0 = mm(e, x0).reshape(step, 8, 256)
                y1 = mm(e, x1).reshape(step, 8, 256)
                v = jnp.concatenate([y0, y1], axis=1).astype(BF)
                spec[step * m : step * (m + 1), row : row + 16, :] = v

        def columns(lo, count):
            for b in range(bands):
                mid[b, lo : lo + count] = mm(spec[b, lo : lo + count][:, :ku], tt[b]).astype(BF)

        packing(0, range(nblk))
        own_edges = [to((0, 0), (1, 0), 0, left), to((1, 0), (0, 0), 1, right)]
        r_up.start()
        r_down.start()
        packing(1, range(nblk - 3, nblk))
        packing(2, range(3))
        halo_edges = [
            to((1, 1), (0, 1), 2, corners[1, 1]),
            to((0, 1), (1, 1), 3, corners[1, -1]),
            to((1, 2), (0, 2), 4, corners[-1, 1]),
            to((0, 2), (1, 2), 5, corners[-1, -1]),
        ]

        @pl.when(n == 0)
        def _():
            lax.fori_loop(0, 2, lambda p, c: tt_pair(p * (slabs - 1), c, depth=SLOT), 0)

        for c in own_edges:
            c.wait()
        for i in range(nblk // 2):
            expand(16 * i, block(2 * i, 0, 2 * i), block(2 * i + 1, 0, 2 * i + 1))
        columns(0, rows)

        @pl.when(n == 0)
        def _():
            lax.fori_loop(0, rows // 16, rr_pair, 0)

        r_up.wait()
        r_down.wait()
        for k in range(2):
            a, b = tight_in[n, k, 0].astype(F32), tight_in[n, k, 1].astype(F32)
            ext[n, nblk + 3 * k] = tight_in[n, k, 0]
            b1 = jnp.where(lane_k < cut, pltpu.roll(a, cut, 1), pltpu.roll(b, cut, 1))
            ext[n, nblk + 3 * k + 1] = b1.astype(BF)
            ext[n, nblk + 3 * k + 2] = pltpu.roll(b, 2 * cut, 1).astype(BF)
        for c in halo_edges:
            c.wait()
        for i in range(3):
            k0, k1 = 2 * i, 2 * i + 1
            expand(
                rows + 16 * i,
                block(nblk + k0, 1 + k0 // 3, k0 % 3),
                block(nblk + k1, 1 + k1 // 3, k1 % 3),
            )
        columns(rows, ext_r - rows)

        for t in range(third):
            v = jnp.concatenate([mid[t], mid[third + t], mid[2 * third + t]], axis=0)
            v = mm(rr[t][:, : 3 * ext_r], v)
            for k in range(3):
                fin[third * k + t] = v[rows * k : rows * (k + 1)]

        for i in range(nblk):
            v = fin[:bands, 8 * i : 8 * (i + 1), :].reshape(bands * 8, LANES).astype(BF)
            vec[n + 1, i] = mm(p8[...], v) + ridge[...] * vec[n, i]
        return carry

    lax.fori_loop(0, 2, normal, 0)

    def products(i, sums):
        a, b, c = vec[0, i], vec[1, i], vec[2, i]
        parts = [a * a, a * b, b * b, a * c, b * c]
        return tuple(s + jnp.sum(v.reshape(comps, 8, LANES), axis=0) for s, v in zip(sums, parts))

    zero = jnp.zeros((8, LANES), F32)
    sums = lax.fori_loop(0, nblk, products, (zero,) * 5)
    total = jnp.concatenate([jnp.sum(v, axis=0, keepdims=True) for v in sums] + [jnp.zeros((3, LANES), F32)], axis=0)
    at = 0
    for level, (group, place, count) in enumerate(((peers, j, nbd), (peers_r, i_row, nrow))):
        red_src[level] = total
        red_in[level, place] = total
        copies = []
        for d in group:
            c = remote(red_src.at[level], red_in.at[level, place], red_sem.at[0, at], red_sem.at[1, at], d)
            c.start()
            copies.append(c)
            at += 1
        for c in copies:
            c.wait()
        total = red_in[level, 0]
        for k in range(1, count):
            total = total + red_in[level, k]
    tot = jnp.sum(total, axis=1, keepdims=True)
    r00, r01, r11, r02, r12 = [tot[k : k + 1] for k in range(5)]
    alpha = r00 / r01
    new = r00 - 2.0 * alpha * r01 + alpha * alpha * r11
    gain = 1.0 + new / r00
    curve = gain * gain * r01 - alpha * gain * (r11 + r02) + alpha * alpha * r12
    alpha2 = new / curve

    def finish(i, carry):
        a, b, c = vec[0, i], vec[1, i], vec[2, i]
        xs = alpha * a + alpha2 * (gain * a - alpha * b)
        rs = (a - alpha * b) - alpha2 * (gain * b - alpha * c)
        sl = pl.ds(pl.multiple_of(8 * i, 8), 8)
        out[0, :, sl, :] = xs.reshape(comps, 8, LANES)
        out[1, :, sl, :] = rs.reshape(comps, 8, LANES)
        return carry

    lax.fori_loop(0, nblk, finish, 0)


def local(height, width, sizes, observed, row_taps, col_taps, spectral_basis, ridge_weights):
    own, rows, _ = observed.shape
    bands, comps = spectral_basis.shape
    ny, nc, nx, nz = sizes
    nbd = ny * nc
    cols = width // nbd
    full = -(-width // LANES) * LANES
    ext_r = rows + 2 * HALO
    ck, nblk = comps * 8, rows // 8
    third = -(-bands // 24) * 8
    ku = -(-(cols + 2 * HALO) // 16) * 16
    kw = -(-(nc * cols + 2 * RAD) // 16) * 16

    pad_own = -(-own // 16) * 16

    def vm(*shape, dtype=BF):
        return pltpu.VMEM(shape, dtype)

    dma = pltpu.SemaphoreType.DMA
    scratch = [
        vm(own, rows, width),
        dma,
        vm(2, own * RAD, width),
        vm(4, pad_own, 256),
        vm(own, 8, LANES, dtype=F32),
        vm(ck, LANES, dtype=F32),
        vm(2 * pad_own, LANES, dtype=F32),
        vm(2, 4 * rows, full, dtype=F32),
        vm(2, own * RAD, width),
        vm(nbd, 2, pad_own, 256),
        vm(2, bands, 256, dtype=F32),
        vm(own // 4, 4 * rows, 256),
        vm(own, kw, 256),
        vm(ny, own, rows, 256, dtype=F32),
        vm(ny, nblk, ck, LANES, dtype=F32),
        vm(ny, nblk, ck, LANES),
        vm(ny, nblk, ck, LANES),
        vm(ny - 1, 3, ck, LANES),
        vm(ny - 1, 3, ck, LANES),
        vm(bands, ku, LANES),
        vm(third, 3 * rows, 256),
        vm(bands * 8, ck),
        vm(ck, bands * 8),
        vm(ck, 256),
        vm(bands, ext_r, 256),
        vm(3 * third, ext_r, LANES),
        vm(3 * third, rows, LANES, dtype=F32),
        vm(bands // 8, LANES, LANES, dtype=F32),
        vm(2, ext_r // 8, ck, LANES),
        vm(2, 2, 3, ck, LANES),
        vm(2, 2, 3, ck, LANES),
        vm(3, nblk, ck, LANES, dtype=F32),
        vm(2, 8, LANES, dtype=F32),
        vm(2, max(nbd, nx * nz), 8, LANES, dtype=F32),
        vm(2, 2, 2, ck, LANES),
        vm(2, 2, 2, ck, LANES),
        dma((2, 2, 2)),
        dma((2, nbd - 1, 2)),
        dma((2, ny)),
        dma((2, ny - 1)),
        dma((2, 4)),
        dma((2, 2, 6)),
        dma((2, nbd + nx * nz - 2)),
    ]
    vmem = pl.BlockSpec(memory_space=pltpu.VMEM)
    both = pl.pallas_call(
        functools.partial(kernel, (cols, sizes)),
        out_shape=jax.ShapeDtypeStruct((2, comps, rows, LANES), F32),
        in_specs=[pl.BlockSpec(memory_space=pl.ANY)] + [vmem] * 4,
        out_specs=vmem,
        scratch_shapes=scratch,
        compiler_params=pltpu.CompilerParams(
            collective_id=0, has_side_effects=True, vmem_limit_bytes=67043328
        ),
    )(observed, row_taps, col_taps, spectral_basis.T, ridge_weights[None, :])
    return both[0, :, :, :cols], both[1, :, :, :cols]


def solution(mesh):
    sizes = (4, 2, 4, 4)
    split = Mesh(mesh.devices.reshape(sizes), AXES)
    placed = (P(BAND, ROW, None), P(BAND, None), P(BAND, None), P(), P())

    def whole(observed, row_taps, col_taps, spectral_basis, ridge_weights):
        _, height, width = observed.shape
        return jax.shard_map(
            functools.partial(local, height, width, sizes),
            mesh=split,
            in_specs=placed,
            out_specs=(P(None, ROW, BAND), P(None, ROW, BAND)),
            check_vma=False,
        )(observed, row_taps, col_taps, spectral_basis, ridge_weights)

    return whole
```

```python
import functools

import jax
import jax.numpy as jnp
from jax import lax
from jax.experimental import pallas as pl
from jax.experimental.pallas import tpu as pltpu
from jax.sharding import Mesh
from jax.sharding import PartitionSpec as P

AXES = ("band_0", "band_1", "row_0", "row_1")
BAND = ("band_0", "band_1")
ROW = ("row_0", "row_1")
TAPS = 25
RAD = 12
HALO = 24
LANES = 128
SLOT = 64
BF = jnp.bfloat16
F32 = jnp.float32


def iota(shape, dim):
    return lax.broadcasted_iota(jnp.int32, shape, dim)


def mm(a, b):
    return lax.dot_general(a, b, (((1,), (0,)), ((), ())), preferred_element_type=F32)


def halves(v):
    hi = v.astype(BF)
    return hi, (v - hi.astype(F32)).astype(BF)


def onehot(mask):
    return jnp.where(mask, 1.0, 0.0)


def staircase(line, rows, shift):
    step = pltpu.roll(jnp.broadcast_to(line, (8, LANES)), 0, 1, stride=1, stride_axis=0)
    tiles = []
    for g in range(rows // 8):
        turn = (shift + 8 * g) % LANES
        tiles.append(pltpu.roll(step, turn, 1) if turn else step)
    return jnp.concatenate(tiles, axis=0)


def kernel(
    dims, obs_in, row_taps, col_taps, basis_t, ridge_in,
    out,
    obs, obs_sem, edges, feats, taps, ridge, raw, vpad, edge_in, line_in, lines, rows_adj, cols_adj, zed, keep, out_a, in_a, out_b, in_b,
    tt, rr, e8, p8, p8_own, spec, mid, fin, work, ext, pack, pack_in, vec, red_src, red_in, tight, tight_in,
    edge_sem, line_sem, a_sem, b_sem, row_sem, col_sem, red_sem,
):
    cols, sizes = dims
    ny, nc, nx, nz = sizes
    nbd, nrow = ny * nc, nx * nz
    y, core = lax.axis_index("band_0"), lax.axis_index("band_1")
    x, z = lax.axis_index("row_0"), lax.axis_index("row_1")
    j, i_row = y * nc + core, x * nz + z
    own, rows, full = obs.shape
    comps, bands = basis_t.shape
    ext_r = rows + 2 * HALO
    nblk = rows // 8
    ck = comps * 8
    ku = tt.shape[1]
    first, last = j == 0, j == nbd - 1
    top_dev, low_dev = i_row == 0, i_row == nrow - 1

    def at_band(jj):
        return (jj // nc, lax.rem(jj, nc), x, z)

    def at_row(ii):
        return (y, core, ii // nz, lax.rem(ii, nz))

    up = at_row(lax.rem(i_row + nrow - 1, nrow))
    down = at_row(lax.rem(i_row + 1, nrow))
    left = at_band(lax.rem(j + nbd - 1, nbd))
    right = at_band(lax.rem(j + 1, nbd))
    partner = (y, 1 - core, x, z)
    peers = [at_band(lax.rem(j + s, nbd)) for s in range(1, nbd)]
    peers_r = [at_row(lax.rem(i_row + s, nrow)) for s in range(1, nrow)]


    def corner(di, dj):
        ii, jj = lax.rem(i_row + nrow + di, nrow), lax.rem(j + nbd + dj, nbd)
        return (jj // nc, lax.rem(jj, nc), ii // nz, lax.rem(ii, nz))

    corners = {(di, dj): corner(di, dj) for di in (-1, 1) for dj in (-1, 1)}

    barrier = pltpu.get_barrier_semaphore()
    everyone = peers + peers_r + list(corners.values())
    for d in everyone:
        pl.semaphore_signal(barrier, inc=1, device_id=d, device_id_type=pl.DeviceIdType.MESH)

    fetch = pltpu.make_async_copy(obs_in, obs, obs_sem)
    fetch.start()
    fetch.wait()

    def pack_edges(g, carry):
        sl = pl.ds(pl.multiple_of(4 * RAD * g, 16), 4 * RAD)
        v = obs[pl.ds(4 * g, 4)].astype(F32)
        for k, lo in enumerate((0, rows - RAD)):
            slab = jnp.concatenate([v[q, lo : lo + RAD] for q in range(4)], axis=0)
            edges[k, sl, :] = slab.astype(BF)
        return carry

    lax.fori_loop(0, own // 4, pack_edges, 0)
    pl.semaphore_wait(barrier, len(everyone))

    def remote(src, dst, send, recv, device):
        return pltpu.make_async_remote_copy(
            src_ref=src, dst_ref=dst, send_sem=send, recv_sem=recv,
            device_id=device, device_id_type=pl.DeviceIdType.MESH,
        )

    slabs_own = own // 4
    starts = [0, slabs_own // 2, slabs_own - 1, slabs_own]
    edge_copies = {}
    for part in range(3):
        sl = pl.ds(4 * RAD * starts[part], 4 * RAD * (starts[part + 1] - starts[part]))
        a = remote(edges.at[0, sl], edge_in.at[1, sl], edge_sem.at[0, part, 0], edge_sem.at[1, part, 0], up)
        b = remote(edges.at[1, sl], edge_in.at[0, sl], edge_sem.at[0, part, 1], edge_sem.at[1, part, 1], down)
        a.start()
        b.start()
        edge_copies[starts[part]] = (a, b)

    pad_own = feats.shape[1]
    raw[...] = jnp.zeros_like(raw)
    raw[:own, :TAPS] = col_taps[...]
    raw[pad_own : pad_own + own, :TAPS] = row_taps[...]
    t = raw[...]
    t_hi, t_lo = halves(t)
    gr, gp = iota((LANES, 640), 0), iota((LANES, 640), 1)
    g1 = (gp * 5243) >> 17
    g1, g2 = onehot(gr == g1).astype(BF), onehot(gr == gp - TAPS * g1).astype(BF)
    prod = (mm(t_hi, g1) + mm(t_lo, g1)) * (mm(t_hi, g2) + mm(t_lo, g2))
    p_hi, p_lo = halves(prod)
    pp, f = iota((640, 256), 0), iota((640, 256), 1)
    m1 = (pp * 5243) >> 17
    m2 = pp - TAPS * m1
    fe = f - SLOT
    fx = (fe * 5462) >> 16
    fy = fe - RAD * fx
    lag = (f < 2 * TAPS - 1) & (m2 - m1 + TAPS - 1 == f)
    edge = (fe >= 0) & (fe < RAD * RAD)
    for k, cut in enumerate((
        (m1 - fx == m2 - fy) & (m1 - fx > RAD) & (m1 < TAPS),
        (m1 + fx == m2 + fy) & (m1 + fx < RAD),
    )):
        sel = onehot(lag | (edge & cut)).astype(BF)
        v = (mm(p_hi, sel) + mm(p_lo, sel)).astype(BF)
        feats[k] = v[:pad_own]
        feats[2 + k] = v[pad_own:]
    flip = onehot(iota((LANES, LANES), 0) + iota((LANES, LANES), 1) == TAPS - 1).astype(BF)
    taps[:, 0:1, :] = t[:own].reshape(own, 1, LANES)
    taps[:, 1:2, :] = mm(t_hi, flip)[pad_own : pad_own + own].reshape(own, 1, LANES)

    line_copies = []
    row_kind = jnp.where(low_dev, 3, 2)
    for s in range(1, nbd):
        dest = lax.rem(j + s, nbd)
        for k, kind in enumerate((jnp.where(dest == nbd - 1, 1, 0), row_kind)):
            c = remote(
                feats.at[kind], line_in.at[j, k], line_sem.at[0, s - 1, k], line_sem.at[1, s - 1, k], at_band(dest)
            )
            c.start()
            line_copies.append(c)
    line_in[j, 0] = feats[jnp.where(last, 1, 0)]
    line_in[j, 1] = feats[row_kind]

    r, l = iota((rows, LANES), 0), iota((rows, LANES), 1)

    def own_rows(g, carry):
        for q in range(4):
            line = taps[4 * g + q][1:2]
            d = l - rows * q + RAD - r
            m = (d >= 0) & (d < TAPS) & (l >= rows * q) & (l < rows * (q + 1))
            mine = jnp.where(m, staircase(line, rows, rows * q - RAD), 0.0)
            k = l - RAD * q
            d = k - r
            m = (d >= 0) & (d < TAPS) & (k >= 0) & (k < RAD)
            above = jnp.where(m, staircase(line, rows, RAD * q), 0.0)
            k = l - 4 * RAD - RAD * q
            d = k + rows + RAD - r
            m = (d >= 0) & (d < TAPS) & (k >= 0) & (k < RAD)
            below = jnp.where(m, staircase(line, rows, 4 * RAD + RAD * q - RAD - rows), 0.0)
            rows_adj[g, rows * q : rows * (q + 1), :LANES] = mine.astype(BF)
            rows_adj[g, rows * q : rows * (q + 1), LANES:] = (above + below).astype(BF)
        return carry

    lax.fori_loop(0, own // 4, own_rows, 0)

    kw = cols_adj.shape[1]
    w, o = iota((kw, LANES), 0), iota((kw, LANES), 1)

    def own_cols(b, carry):
        line = taps[b][0:1]
        for k in range(2):
            d = w - o - cols * k
            m = (d >= 0) & (d < TAPS) & (o < cols)
            t = jnp.where(m, staircase(line, kw, -HALO - cols * k), 0.0)
            cols_adj[b, :, LANES * k : LANES * (k + 1)] = t.astype(BF)
        return carry

    lax.fori_loop(0, own, own_cols, 0)

    spread = onehot(iota((comps, ck), 0) == (iota((comps, ck), 1) >> 3)).astype(BF)
    wide = lax.dot_general(basis_t[...], spread, (((0,), (0,)), ((), ())), preferred_element_type=F32)
    step = bands // 4
    er, el = iota((8 * step, ck), 0), iota((8 * step, ck), 1)
    for c in range(4):
        v = jnp.broadcast_to(wide[step * c : step * (c + 1)][:, None, :], (step, 8, ck)).reshape(8 * step, ck)
        e8[8 * step * c : 8 * step * (c + 1)] = jnp.where((er & 7) == (el & 7), v, 0.0).astype(BF)
    tall = onehot(iota((ck, comps), 1) == (iota((ck, comps), 0) >> 3)).astype(BF)
    tall = mm(tall, basis_t[...]).astype(BF)
    br, bl = iota((bands, 256), 0), iota((bands, 256), 1)
    same = (iota((ck, 256), 0) & 7) == (iota((ck, 256), 1) & 7)
    kr, kl = iota((ck, comps), 0), iota((ck, comps), 1)
    ridge_col = jnp.sum(jnp.where(kl == (kr >> 3), ridge_in[...], 0.0), axis=1, keepdims=True)
    ridge[...] = jnp.broadcast_to(ridge_col, (ck, LANES))
    vpad[...] = jnp.zeros_like(vpad)

    def widen(start):
        return jnp.where(same, mm(tall, onehot(br == start + (bl >> 3)).astype(BF)), 0.0).astype(BF)

    for c in range(bands // 32):
        p8[:, 256 * c : 256 * (c + 1)] = widen(32 * c)
    p8_own[...] = widen(own * j)

    for c in line_copies:
        c.wait()
    for k in range(2):
        for jj in range(nbd):
            lines[k, own * jj : own * (jj + 1)] = line_in[jj, k][:own].astype(F32)
    groups = bands // 8
    wide_n = 16 * LANES

    def shifted(depth, hit, edge_hit):
        f, n = iota((depth, wide_n), 0), iota((1, wide_n), 1)
        s = onehot(f == hit(n))
        if edge_hit is not None:
            s = s - onehot(f == edge_hit(n))
        return s.astype(BF)

    def unfold(k, depth, sel):
        res = mm(lines[k, :, :depth].astype(BF), sel)
        for t in range(16):
            work[:, 8 * t : 8 * (t + 1), :] = res[:, LANES * t : LANES * (t + 1)].reshape(groups, 8, LANES)

    def tt_pair(p, carry, depth):
        def hit(n):
            a, b = 16 * p + (n >> 7), n & 127
            return jnp.where((b < cols) & (a < cols + 2 * HALO) & (a - b <= 2 * HALO), a - b, -1)

        def edge_hit(n):
            a, b = 16 * p + (n >> 7) - HALO, n & 127
            a, b = jnp.where(last, cols - 1 - a, a), jnp.where(last, cols - 1 - b, b)
            ok = (first | last) & (a >= 0) & (a < RAD) & (b >= 0) & (b < RAD)
            return jnp.where(ok, SLOT + RAD * a + b, -1)

        unfold(0, depth, shifted(depth, hit, edge_hit if depth > SLOT else None))

        def place(g, c):
            for s in range(8):
                v = work[g, pl.ds(s, 16, stride=8), :]
                tt[8 * g + s, pl.ds(pl.multiple_of(16 * p, 16), 16), :] = v.astype(BF)
            return c

        lax.fori_loop(0, groups, place, 0)
        return carry

    third = rr.shape[0]
    lane16 = iota((16, LANES), 1)

    def rr_pair(p, carry):
        def row_of(n):
            b = n & 127
            return jnp.where(b < rows, b + HALO, jnp.where(b < rows + HALO, b - rows, b))

        def hit(n):
            a, b = 16 * p + (n >> 7), row_of(n)
            return jnp.where((b < ext_r) & (b >= a) & (b - a <= 2 * HALO), b - a, -1)

        def edge_hit(n):
            a, b = 16 * p + (n >> 7), row_of(n) - HALO
            a, b = jnp.where(low_dev, rows - 1 - a, a), jnp.where(low_dev, rows - 1 - b, b)
            ok = (top_dev | low_dev) & (a >= 0) & (a < RAD) & (b >= 0) & (b < RAD)
            return jnp.where(ok, SLOT + RAD * a + b, -1)

        unfold(1, 256, shifted(256, hit, edge_hit))
        for q in range(3):
            lo = ext_r * q

            def place(g, c):
                for s in range(8):
                    v = work[g, pl.ds(s, 16, stride=8), :]
                    if lo % LANES:
                        v = pltpu.roll(v, lo % LANES, 1)
                    t0 = v if lo + ext_r <= LANES else jnp.where(lane16 >= lo, v, 0.0)
                    t1 = v if lo >= LANES else jnp.where(lane16 < lo + ext_r - LANES, v, 0.0)
                    at = (8 * g + s - third * q, pl.ds(pl.multiple_of(rows * q + 16 * p, 16), 16))
                    rr[at + (slice(0, LANES),)] = t0.astype(BF)
                    rr[at + (slice(LANES, 2 * LANES),)] = t1.astype(BF)
                return c

            lax.fori_loop(third * q // 8, min(third * (q + 1), bands) // 8, place, 0)
        return carry

    slabs = ku // 16
    lax.fori_loop(1, 3, functools.partial(tt_pair, depth=SLOT), 0)

    above_ok, below_ok = i_row > 0, i_row < nrow - 1

    def adjoint(g):
        e = slice(4 * RAD * g, 4 * RAD * (g + 1))
        above = edge_in[0, e]
        below = edge_in[1, e]
        mine = obs[4 * g : 4 * g + 4].reshape(4 * rows, full)
        above = jnp.where(above_ok, above, jnp.zeros_like(above))
        below = jnp.where(below_ok, below, jnp.zeros_like(below))
        v = mm(rows_adj[g][:, : 4 * rows + 8 * RAD], jnp.concatenate([mine, above, below], axis=0))
        vpad[g % 2, :, :full] = v
        v = vpad[g % 2]
        wins = []
        for k in range(ny):
            start = nc * cols * k - RAD
            wins.append(pltpu.roll(v, (v.shape[1] - start) % v.shape[1], 1)[:, :256].astype(BF))
        for q in range(4):
            u = jnp.concatenate([t[rows * q : rows * (q + 1)] for t in wins], axis=0)
            u = mm(u[:, :kw], cols_adj[4 * g + q])
            for k in range(ny):
                zed[k, 4 * g + q] = u[rows * k : rows * (k + 1)]

    for g in range(own // 4):
        for c in edge_copies.get(g, ()):
            c.wait()
        adjoint(g)

    lane_k = iota((ck, LANES), 1)
    cut = LANES - cols
    way = jnp.where(core == 0, ny - 1, 1)
    offsets = [2, ny - way, way, 0]
    hops = [way, ny - way, way]
    swap = [0, 2, 1, 3]
    a_copies, b_copies = [], {}

    def merge(idx):
        a_copies[swap[idx]].wait_recv()
        done = idx == len(offsets) - 1

        def add(i):
            return keep[idx, i] + in_a[idx, i].astype(F32)

        if done:
            for i in range(nblk):
                vec[0, i] = add(i)
        else:
            b = pltpu.roll(add(1), cols, 1)
            tiles = [
                jnp.where(lane_k < cols, add(0), b),
                jnp.where(lane_k < cols - cut, b, pltpu.roll(add(2), cols - cut, 1)),
                add(3),
            ]
            if idx == 2:
                b_copies[0].wait()
            for t, v in enumerate(tiles):
                if idx == 2:
                    v = v + in_b[0, t].astype(F32)
                out_b[idx, t] = v.astype(BF)
        if not done:
            dest = (lax.rem(y + hops[idx], ny), core, x, z)
            c = remote(out_b.at[idx], in_b.at[idx], b_sem.at[0, idx], b_sem.at[1, idx], dest)
            c.start()
            b_copies[idx] = c

    for idx, off in enumerate(offsets):
        k = lax.rem(y + off, ny)

        for i in range(nblk):
            v = zed[k, :, 8 * i : 8 * (i + 1), :].reshape(own * 8, 256).astype(BF)
            v = mm(p8_own[:, : own * 8], v)
            lo, hi = v[:, :LANES], v[:, LANES:]
            keep[idx, i] = jnp.where(core == 0, lo, hi)
            out_a[idx, i] = jnp.where(core == 0, hi, lo).astype(BF)
        c = remote(out_a.at[idx], in_a.at[swap[idx]], a_sem.at[0, idx], a_sem.at[1, swap[idx]], partner)
        c.start()
        a_copies.append(c)
        if idx in (1, 2):
            merge(idx - 1)
    merge(3)
    lax.fori_loop(3, slabs - 3, functools.partial(tt_pair, depth=SLOT), 0)
    merge(2)
    lax.fori_loop(slabs - 3, slabs - 1, functools.partial(tt_pair, depth=SLOT), 0)

    @pl.when(first | last)
    def _():
        p0 = jnp.where(first, HALO // 16, (cols + RAD - 1) // 16)
        lax.fori_loop(p0, p0 + 2, functools.partial(tt_pair, depth=256), 0)

    mid[pl.ds(bands, mid.shape[0] - bands)] = jnp.zeros((mid.shape[0] - bands, ext_r, LANES), BF)
    b_copies[1].wait()
    b_copies[2].wait()
    for c in a_copies:
        c.wait_send()
    a, b, c = (in_b[1, t].astype(F32) + in_b[2, t].astype(F32) for t in range(3))
    b1 = jnp.where(lane_k < cut, pltpu.roll(a, cut, 1), pltpu.roll(b, cut, 1))
    for i, v in enumerate((a, b1, pltpu.roll(b, 2 * cut, 1), c)):
        vec[0, i] = vec[0, i] + jnp.where(lane_k < cols, v, 0.0)

    chunk = ck // 4
    lane_c = iota((chunk, LANES), 1)

    def normal(n, carry):
        def stage(i, c):
            ext[n, i] = vec[n, i].astype(BF)
            return c

        lax.fori_loop(0, nblk, stage, 0)
        for k, lo in enumerate((0, nblk - 3)):
            a, b, c = (vec[n, lo + q] for q in range(3))
            b = pltpu.roll(b, cols, 1)
            c = pltpu.roll(c, cols - cut, 1)
            tight[n, k, 0] = jnp.where(lane_k < cols, a, b).astype(BF)
            tight[n, k, 1] = jnp.where(lane_k < cols - cut, b, c).astype(BF)
        r_up = remote(tight.at[n, 0], tight_in.at[n, 1], row_sem.at[n, 0], row_sem.at[n, 2], up)
        r_down = remote(tight.at[n, 1], tight_in.at[n, 0], row_sem.at[n, 1], row_sem.at[n, 3], down)

        def packing(t, blocks):
            def part(c, cc):
                sl = pl.ds(pl.multiple_of(chunk * c, chunk), chunk)
                a = jnp.zeros((chunk, LANES), F32)
                b = a
                for g, blk in enumerate(blocks):
                    v = ext[n, blk, sl, :].astype(F32)
                    m = (lane_c >= HALO * g) & (lane_c < HALO * (g + 1))
                    a = jnp.where(m, pltpu.roll(v, HALO * g, 1) if g else v, a)
                    b = jnp.where(m, pltpu.roll(v, (HALO * g - cols + HALO) % LANES, 1), b)
                pack[n, 0, t, sl, :] = a.astype(BF)
                pack[n, 1, t, sl, :] = b.astype(BF)
                return cc

            lax.fori_loop(0, ck // chunk, part, 0)

        def to(src, dst, k, device):
            c = remote(pack.at[(n,) + src], pack_in.at[(n,) + dst], col_sem.at[n, 0, k], col_sem.at[n, 1, k], device)
            c.start()
            return c

        def block(blk, t, g):
            mine = pltpu.roll(ext[n, blk].astype(F32), HALO, 1)
            a = pltpu.roll(pack_in[n, 0, t].astype(F32), (LANES - HALO * g) % LANES, 1)
            b = pltpu.roll(pack_in[n, 1, t].astype(F32), (cols + HALO - HALO * g) % LANES, 1)
            a_ok, b_ok = jnp.logical_not(first), jnp.logical_not(last)
            if blk >= nblk:
                inside = jnp.logical_not(top_dev if blk < nblk + 3 else low_dev)
                a_ok, b_ok = a_ok & inside, b_ok & inside
                mine = jnp.where(inside, mine, 0.0)
            a = jnp.where(a_ok, a, 0.0)
            b = jnp.where(b_ok, b, 0.0)
            t0 = jnp.where(lane_k < HALO, a, jnp.where(lane_k < HALO + cols, mine, b))
            t1 = jnp.where(lane_k < cols + 2 * HALO - LANES, b, 0.0)
            return jnp.concatenate([t0, t1], axis=1).astype(BF)

        def expand(row, x0, x1):
            for m in range(4):
                e = e8[8 * step * m : 8 * step * (m + 1)]
                y0 = mm(e, x0).reshape(step, 8, 256)
                y1 = mm(e, x1).reshape(step, 8, 256)
                v = jnp.concatenate([y0, y1], axis=1).astype(BF)
                spec[step * m : step * (m + 1), row : row + 16, :] = v

        def columns(lo, count):
            for b in range(bands):
                mid[b, lo : lo + count] = mm(spec[b, lo : lo + count][:, :ku], tt[b]).astype(BF)

        packing(0, range(nblk))
        own_edges = [to((0, 0), (1, 0), 0, left), to((1, 0), (0, 0), 1, right)]
        r_up.start()
        r_down.start()
        packing(1, range(nblk - 3, nblk))
        packing(2, range(3))
        halo_edges = [
            to((1, 1), (0, 1), 2, corners[1, 1]),
            to((0, 1), (1, 1), 3, corners[1, -1]),
            to((1, 2), (0, 2), 4, corners[-1, 1]),
            to((0, 2), (1, 2), 5, corners[-1, -1]),
        ]

        @pl.when(n == 0)
        def _():
            lax.fori_loop(0, 2, lambda p, c: tt_pair(p * (slabs - 1), c, depth=SLOT), 0)

        for c in own_edges:
            c.wait()
        for i in range(nblk // 2):
            expand(16 * i, block(2 * i, 0, 2 * i), block(2 * i + 1, 0, 2 * i + 1))
        columns(0, rows)

        @pl.when(n == 0)
        def _():
            lax.fori_loop(0, rows // 16, rr_pair, 0)

        r_up.wait()
        r_down.wait()
        for k in range(2):
            a, b = tight_in[n, k, 0].astype(F32), tight_in[n, k, 1].astype(F32)
            ext[n, nblk + 3 * k] = tight_in[n, k, 0]
            b1 = jnp.where(lane_k < cut, pltpu.roll(a, cut, 1), pltpu.roll(b, cut, 1))
            ext[n, nblk + 3 * k + 1] = b1.astype(BF)
            ext[n, nblk + 3 * k + 2] = pltpu.roll(b, 2 * cut, 1).astype(BF)
        for c in halo_edges:
            c.wait()
        for i in range(3):
            k0, k1 = 2 * i, 2 * i + 1
            expand(
                rows + 16 * i,
                block(nblk + k0, 1 + k0 // 3, k0 % 3),
                block(nblk + k1, 1 + k1 // 3, k1 % 3),
            )
        columns(rows, ext_r - rows)

        for t in range(third):
            v = jnp.concatenate([mid[t], mid[third + t], mid[2 * third + t]], axis=0)
            v = mm(rr[t][:, : 3 * ext_r], v)
            for k in range(3):
                fin[third * k + t] = v[rows * k : rows * (k + 1)]

        for i in range(nblk):
            v = fin[:bands, 8 * i : 8 * (i + 1), :].reshape(bands * 8, LANES).astype(BF)
            vec[n + 1, i] = mm(p8[...], v) + ridge[...] * vec[n, i]
        return carry

    lax.fori_loop(0, 2, normal, 0)

    def products(i, sums):
        a, b, c = vec[0, i], vec[1, i], vec[2, i]
        parts = [a * a, a * b, b * b, a * c, b * c]
        return tuple(s + jnp.sum(v.reshape(comps, 8, LANES), axis=0) for s, v in zip(sums, parts))

    zero = jnp.zeros((8, LANES), F32)
    sums = lax.fori_loop(0, nblk, products, (zero,) * 5)
    total = jnp.concatenate([jnp.sum(v, axis=0, keepdims=True) for v in sums] + [jnp.zeros((3, LANES), F32)], axis=0)
    at = 0
    for level, (group, place, count) in enumerate(((peers, j, nbd), (peers_r, i_row, nrow))):
        red_src[level] = total
        red_in[level, place] = total
        copies = []
        for d in group:
            c = remote(red_src.at[level], red_in.at[level, place], red_sem.at[0, at], red_sem.at[1, at], d)
            c.start()
            copies.append(c)
            at += 1
        for c in copies:
            c.wait()
        total = red_in[level, 0]
        for k in range(1, count):
            total = total + red_in[level, k]
    tot = jnp.sum(total, axis=1, keepdims=True)
    r00, r01, r11, r02, r12 = [tot[k : k + 1] for k in range(5)]
    alpha = r00 / r01
    new = r00 - 2.0 * alpha * r01 + alpha * alpha * r11
    gain = 1.0 + new / r00
    curve = gain * gain * r01 - alpha * gain * (r11 + r02) + alpha * alpha * r12
    alpha2 = new / curve

    def finish(i, carry):
        a, b, c = vec[0, i], vec[1, i], vec[2, i]
        xs = alpha * a + alpha2 * (gain * a - alpha * b)
        rs = (a - alpha * b) - alpha2 * (gain * b - alpha * c)
        sl = pl.ds(pl.multiple_of(8 * i, 8), 8)
        out[0, :, sl, :] = xs.reshape(comps, 8, LANES)
        out[1, :, sl, :] = rs.reshape(comps, 8, LANES)
        return carry

    lax.fori_loop(0, nblk, finish, 0)


def local(height, width, sizes, observed, row_taps, col_taps, spectral_basis, ridge_weights):
    own, rows, _ = observed.shape
    bands, comps = spectral_basis.shape
    ny, nc, nx, nz = sizes
    nbd = ny * nc
    cols = width // nbd
    full = -(-width // LANES) * LANES
    ext_r = rows + 2 * HALO
    ck, nblk = comps * 8, rows // 8
    third = -(-bands // 24) * 8
    ku = -(-(cols + 2 * HALO) // 16) * 16
    kw = -(-(nc * cols + 2 * RAD) // 16) * 16

    pad_own = -(-own // 16) * 16

    def vm(*shape, dtype=BF):
        return pltpu.VMEM(shape, dtype)

    dma = pltpu.SemaphoreType.DMA
    scratch = [
        vm(own, rows, width),
        dma,
        vm(2, own * RAD, width),
        vm(4, pad_own, 256),
        vm(own, 8, LANES, dtype=F32),
        vm(ck, LANES, dtype=F32),
        vm(2 * pad_own, LANES, dtype=F32),
        vm(2, 4 * rows, full, dtype=F32),
        vm(2, own * RAD, width),
        vm(nbd, 2, pad_own, 256),
        vm(2, bands, 256, dtype=F32),
        vm(own // 4, 4 * rows, 256),
        vm(own, kw, 256),
        vm(ny, own, rows, 256, dtype=F32),
        vm(ny, nblk, ck, LANES, dtype=F32),
        vm(ny, nblk, ck, LANES),
        vm(ny, nblk, ck, LANES),
        vm(ny - 1, 3, ck, LANES),
        vm(ny - 1, 3, ck, LANES),
        vm(bands, ku, LANES),
        vm(third, 3 * rows, 256),
        vm(bands * 8, ck),
        vm(ck, bands * 8),
        vm(ck, 256),
        vm(bands, ext_r, 256),
        vm(3 * third, ext_r, LANES),
        vm(3 * third, rows, LANES, dtype=F32),
        vm(bands // 8, LANES, LANES, dtype=F32),
        vm(2, ext_r // 8, ck, LANES),
        vm(2, 2, 3, ck, LANES),
        vm(2, 2, 3, ck, LANES),
        vm(3, nblk, ck, LANES, dtype=F32),
        vm(2, 8, LANES, dtype=F32),
        vm(2, max(nbd, nx * nz), 8, LANES, dtype=F32),
        vm(2, 2, 2, ck, LANES),
        vm(2, 2, 2, ck, LANES),
        dma((2, 3, 2)),
        dma((2, nbd - 1, 2)),
        dma((2, ny)),
        dma((2, ny - 1)),
        dma((2, 4)),
        dma((2, 2, 6)),
        dma((2, nbd + nx * nz - 2)),
    ]
    vmem = pl.BlockSpec(memory_space=pltpu.VMEM)
    both = pl.pallas_call(
        functools.partial(kernel, (cols, sizes)),
        out_shape=jax.ShapeDtypeStruct((2, comps, rows, LANES), F32),
        in_specs=[pl.BlockSpec(memory_space=pl.ANY)] + [vmem] * 4,
        out_specs=vmem,
        scratch_shapes=scratch,
        compiler_params=pltpu.CompilerParams(
            collective_id=0, has_side_effects=True, vmem_limit_bytes=67043328
        ),
    )(observed, row_taps, col_taps, spectral_basis.T, ridge_weights[None, :])
    return both[0, :, :, :cols], both[1, :, :, :cols]


def solution(mesh):
    sizes = (4, 2, 4, 4)
    split = Mesh(mesh.devices.reshape(sizes), AXES)
    placed = (P(BAND, ROW, None), P(BAND, None), P(BAND, None), P(), P())

    def whole(observed, row_taps, col_taps, spectral_basis, ridge_weights):
        _, height, width = observed.shape
        return jax.shard_map(
            functools.partial(local, height, width, sizes),
            mesh=split,
            in_specs=placed,
            out_specs=(P(None, ROW, BAND), P(None, ROW, BAND)),
            check_vma=False,
        )(observed, row_taps, col_taps, spectral_basis, ridge_weights)

    return whole
```
